32 devices in a mesh: dp: 1 (over z), gz: 4 (over y), gy: 4 (over x), gx: 2 (over core).
Axes of the slice: x: 4, y: 4, z: 1, core: 2. Of those that a mesh axis runs over, the one named last changes fastest.
The devices are a block of a 4x4x8 slice.
Arguments:
- volume: bfloat16 [256, 32, 64, 64], P('dp', 'gx', 'gy', 'gz')
- cot_out: bfloat16 [256, 32, 64, 64], P('dp', 'gx', 'gy', 'gz')
- filter_taps: float32 [3, 3, 5], replicated
- w_mix: bfloat16 [3, 256, 256], replicated
- b_mix: float32 [3, 256], replicated
Outputs:
- output 1: bfloat16 [256, 32, 64, 64], P('dp', 'gx', 'gy', 'gz')
- output 2: float32 [3, 256, 256], P('dp')
- output 3: float32 [3, 256], P('dp')
All inputs are finite; a program needn't handle non-finite values.
Results may differ from the reference program's by a relative error of at most 0.0125956.
Values are sent between devices in bfloat16 or wider.
A program may use at most 768 MiB of HBM per device.

```python
import jax
import jax.numpy as jnp
from jax import lax

CHANNELS = 256
NUM_TAPS = 5
LAYERS = 3
GRID_X = 32
GRID_Y = 64
GRID_Z = 64
HALF_TAPS = (NUM_TAPS - 1) // 2
TWO_PI = 6.283185307179586


def smooth_field(key):
    keys = jax.random.split(key, 4)
    num_modes = 4
    wave_len = NUM_TAPS * jax.random.uniform(keys[0], (3, num_modes), jnp.float32, 1.0, 3.0)
    phases = jax.random.uniform(keys[1], (3, num_modes), jnp.float32, 0.0, TWO_PI)
    mode_amp = 1.4 * jax.random.normal(keys[2], (CHANNELS, num_modes), jnp.float32)
    profiles = [jnp.cos(TWO_PI * jnp.arange(extent, dtype=jnp.float32)[None, :] / wave_len[axis][:, None] + phases[axis][:, None]) for axis, extent in enumerate((GRID_X, GRID_Y, GRID_Z))]
    field = jnp.einsum('cm,mx,my,mz->cxyz', mode_amp, profiles[0], profiles[1], profiles[2])
    noise = jax.random.normal(keys[3], field.shape, jnp.float32)
    return field + 0.3 * noise


def setup_inputs(seed: int = 0, part: int = 0) -> dict:
    base_key = jax.random.key(seed)
    shared_key, part_root = jax.random.split(base_key)
    vol_key, cot_key = jax.random.split(jax.random.fold_in(part_root, part), 2)
    tap_key, mix_key, bias_key = jax.random.split(shared_key, 3)
    volume = smooth_field(vol_key).astype(jnp.bfloat16)
    cot_out = smooth_field(cot_key).astype(jnp.bfloat16)
    raw_taps = jax.random.uniform(tap_key, (LAYERS, 3, NUM_TAPS), jnp.float32, 0.5, 1.5)
    filter_taps = (raw_taps / jnp.sum(raw_taps, axis=-1, keepdims=True)).astype(jnp.bfloat16).astype(jnp.float32)
    w_mix = (jax.random.normal(mix_key, (LAYERS, CHANNELS, CHANNELS), jnp.float32) * CHANNELS ** -0.5).astype(jnp.bfloat16)
    b_mix = 0.5 * jax.random.normal(bias_key, (LAYERS, CHANNELS), jnp.float32)
    return {'volume': volume, 'cot_out': cot_out, 'filter_taps': filter_taps, 'w_mix': w_mix, 'b_mix': b_mix}


def filter_line(values, taps, axis):
    length = values.shape[axis]
    pad_widths = [(0, 0)] * values.ndim
    pad_widths[axis] = (HALF_TAPS, HALF_TAPS)
    padded = jnp.pad(values, pad_widths)
    total = jnp.zeros(values.shape, jnp.float32)
    for tap_idx in range(NUM_TAPS):
        total = total + taps[tap_idx] * lax.slice_in_dim(padded, tap_idx, tap_idx + length, axis=axis)
    return total


def filter_three(channel, taps3):
    first = filter_line(channel.astype(jnp.float32), taps3[0], 0).astype(jnp.bfloat16)
    second = filter_line(first.astype(jnp.float32), taps3[1], 1).astype(jnp.bfloat16)
    return filter_line(second.astype(jnp.float32), taps3[2], 2).astype(jnp.bfloat16)


def filter_three_back(channel, taps3):
    first = filter_line(channel.astype(jnp.float32), taps3[2][::-1], 2).astype(jnp.bfloat16)
    second = filter_line(first.astype(jnp.float32), taps3[1][::-1], 1).astype(jnp.bfloat16)
    return filter_line(second.astype(jnp.float32), taps3[0][::-1], 0)


def gelu_exact(pre_act):
    return jax.nn.gelu(pre_act, approximate=False)


def reference(volume, cot_out, filter_taps, w_mix, b_mix):
    def forward_layer(vol_cur, layer):
        taps3, w_layer, b_layer = layer
        filtered = lax.map(lambda channel: filter_three(channel, taps3), vol_cur)
        pre_act = jnp.einsum('cd,cxyz->dxyz', w_layer.astype(jnp.float32), filtered.astype(jnp.float32)) + b_layer[:, None, None, None]
        vol_next = (vol_cur.astype(jnp.float32) + gelu_exact(pre_act)).astype(jnp.bfloat16)
        return vol_next, filtered

    _, filtered_all = lax.scan(forward_layer, volume, (filter_taps, w_mix, b_mix))

    def backward_layer(grad_next, layer):
        taps3, w_layer, b_layer, filtered = layer
        pre_act = jnp.einsum('cd,cxyz->dxyz', w_layer.astype(jnp.float32), filtered.astype(jnp.float32)) + b_layer[:, None, None, None]
        _, pullback = jax.vjp(gelu_exact, pre_act)
        scaled = pullback(grad_next.astype(jnp.float32))[0]
        scaled_b = scaled.astype(jnp.bfloat16).astype(jnp.float32)
        grad_b = jnp.sum(scaled, axis=(1, 2, 3))
        grad_w = jnp.einsum('cxyz,dxyz->cd', filtered.astype(jnp.float32), scaled_b)
        mixed_back = jnp.einsum('cd,dxyz->cxyz', w_layer.astype(jnp.float32), scaled_b).astype(jnp.bfloat16)
        spread = lax.map(lambda channel: filter_three_back(channel, taps3), mixed_back)
        grad_prev = (grad_next.astype(jnp.float32) + spread).astype(jnp.bfloat16)
        return grad_prev, (grad_w, grad_b)

    grad_volume, (grad_w_mix, grad_bias) = lax.scan(backward_layer, cot_out, (filter_taps, w_mix, b_mix, filtered_all), reverse=True)
    return grad_volume, grad_w_mix, grad_bias
```

```python
import functools

import jax
import jax.numpy as jnp
from jax import lax
from jax.experimental import pallas as pl
from jax.experimental.pallas import tpu as pltpu
from jax.sharding import PartitionSpec as P

MESH = pl.DeviceIdType.MESH
PLANES = 2
LAG = 1
XLAG = 1
F32 = jnp.float32
BF16 = jnp.bfloat16
SQRT_HALF = 0.7071067811865476
INV_SQRT_2PI = 0.3989422804014327


def dot(a, b):
    return jnp.dot(a, b, preferred_element_type=F32)


def stage_list(num_layers):
    stages = []
    start = 0
    for layer in range(num_layers):
        stages.append(('fx', layer, start))
        stages.append(('fy', layer, start + LAG))
        stages.append(('fz', layer, start + 2 * LAG))
        start += 2 * LAG + (XLAG if layer + 1 < num_layers else 0)
    for layer in reversed(range(num_layers)):
        stages.append(('bs', layer, start))
        stages.append(('bz', layer, start + LAG))
        stages.append(('by', layer, start + 2 * LAG))
        stages.append(('bx', layer, start + 2 * LAG + XLAG))
        start += 2 * LAG + XLAG
    return stages, start


def kernel(sizes, vol, cot, taps, w, b, out, gw_out, gb_out,
           vols, a1, a2, a3, gp, grad, d3, d2, d1, sb, yh, zh, zs, gb_acc,
           mfy, mfyh, mfz, mfzh, mby, mbyh, mbz, mbzh, sel,
           in_sem, cot_sem, out_sem, ysend, yrecv, zsend, zrecv, xsend, xrecv):
    nx, ny, nz, num_layers, num_taps, by_len, bz_len = sizes
    half = (num_taps - 1) // 2
    planes = a1.shape[0]
    rows = by_len * bz_len
    edge_y = half * bz_len
    edge_z = half * by_len
    nt = planes // PLANES
    my_x, my_y, my_z = lax.axis_index('gx'), lax.axis_index('gy'), lax.axis_index('gz')
    y_lo, y_hi = my_y > 0, my_y < ny - 1
    z_lo, z_hi = my_z > 0, my_z < nz - 1
    y_prev, y_next = {'gy': jnp.maximum(my_y - 1, 0)}, {'gy': jnp.minimum(my_y + 1, ny - 1)}
    z_prev, z_next = {'gz': jnp.maximum(my_z - 1, 0)}, {'gz': jnp.minimum(my_z + 1, nz - 1)}
    x_peer = {'gx': 1 - my_x}

    def x_of(j):
        return my_x * j + (1 - my_x) * (planes - 1 - j)

    def in_copy(j):
        return pltpu.make_async_copy(vol.at[x_of(j)], vols.at[0, j + half], in_sem.at[j])

    def cot_copy(j):
        return pltpu.make_async_copy(cot.at[x_of(j)], grad.at[j], cot_sem.at[j])

    def start_in(j, carry):
        in_copy(j).start()
        cot_copy(j).start()
        return carry

    lax.fori_loop(0, planes, start_in, 0)

    barrier = pltpu.get_barrier_semaphore()
    pl.semaphore_signal(barrier, inc=1, device_id=x_peer, device_id_type=MESH)
    for has, device in ((y_lo, y_prev), (y_hi, y_next), (z_lo, z_prev), (z_hi, z_next)):
        @pl.when(has)
        def _():
            pl.semaphore_signal(barrier, inc=1, device_id=device, device_id_type=MESH)

    def iota(shape, axis):
        return lax.broadcasted_iota(jnp.int32, shape, axis)

    def banded(layer, axis, back, diff, step, inside):
        total = jnp.zeros(diff.shape, F32)
        for t in range(num_taps):
            tap = taps[(layer * 3 + axis) * num_taps + (num_taps - 1 - t if back else t)]
            total = jnp.where(diff == step * (t - half), tap, total)
        if inside is not None:
            total = jnp.where(inside, total, 0.0)
        return total.astype(BF16)

    def build_chunk(chunk, carry):
        size = 64
        base = pl.multiple_of(chunk * size, size)
        at = pl.ds(base, size)
        halo_cols = 2 * edge_y
        i_in, k_in = base + iota((size, rows), 0), iota((size, rows), 1)
        i_halo, k_halo = base + iota((size, halo_cols), 0), iota((size, halo_cols), 1)
        k_y = jnp.where(k_halo < edge_y, k_halo - edge_y, k_halo + rows - edge_y)
        side = k_halo // edge_z
        hop = (k_halo % edge_z) // by_len
        zin = jnp.where(side == 0, hop - half, hop + bz_len)
        same_y = k_halo % by_len == i_halo // bz_len
        same_row = k_in // bz_len == i_in // bz_len
        for layer in range(num_layers):
            mfy[layer, at, :] = banded(layer, 1, False, k_in - i_in, bz_len, None)
            mby[layer, at, :] = banded(layer, 1, True, k_in - i_in, bz_len, None)
            mfyh[layer, at, :] = banded(layer, 1, False, k_y - i_halo, bz_len, None)
            mbyh[layer, at, :] = banded(layer, 1, True, k_y - i_halo, bz_len, None)
            mfz[layer, at, :] = banded(layer, 2, False, k_in - i_in, 1, same_row)
            mbz[layer, at, :] = banded(layer, 2, True, k_in - i_in, 1, same_row)
            mfzh[layer, at, :] = banded(layer, 2, False, zin - i_halo % bz_len, 1, same_y)
            mbzh[layer, at, :] = banded(layer, 2, True, zin - i_halo % bz_len, 1, same_y)
        return carry

    lax.fori_loop(0, rows // 64, build_chunk, 0)
    q, k_in = iota((2 * edge_z, rows), 0), iota((2 * edge_z, rows), 1)
    i_edge = (q % by_len) * bz_len + (q % edge_z) // by_len + (q // edge_z) * (bz_len - half)
    sel[...] = jnp.where(k_in == i_edge, 1.0, 0.0).astype(BF16)
    q, k_halo = iota((2 * edge_z, 2 * edge_y), 0), iota((2 * edge_z, 2 * edge_y), 1)
    i_edge_h = (q % by_len) * bz_len + (q % edge_z) // by_len + (q // edge_z) * (bz_len - half)
    k_y = jnp.where(k_halo < edge_y, k_halo - edge_y, k_halo + rows - edge_y)
    for layer in range(num_layers):
        mfy[layer, rows:, :] = banded(layer, 1, False, k_in - i_edge, bz_len, None)
        mfyh[layer, rows:, :] = banded(layer, 1, False, k_y - i_edge_h, bz_len, None)

    for layer in range(num_layers):
        vols[layer, planes + half:] = jnp.zeros((half,) + vols.shape[2:], BF16)
        d1[layer, planes + half:] = jnp.zeros((half,) + d1.shape[2:], BF16)

    def zero_halo(halo, where, side, edge):
        @pl.when(where)
        def _():
            def clear(j, carry):
                for stage in range(2 * num_layers):
                    halo[stage, j, side * edge:(side + 1) * edge] = jnp.zeros((edge, halo.shape[3]), BF16)
                return carry
            lax.fori_loop(0, planes, clear, 0)

    zero_halo(yh, my_y == 0, 0, edge_y)
    zero_halo(yh, my_y == ny - 1, 1, edge_y)
    zero_halo(zh, my_z == 0, 0, edge_z)
    zero_halo(zh, my_z == nz - 1, 1, edge_z)
    gw_out[...] = jnp.zeros(gw_out.shape, F32)
    gb_acc[...] = jnp.zeros(gb_acc.shape, F32)

    pl.semaphore_wait(barrier, 1 + y_lo.astype(jnp.int32) + y_hi.astype(jnp.int32) + z_lo.astype(jnp.int32) + z_hi.astype(jnp.int32))

    def y_copies(src, stage, tau):
        at = pl.ds(tau * PLANES, PLANES)
        up = pltpu.make_async_remote_copy(
            src_ref=src.at[at, pl.ds(rows - edge_y, edge_y)], dst_ref=yh.at[stage, at, pl.ds(0, edge_y)],
            send_sem=ysend.at[stage, tau, 0], recv_sem=yrecv.at[stage, tau, 0], device_id=y_next, device_id_type=MESH)
        dn = pltpu.make_async_remote_copy(
            src_ref=src.at[at, pl.ds(0, edge_y)], dst_ref=yh.at[stage, at, pl.ds(edge_y, edge_y)],
            send_sem=ysend.at[stage, tau, 1], recv_sem=yrecv.at[stage, tau, 1], device_id=y_prev, device_id_type=MESH)
        return up, dn, y_lo, y_hi

    def z_copies(stage, tau):
        at = pl.ds(tau * PLANES, PLANES)
        up = pltpu.make_async_remote_copy(
            src_ref=zs.at[stage, at, pl.ds(edge_z, edge_z)], dst_ref=zh.at[stage, at, pl.ds(0, edge_z)],
            send_sem=zsend.at[stage, tau, 0], recv_sem=zrecv.at[stage, tau, 0], device_id=z_next, device_id_type=MESH)
        dn = pltpu.make_async_remote_copy(
            src_ref=zs.at[stage, at, pl.ds(0, edge_z)], dst_ref=zh.at[stage, at, pl.ds(edge_z, edge_z)],
            send_sem=zsend.at[stage, tau, 1], recv_sem=zrecv.at[stage, tau, 1], device_id=z_prev, device_id_type=MESH)
        return up, dn, z_lo, z_hi

    def start(copies):
        up, dn, has_lo, has_hi = copies
        pl.when(has_hi)(up.start)
        pl.when(has_lo)(dn.start)

    def wait(copies):
        up, dn, has_lo, has_hi = copies

        @pl.when(has_hi)
        def _():
            up.wait_send()
            dn.wait_recv()

        @pl.when(has_lo)
        def _():
            dn.wait_send()
            up.wait_recv()

    def x_copy(buf, stage, layer, j):
        src = vol.at[x_of(j)] if stage == 0 else buf.at[layer, half + j]
        return pltpu.make_async_remote_copy(
            src_ref=src, dst_ref=buf.at[layer, half - 1 - j],
            send_sem=xsend.at[stage, j], recv_sem=xrecv.at[stage, j], device_id=x_peer, device_id_type=MESH)

    def start_x(buf, stage, layer, tau):
        for task in range(-(-half // PLANES)):
            @pl.when(tau == task)
            def _():
                for j in range(task * PLANES, min(half, (task + 1) * PLANES)):
                    x_copy(buf, stage, layer, j).start()

    def wait_x(buf, stage, layer, tau):
        @pl.when(tau == 0)
        def _():
            for j in range(half):
                x_copy(buf, stage, layer, j).wait()

    for j in range(half):
        x_copy(vols, 0, 0, j).start()

    def wait_in(j, carry):
        in_copy(j).wait()
        return carry

    lax.fori_loop(0, planes, wait_in, 0)

    def x_tap(layer, back, u):
        base = layer * 3 * num_taps
        plain, flipped = taps[base + u], taps[base + num_taps - 1 - u]
        return jnp.where(my_x == 1, flipped, plain) if back else jnp.where(my_x == 1, plain, flipped)

    def x_pass(buf, layer, back, tau, emit):
        weights = [x_tap(layer, back, u) for u in range(num_taps)]
        size = 16

        def body(chunk, carry):
            at = pl.ds(pl.multiple_of(chunk * size, size), size)
            loaded = [buf[layer, tau * PLANES + p, at, :].astype(F32) for p in range(PLANES + num_taps - 1)]
            for p in range(PLANES):
                total = weights[0] * loaded[p]
                for u in range(1, num_taps):
                    total = total + weights[u] * loaded[p + u]
                emit(tau * PLANES + p, at, total)
            return carry

        lax.fori_loop(0, rows // size, body, 0, unroll=2)

    def fx(layer, tau):
        wait_x(vols, layer, layer, tau)

        def emit(j, at, total):
            a1[j, at, :] = total.astype(BF16)

        x_pass(vols, layer, False, tau, emit)
        start(y_copies(a1, layer, tau))

    def fy(layer, tau):
        wait(y_copies(a1, layer, tau))
        for p in range(PLANES):
            j = tau * PLANES + p
            total = dot(mfy[layer], a1[j]) + dot(mfyh[layer], yh[layer, j])
            a2[j] = total[:rows].astype(BF16)
            zs[layer, j] = total[rows:].astype(BF16)
        start(z_copies(layer, tau))

    def fz(layer, tau):
        wait(z_copies(layer, tau))
        for p in range(PLANES):
            j = tau * PLANES + p
            total = dot(mfz[layer], a2[j]) + dot(mfzh[layer], zh[layer, j])
            filtered = total.astype(BF16)
            a3[layer, j] = filtered
            gp[layer, j] = dot(filtered, w[layer]) + b[layer, :][None, :]
        size = 16

        def body(chunk, carry):
            at = pl.ds(pl.multiple_of(chunk * size, size), size)
            for p in range(PLANES):
                j = tau * PLANES + p
                z = gp[layer, j, at, :]
                cdf = 0.5 * (1.0 + lax.erf(z * SQRT_HALF))
                gp[layer, j, at, :] = cdf + z * (jnp.exp(-0.5 * (z * z)) * INV_SQRT_2PI)
                if layer + 1 < num_layers:
                    vols[layer + 1, j + half, at, :] = (vols[layer, j + half, at, :].astype(F32) + z * cdf).astype(BF16)
            return carry

        lax.fori_loop(0, rows // size, body, 0, unroll=2)
        if layer + 1 < num_layers:
            start_x(vols, layer + 1, layer + 1, tau)

    def bs(layer, tau):
        stage = num_layers + layer
        if layer == num_layers - 1:
            for p in range(PLANES):
                cot_copy(tau * PLANES + p).wait()
        size = 16

        def body(chunk, acc):
            at = pl.ds(pl.multiple_of(chunk * size, size), size)
            for p in range(PLANES):
                j = tau * PLANES + p
                scaled = gp[layer, j, at, :] * grad[j, at, :].astype(F32)
                sb[p, at, :] = scaled.astype(BF16)
                acc = acc + scaled[:8] + scaled[8:]
            return acc

        gb_acc[layer] = lax.fori_loop(0, rows // size, body, gb_acc[layer], unroll=2)
        for p in range(PLANES):
            j = tau * PLANES + p
            mixed = lax.dot_general(sb[p], w[layer], (((1,), (1,)), ((), ())), preferred_element_type=F32).astype(BF16)
            d3[j] = mixed
            zs[stage, j] = dot(sel[...], mixed).astype(BF16)
        start(z_copies(stage, tau))
        for p in range(PLANES):
            j = tau * PLANES + p
            gw_out[layer] += lax.dot_general(a3[layer, j], sb[p], (((0,), (0,)), ((), ())), preferred_element_type=F32)

    def bz(layer, tau):
        stage = num_layers + layer
        wait(z_copies(stage, tau))
        for p in range(PLANES):
            j = tau * PLANES + p
            d2[j] = (dot(mbz[layer], d3[j]) + dot(mbzh[layer], zh[stage, j])).astype(BF16)
        start(y_copies(d2, stage, tau))

    def by(layer, tau):
        stage = num_layers + layer
        wait(y_copies(d2, stage, tau))
        for p in range(PLANES):
            j = tau * PLANES + p
            d1[layer, j + half] = (dot(mby[layer], d2[j]) + dot(mbyh[layer], yh[stage, j])).astype(BF16)
        start_x(d1, stage, layer, tau)

    def out_copy(j):
        return pltpu.make_async_copy(grad.at[j], out.at[x_of(j)], out_sem.at[j])

    def bx(layer, tau):
        wait_x(d1, num_layers + layer, layer, tau)

        def emit(j, at, total):
            grad[j, at, :] = (grad[j, at, :].astype(F32) + total).astype(BF16)

        x_pass(d1, layer, True, tau, emit)
        if layer == 0:
            for p in range(PLANES):
                out_copy(tau * PLANES + p).start()

    tasks = {'fx': fx, 'fy': fy, 'fz': fz, 'bs': bs, 'bz': bz, 'by': by, 'bx': bx}
    stages, last = stage_list(num_layers)

    def step(s, carry):
        for kind, layer, first in stages:
            tau = s - first

            @pl.when((tau >= 0) & (tau < nt))
            def _():
                tasks[kind](layer, tau)
        return carry

    lax.fori_loop(0, last + nt, step, 0)
    gb_out[...] = jnp.sum(gb_acc[...], axis=1)

    def wait_out(j, carry):
        out_copy(j).wait()
        return carry

    lax.fori_loop(0, planes, wait_out, 0)


def solution(mesh):
    names = ('gx', 'gy', 'gz')
    nx, ny, nz = (mesh.shape[axis_name] for axis_name in names)
    assert nx == 2
    vol_spec = P('dp', 'gx', 'gy', 'gz')

    def local_step(volume, cot_out, filter_taps, w_mix, b_mix):
        channels, planes, by_len, bz_len = volume.shape
        num_layers, _, num_taps = filter_taps.shape
        half = (num_taps - 1) // 2
        rows = by_len * bz_len
        edge_y, edge_z = half * bz_len, half * by_len
        nt = planes // PLANES
        stages = 2 * num_layers

        def to_rows(block):
            return jnp.transpose(block, (1, 2, 3, 0)).reshape(planes, rows, channels)

        any_spec = pl.BlockSpec(memory_space=pl.ANY)
        vmem_spec = pl.BlockSpec(memory_space=pltpu.VMEM)
        smem_spec = pl.BlockSpec(memory_space=pltpu.SMEM)
        block = (planes, rows, channels)
        dma = pltpu.SemaphoreType.DMA
        grad_rows, grad_w, grad_b = pl.pallas_call(
            functools.partial(kernel, (nx, ny, nz, num_layers, num_taps, by_len, bz_len)),
            out_shape=(
                jax.ShapeDtypeStruct(block, BF16),
                jax.ShapeDtypeStruct((num_layers, channels, channels), F32),
                jax.ShapeDtypeStruct((num_layers, channels), F32),
            ),
            in_specs=[any_spec, any_spec, smem_spec, vmem_spec, vmem_spec],
            out_specs=(any_spec, vmem_spec, vmem_spec),
            scratch_shapes=[
                pltpu.VMEM((num_layers, planes + 2 * half, rows, channels), BF16),
                pltpu.VMEM(block, BF16),
                pltpu.VMEM(block, BF16),
                pltpu.VMEM((num_layers,) + block, BF16),
                pltpu.VMEM((num_layers,) + block, F32),
                pltpu.VMEM(block, BF16),
                pltpu.VMEM(block, BF16),
                pltpu.VMEM(block, BF16),
                pltpu.VMEM((num_layers, planes + 2 * half, rows, channels), BF16),
                pltpu.VMEM((PLANES, rows, channels), BF16),
                pltpu.VMEM((stages, planes, 2 * edge_y, channels), BF16),
                pltpu.VMEM((stages, planes, 2 * edge_z, channels), BF16),
                pltpu.VMEM((stages, planes, 2 * edge_z, channels), BF16),
                pltpu.VMEM((num_layers, 8, channels), F32),
                pltpu.VMEM((num_layers, rows + 2 * edge_z, rows), BF16),
                pltpu.VMEM((num_layers, rows + 2 * edge_z, 2 * edge_y), BF16),
                pltpu.VMEM((num_layers, rows, rows), BF16),
                pltpu.VMEM((num_layers, rows, 2 * edge_z), BF16),
                pltpu.VMEM((num_layers, rows, rows), BF16),
                pltpu.VMEM((num_layers, rows, 2 * edge_y), BF16),
                pltpu.VMEM((num_layers, rows, rows), BF16),
                pltpu.VMEM((num_layers, rows, 2 * edge_z), BF16),
                pltpu.VMEM((2 * edge_z, rows), BF16),
                dma((planes,)), dma((planes,)), dma((planes,)),
                dma((stages, nt, 2)), dma((stages, nt, 2)), dma((stages, nt, 2)), dma((stages, nt, 2)),
                dma((stages, half)), dma((stages, half)),
            ],
            compiler_params=pltpu.CompilerParams(
                collective_id=0, has_side_effects=True, vmem_limit_bytes=64000 * 1024),
            name='stack',
        )(to_rows(volume), to_rows(cot_out), filter_taps.reshape(-1), w_mix, b_mix)
        grad_volume = jnp.transpose(grad_rows.reshape(planes, by_len, bz_len, channels), (3, 0, 1, 2))
        grad_w_sum = lax.psum(grad_w, names)
        grad_b_sum = lax.psum(grad_b, names)
        return grad_volume, grad_w_sum, grad_b_sum

    return jax.shard_map(local_step, mesh=mesh, in_specs=(vol_spec, vol_spec, P(), P(), P()), out_specs=(vol_spec, P('dp'), P('dp')), check_vma=False)
```

```python
import functools

import jax
import jax.numpy as jnp
from jax import lax
from jax.experimental import pallas as pl
from jax.experimental.pallas import tpu as pltpu
from jax.sharding import PartitionSpec as P

MESH = pl.DeviceIdType.MESH
PLANES = 2
LAG = 1
XLAG = 1
F32 = jnp.float32
BF16 = jnp.bfloat16
SQRT_HALF = 0.7071067811865476
INV_SQRT_2PI = 0.3989422804014327


def dot(a, b):
    return jnp.dot(a, b, preferred_element_type=F32)


def stage_list(num_layers, nt):
    stages = []
    start = 0
    for layer in range(num_layers):
        stages.append(('fx', layer, start))
        stages.append(('fy', layer, start + LAG))
        stages.append(('fz', layer, start + 2 * LAG))
        start += 2 * LAG + (XLAG if layer + 1 < num_layers else 0)
    for layer in reversed(range(num_layers)):
        stages.append(('bs', layer, start))
        stages.append(('bz', layer, start + LAG))
        stages.append(('by', layer, start + 2 * LAG))
        stages.append(('bx', layer, start + 2 * LAG + XLAG))
        start += 2 * LAG + XLAG
    for kind, layer, first in list(stages):
        if kind == 'bs':
            stages += [('r%d' % phase, layer, first + nt - 1 + phase) for phase in range(7)]
    return stages, max(first + (1 if kind[0] == 'r' else nt) for kind, _, first in stages)


def kernel(sizes, vol, cot, taps, w, b, out, gw_out, gb_out,
           vols, a1, a2, a3, gp, grad, d3, d2, d1, sb, yh, zh, zs,
           mfy, mfyh, mfz, mfzh, mby, mbyh, mbz, mbzh, sel,
           gwx, rx, ry, rz, sum_send, sum_recv,
           in_sem, cot_sem, out_sem, ysend, yrecv, zsend, zrecv, xsend, xrecv):
    nx, ny, nz, num_layers, num_taps, by_len, bz_len = sizes
    half = (num_taps - 1) // 2
    planes = a1.shape[0]
    rows = by_len * bz_len
    edge_y = half * bz_len
    edge_z = half * by_len
    nt = planes // PLANES
    part_x = w.shape[1] // nx
    part_y = part_x // ny
    part_z = part_y // nz
    my_x, my_y, my_z = lax.axis_index('gx'), lax.axis_index('gy'), lax.axis_index('gz')
    y_lo, y_hi = my_y > 0, my_y < ny - 1
    z_lo, z_hi = my_z > 0, my_z < nz - 1
    y_prev, y_next = {'gy': jnp.maximum(my_y - 1, 0)}, {'gy': jnp.minimum(my_y + 1, ny - 1)}
    z_prev, z_next = {'gz': jnp.maximum(my_z - 1, 0)}, {'gz': jnp.minimum(my_z + 1, nz - 1)}
    x_peer = {'gx': 1 - my_x}

    def x_of(j):
        return my_x * j + (1 - my_x) * (planes - 1 - j)

    def in_copy(j):
        return pltpu.make_async_copy(vol.at[x_of(j)], vols.at[0, j + half], in_sem.at[j])

    def cot_copy(j):
        return pltpu.make_async_copy(cot.at[x_of(j)], grad.at[j], cot_sem.at[j])

    def start_in(j, carry):
        in_copy(j).start()
        cot_copy(j).start()
        return carry

    lax.fori_loop(0, planes, start_in, 0)

    barrier = pltpu.get_barrier_semaphore()
    pl.semaphore_signal(barrier, inc=1, device_id=x_peer, device_id_type=MESH)
    for offset in range(1, ny):
        pl.semaphore_signal(barrier, inc=1, device_id={'gy': lax.rem(my_y + offset, ny)}, device_id_type=MESH)
    for offset in range(1, nz):
        pl.semaphore_signal(barrier, inc=1, device_id={'gz': lax.rem(my_z + offset, nz)}, device_id_type=MESH)

    def iota(shape, axis):
        return lax.broadcasted_iota(jnp.int32, shape, axis)

    def banded(layer, axis, back, diff, step, inside):
        total = jnp.zeros(diff.shape, F32)
        for t in range(num_taps):
            tap = taps[(layer * 3 + axis) * num_taps + (num_taps - 1 - t if back else t)]
            total = jnp.where(diff == step * (t - half), tap, total)
        if inside is not None:
            total = jnp.where(inside, total, 0.0)
        return total.astype(BF16)

    def build_chunk(chunk, carry):
        size = 64
        base = pl.multiple_of(chunk * size, size)
        at = pl.ds(base, size)
        halo_cols = 2 * edge_y
        i_in, k_in = base + iota((size, rows), 0), iota((size, rows), 1)
        i_halo, k_halo = base + iota((size, halo_cols), 0), iota((size, halo_cols), 1)
        k_y = jnp.where(k_halo < edge_y, k_halo - edge_y, k_halo + rows - edge_y)
        side = k_halo // edge_z
        hop = (k_halo % edge_z) // by_len
        zin = jnp.where(side == 0, hop - half, hop + bz_len)
        same_y = k_halo % by_len == i_halo // bz_len
        same_row = k_in // bz_len == i_in // bz_len
        for layer in range(num_layers):
            mfy[layer, at, :] = banded(layer, 1, False, k_in - i_in, bz_len, None)
            mby[layer, at, :] = banded(layer, 1, True, k_in - i_in, bz_len, None)
            mfyh[layer, at, :] = banded(layer, 1, False, k_y - i_halo, bz_len, None)
            mbyh[layer, at, :] = banded(layer, 1, True, k_y - i_halo, bz_len, None)
            mfz[layer, at, :] = banded(layer, 2, False, k_in - i_in, 1, same_row)
            mbz[layer, at, :] = banded(layer, 2, True, k_in - i_in, 1, same_row)
            mfzh[layer, at, :] = banded(layer, 2, False, zin - i_halo % bz_len, 1, same_y)
            mbzh[layer, at, :] = banded(layer, 2, True, zin - i_halo % bz_len, 1, same_y)
        return carry

    lax.fori_loop(0, rows // 64, build_chunk, 0)
    q, k_in = iota((2 * edge_z, rows), 0), iota((2 * edge_z, rows), 1)
    i_edge = (q % by_len) * bz_len + (q % edge_z) // by_len + (q // edge_z) * (bz_len - half)
    sel[...] = jnp.where(k_in == i_edge, 1.0, 0.0).astype(BF16)
    q, k_halo = iota((2 * edge_z, 2 * edge_y), 0), iota((2 * edge_z, 2 * edge_y), 1)
    i_edge_h = (q % by_len) * bz_len + (q % edge_z) // by_len + (q // edge_z) * (bz_len - half)
    k_y = jnp.where(k_halo < edge_y, k_halo - edge_y, k_halo + rows - edge_y)
    for layer in range(num_layers):
        mfy[layer, rows:, :] = banded(layer, 1, False, k_in - i_edge, bz_len, None)
        mfyh[layer, rows:, :] = banded(layer, 1, False, k_y - i_edge_h, bz_len, None)

    for layer in range(num_layers):
        vols[layer, planes + half:] = jnp.zeros((half,) + vols.shape[2:], BF16)
        d1[layer, planes + half:] = jnp.zeros((half,) + d1.shape[2:], BF16)

    def zero_halo(halo, where, side, edge):
        @pl.when(where)
        def _():
            def clear(j, carry):
                for stage in range(2 * num_layers):
                    halo[stage, j, side * edge:(side + 1) * edge] = jnp.zeros((edge, halo.shape[3]), BF16)
                return carry
            lax.fori_loop(0, planes, clear, 0)

    zero_halo(yh, my_y == 0, 0, edge_y)
    zero_halo(yh, my_y == ny - 1, 1, edge_y)
    zero_halo(zh, my_z == 0, 0, edge_z)
    zero_halo(zh, my_z == nz - 1, 1, edge_z)
    gwx[...] = jnp.zeros(gwx.shape, F32)

    pl.semaphore_wait(barrier, 1 + (ny - 1) + (nz - 1))

    def y_copies(src, stage, tau):
        at = pl.ds(tau * PLANES, PLANES)
        up = pltpu.make_async_remote_copy(
            src_ref=src.at[at, pl.ds(rows - edge_y, edge_y)], dst_ref=yh.at[stage, at, pl.ds(0, edge_y)],
            send_sem=ysend.at[stage, tau, 0], recv_sem=yrecv.at[stage, tau, 0], device_id=y_next, device_id_type=MESH)
        dn = pltpu.make_async_remote_copy(
            src_ref=src.at[at, pl.ds(0, edge_y)], dst_ref=yh.at[stage, at, pl.ds(edge_y, edge_y)],
            send_sem=ysend.at[stage, tau, 1], recv_sem=yrecv.at[stage, tau, 1], device_id=y_prev, device_id_type=MESH)
        return up, dn, y_lo, y_hi

    def z_copies(stage, tau):
        at = pl.ds(tau * PLANES, PLANES)
        up = pltpu.make_async_remote_copy(
            src_ref=zs.at[stage, at, pl.ds(edge_z, edge_z)], dst_ref=zh.at[stage, at, pl.ds(0, edge_z)],
            send_sem=zsend.at[stage, tau, 0], recv_sem=zrecv.at[stage, tau, 0], device_id=z_next, device_id_type=MESH)
        dn = pltpu.make_async_remote_copy(
            src_ref=zs.at[stage, at, pl.ds(0, edge_z)], dst_ref=zh.at[stage, at, pl.ds(edge_z, edge_z)],
            send_sem=zsend.at[stage, tau, 1], recv_sem=zrecv.at[stage, tau, 1], device_id=z_prev, device_id_type=MESH)
        return up, dn, z_lo, z_hi

    def start(copies):
        up, dn, has_lo, has_hi = copies
        pl.when(has_hi)(up.start)
        pl.when(has_lo)(dn.start)

    def wait(copies):
        up, dn, has_lo, has_hi = copies

        @pl.when(has_hi)
        def _():
            up.wait_send()
            dn.wait_recv()

        @pl.when(has_lo)
        def _():
            dn.wait_send()
            up.wait_recv()

    def x_copy(buf, stage, layer, j):
        src = vol.at[x_of(j)] if stage == 0 else buf.at[layer, half + j]
        return pltpu.make_async_remote_copy(
            src_ref=src, dst_ref=buf.at[layer, half - 1 - j],
            send_sem=xsend.at[stage, j], recv_sem=xrecv.at[stage, j], device_id=x_peer, device_id_type=MESH)

    def start_x(buf, stage, layer, tau):
        for task in range(-(-half // PLANES)):
            @pl.when(tau == task)
            def _():
                for j in range(task * PLANES, min(half, (task + 1) * PLANES)):
                    x_copy(buf, stage, layer, j).start()

    def wait_x(buf, stage, layer, tau):
        @pl.when(tau == 0)
        def _():
            for j in range(half):
                x_copy(buf, stage, layer, j).wait()

    for j in range(half):
        x_copy(vols, 0, 0, j).start()

    def wait_in(j, carry):
        in_copy(j).wait()
        return carry

    lax.fori_loop(0, planes, wait_in, 0)

    def x_tap(layer, back, u):
        base = layer * 3 * num_taps
        plain, flipped = taps[base + u], taps[base + num_taps - 1 - u]
        return jnp.where(my_x == 1, flipped, plain) if back else jnp.where(my_x == 1, plain, flipped)

    def x_pass(buf, layer, back, tau, emit):
        weights = [x_tap(layer, back, u) for u in range(num_taps)]
        size = 16

        def body(chunk, carry):
            at = pl.ds(pl.multiple_of(chunk * size, size), size)
            loaded = [buf[layer, tau * PLANES + p, at, :].astype(F32) for p in range(PLANES + num_taps - 1)]
            for p in range(PLANES):
                total = weights[0] * loaded[p]
                for u in range(1, num_taps):
                    total = total + weights[u] * loaded[p + u]
                emit(tau * PLANES + p, at, total)
            return carry

        lax.fori_loop(0, rows // size, body, 0, unroll=2)

    def fx(layer, tau):
        wait_x(vols, layer, layer, tau)

        def emit(j, at, total):
            a1[j, at, :] = total.astype(BF16)

        x_pass(vols, layer, False, tau, emit)
        start(y_copies(a1, layer, tau))

    def fy(layer, tau):
        wait(y_copies(a1, layer, tau))
        for p in range(PLANES):
            j = tau * PLANES + p
            total = dot(mfy[layer], a1[j]) + dot(mfyh[layer], yh[layer, j])
            a2[j] = total[:rows].astype(BF16)
            zs[layer, j] = total[rows:].astype(BF16)
        start(z_copies(layer, tau))

    def fz(layer, tau):
        wait(z_copies(layer, tau))
        for p in range(PLANES):
            j = tau * PLANES + p
            total = dot(mfz[layer], a2[j]) + dot(mfzh[layer], zh[layer, j])
            filtered = total.astype(BF16)
            a3[layer, j] = filtered
            gp[layer, j] = dot(filtered, w[layer]) + b[layer, :][None, :]
        size = 16

        def body(chunk, carry):
            at = pl.ds(pl.multiple_of(chunk * size, size), size)
            for p in range(PLANES):
                j = tau * PLANES + p
                z = gp[layer, j, at, :]
                cdf = 0.5 * (1.0 + lax.erf(z * SQRT_HALF))
                gp[layer, j, at, :] = cdf + z * (jnp.exp(-0.5 * (z * z)) * INV_SQRT_2PI)
                if layer + 1 < num_layers:
                    vols[layer + 1, j + half, at, :] = (vols[layer, j + half, at, :].astype(F32) + z * cdf).astype(BF16)
            return carry

        lax.fori_loop(0, rows // size, body, 0, unroll=2)
        if layer + 1 < num_layers:
            start_x(vols, layer + 1, layer + 1, tau)

    def bs(layer, tau):
        stage = num_layers + layer
        if layer == num_layers - 1:
            for p in range(PLANES):
                cot_copy(tau * PLANES + p).wait()
        size = 16

        def body(chunk, acc):
            at = pl.ds(pl.multiple_of(chunk * size, size), size)
            for p in range(PLANES):
                j = tau * PLANES + p
                scaled = gp[layer, j, at, :] * grad[j, at, :].astype(F32)
                sb[p, at, :] = scaled.astype(BF16)
                acc = acc + scaled[:8] + scaled[8:]
            return acc

        gwx[layer, 0, part_x:] = lax.fori_loop(0, rows // size, body, gwx[layer, 0, part_x:], unroll=2)
        for p in range(PLANES):
            j = tau * PLANES + p
            mixed = lax.dot_general(sb[p], w[layer], (((1,), (1,)), ((), ())), preferred_element_type=F32).astype(BF16)
            d3[j] = mixed
            zs[stage, j] = dot(sel[...], mixed).astype(BF16)
        start(z_copies(stage, tau))
        channels = w.shape[1]
        product = lax.dot_general(
            a3[layer, pl.ds(tau * PLANES, PLANES)].reshape(PLANES * rows, channels), sb[...].reshape(PLANES * rows, channels),
            (((0,), (0,)), ((), ())), preferred_element_type=F32)
        for side in range(nx):
            gwx[layer, side, :part_x] += product[side * part_x:(side + 1) * part_x]

    def bz(layer, tau):
        stage = num_layers + layer
        wait(z_copies(stage, tau))
        for p in range(PLANES):
            j = tau * PLANES + p
            d2[j] = (dot(mbz[layer], d3[j]) + dot(mbzh[layer], zh[stage, j])).astype(BF16)
        start(y_copies(d2, stage, tau))

    def by(layer, tau):
        stage = num_layers + layer
        wait(y_copies(d2, stage, tau))
        for p in range(PLANES):
            j = tau * PLANES + p
            d1[layer, j + half] = (dot(mby[layer], d2[j]) + dot(mbyh[layer], yh[stage, j])).astype(BF16)
        start_x(d1, stage, layer, tau)

    def out_copy(j):
        return pltpu.make_async_copy(grad.at[j], out.at[x_of(j)], out_sem.at[j])

    def bx(layer, tau):
        wait_x(d1, num_layers + layer, layer, tau)

        def emit(j, at, total):
            grad[j, at, :] = (grad[j, at, :].astype(F32) + total).astype(BF16)

        x_pass(d1, layer, True, tau, emit)
        if layer == 0:
            for p in range(PLANES):
                out_copy(tau * PLANES + p).start()

    def sum_copy(layer, phase, offset, src, dst, device):
        return pltpu.make_async_remote_copy(
            src_ref=src, dst_ref=dst, send_sem=sum_send.at[layer, phase, offset], recv_sem=sum_recv.at[layer, phase, offset],
            device_id=device, device_id_type=MESH)

    def phase_copies(layer, phase):
        base_x = my_x * part_x
        base_y = base_x + my_y * part_y
        base_z = base_y + my_z * part_z
        if phase == 0:
            return [sum_copy(layer, 0, 0, gwx.at[layer, 1 - my_x], rx.at[layer], x_peer)]
        if phase == 5:
            at = pl.ds(pl.multiple_of(base_x, part_x), part_x)
            return [sum_copy(layer, 5, 0, gw_out.at[layer, at], gw_out.at[layer, at], x_peer)]
        copies = []
        along_y = phase in (1, 4)
        count, me, name = (ny, my_y, 'gy') if along_y else (nz, my_z, 'gz')
        for offset in range(1, count):
            other = lax.rem(me + offset, count)
            if phase == 1:
                src, dst = ry.at[layer, 1, other], ry.at[layer, 0, me]
            elif phase == 2:
                src, dst = rz.at[layer, 1, other], rz.at[layer, 0, me]
            else:
                at = pl.ds(pl.multiple_of(base_z, part_z), part_z) if phase == 3 else pl.ds(pl.multiple_of(base_y, part_y), part_y)
                src, dst = gw_out.at[layer, at], gw_out.at[layer, at]
            copies.append(sum_copy(layer, phase, offset - 1, src, dst, {name: other}))
        return copies

    def start_phase(layer, phase):
        for copy in phase_copies(layer, phase):
            copy.start()

    def wait_phase(layer, phase):
        for copy in phase_copies(layer, phase):
            copy.wait()

    def r0(layer, tau):
        gwx[layer, 1, part_x:] = gwx[layer, 0, part_x:]
        start_phase(layer, 0)

    def spread(total, count, part, slots, layer, me):
        bias = total[count * part:]
        for k in range(count):
            slots[layer, 1, k, :part] = total[k * part:(k + 1) * part]
            slots[layer, 1, k, part:] = bias
        slots[layer, 0, me] = slots[layer, 1, me]

    def r1(layer, tau):
        wait_phase(layer, 0)
        spread(gwx[layer, my_x] + rx[layer], ny, part_y, ry, layer, my_y)
        start_phase(layer, 1)

    def gathered(slots, layer, count):
        total = slots[layer, 0, 0]
        for k in range(1, count):
            total = total + slots[layer, 0, k]
        return total

    def r2(layer, tau):
        wait_phase(layer, 1)
        spread(gathered(ry, layer, ny), nz, part_z, rz, layer, my_z)
        start_phase(layer, 2)

    def r3(layer, tau):
        wait_phase(layer, 2)
        total = gathered(rz, layer, nz)
        gw_out[layer, pl.ds(pl.multiple_of(my_x * part_x + my_y * part_y + my_z * part_z, part_z), part_z)] = total[:part_z]
        gb_out[layer, :] = jnp.sum(total[part_z:], axis=0)
        start_phase(layer, 3)

    def r4(layer, tau):
        wait_phase(layer, 3)
        start_phase(layer, 4)

    def r5(layer, tau):
        wait_phase(layer, 4)
        start_phase(layer, 5)

    def r6(layer, tau):
        wait_phase(layer, 5)

    tasks = {'r0': r0, 'r1': r1, 'r2': r2, 'r3': r3, 'r4': r4, 'r5': r5, 'r6': r6, 'fx': fx, 'fy': fy, 'fz': fz, 'bs': bs, 'bz': bz, 'by': by, 'bx': bx}
    stages, last = stage_list(num_layers, nt)

    def step(s, carry):
        for kind, layer, first in stages:
            tau = s - first

            @pl.when((tau >= 0) & (tau < (1 if kind[0] == 'r' else nt)))
            def _():
                tasks[kind](layer, tau)
        return carry

    lax.fori_loop(0, last, step, 0)

    def wait_out(j, carry):
        out_copy(j).wait()
        return carry

    lax.fori_loop(0, planes, wait_out, 0)


def solution(mesh):
    names = ('gx', 'gy', 'gz')
    nx, ny, nz = (mesh.shape[axis_name] for axis_name in names)
    assert nx == 2
    vol_spec = P('dp', 'gx', 'gy', 'gz')

    def local_step(volume, cot_out, filter_taps, w_mix, b_mix):
        channels, planes, by_len, bz_len = volume.shape
        num_layers, _, num_taps = filter_taps.shape
        half = (num_taps - 1) // 2
        rows = by_len * bz_len
        edge_y, edge_z = half * bz_len, half * by_len
        nt = planes // PLANES
        stages = 2 * num_layers
        part_x = channels // nx
        part_y = part_x // ny
        part_z = part_y // nz

        def to_rows(block):
            return jnp.transpose(block, (1, 2, 3, 0)).reshape(planes, rows, channels)

        any_spec = pl.BlockSpec(memory_space=pl.ANY)
        vmem_spec = pl.BlockSpec(memory_space=pltpu.VMEM)
        smem_spec = pl.BlockSpec(memory_space=pltpu.SMEM)
        block = (planes, rows, channels)
        dma = pltpu.SemaphoreType.DMA
        grad_rows, grad_w, grad_b = pl.pallas_call(
            functools.partial(kernel, (nx, ny, nz, num_layers, num_taps, by_len, bz_len)),
            out_shape=(
                jax.ShapeDtypeStruct(block, BF16),
                jax.ShapeDtypeStruct((num_layers, channels, channels), F32),
                jax.ShapeDtypeStruct((num_layers, channels), F32),
            ),
            in_specs=[any_spec, any_spec, smem_spec, vmem_spec, vmem_spec],
            out_specs=(any_spec, vmem_spec, vmem_spec),
            scratch_shapes=[
                pltpu.VMEM((num_layers, planes + 2 * half, rows, channels), BF16),
                pltpu.VMEM(block, BF16),
                pltpu.VMEM(block, BF16),
                pltpu.VMEM((num_layers,) + block, BF16),
                pltpu.VMEM((num_layers,) + block, F32),
                pltpu.VMEM(block, BF16),
                pltpu.VMEM(block, BF16),
                pltpu.VMEM(block, BF16),
                pltpu.VMEM((num_layers, planes + 2 * half, rows, channels), BF16),
                pltpu.VMEM((PLANES, rows, channels), BF16),
                pltpu.VMEM((stages, planes, 2 * edge_y, channels), BF16),
                pltpu.VMEM((stages, planes, 2 * edge_z, channels), BF16),
                pltpu.VMEM((stages, planes, 2 * edge_z, channels), BF16),
                pltpu.VMEM((num_layers, rows + 2 * edge_z, rows), BF16),
                pltpu.VMEM((num_layers, rows + 2 * edge_z, 2 * edge_y), BF16),
                pltpu.VMEM((num_layers, rows, rows), BF16),
                pltpu.VMEM((num_layers, rows, 2 * edge_z), BF16),
                pltpu.VMEM((num_layers, rows, rows), BF16),
                pltpu.VMEM((num_layers, rows, 2 * edge_y), BF16),
                pltpu.VMEM((num_layers, rows, rows), BF16),
                pltpu.VMEM((num_layers, rows, 2 * edge_z), BF16),
                pltpu.VMEM((2 * edge_z, rows), BF16),
                pltpu.VMEM((num_layers, nx, part_x + 8, channels), F32),
                pltpu.VMEM((num_layers, part_x + 8, channels), F32),
                pltpu.VMEM((num_layers, 2, ny, part_y + 8, channels), F32),
                pltpu.VMEM((num_layers, 2, nz, part_z + 8, channels), F32),
                dma((num_layers, 6, max(ny, nz, 2) - 1)), dma((num_layers, 6, max(ny, nz, 2) - 1)),
                dma((planes,)), dma((planes,)), dma((planes,)),
                dma((stages, nt, 2)), dma((stages, nt, 2)), dma((stages, nt, 2)), dma((stages, nt, 2)),
                dma((stages, half)), dma((stages, half)),
            ],
            compiler_params=pltpu.CompilerParams(
                collective_id=0, has_side_effects=True, vmem_limit_bytes=64000 * 1024),
            name='stack',
        )(to_rows(volume), to_rows(cot_out), filter_taps.reshape(-1), w_mix, b_mix)
        grad_volume = jnp.transpose(grad_rows.reshape(planes, by_len, bz_len, channels), (3, 0, 1, 2))
        return grad_volume, grad_w, grad_b

    return jax.shard_map(local_step, mesh=mesh, in_specs=(vol_spec, vol_spec, P(), P(), P()), out_specs=(vol_spec, P('dp'), P('dp')), check_vma=False)
```

```python
import functools

import jax
import jax.numpy as jnp
from jax import lax
from jax.experimental import pallas as pl
from jax.experimental.pallas import tpu as pltpu
from jax.sharding import PartitionSpec as P

MESH = pl.DeviceIdType.MESH
PLANES = 2
LAG = 3
SUM_LAG = 2
XLAG = 1
F32 = jnp.float32
BF16 = jnp.bfloat16
SQRT_HALF = 0.7071067811865476
HALF_LOG2_E = 0.7213475204444817
CHUNK = 16
GROUP = 32
INV_SQRT_2PI = 0.3989422804014327


def dot(a, b):
    return jnp.dot(a, b, preferred_element_type=F32)


def stage_list(num_layers, nt):
    stages = []
    start = 0
    for layer in range(num_layers):
        stages.append(('fx', layer, start))
        stages.append(('fy', layer, start + LAG))
        stages.append(('fz', layer, start + 2 * LAG))
        start += 2 * LAG + (XLAG if layer + 1 < num_layers else 0)
    for layer in reversed(range(num_layers)):
        stages.append(('bs', layer, start))
        stages.append(('bz', layer, start + LAG))
        stages.append(('by', layer, start + 2 * LAG))
        stages.append(('bx', layer, start + 2 * LAG + XLAG))
        start += 2 * LAG + XLAG
    for kind, layer, first in list(stages):
        if kind == 'bs':
            stages += [('r%d' % phase, layer, first + nt - 1 + phase * (SUM_LAG if layer else 1)) for phase in range(7)]
    return stages, max(first + (1 if kind[0] == 'r' else nt) for kind, _, first in stages)


def kernel(sizes, vol, cot, taps, w, b, out, gw_out, gb_out,
           vols, a1, a2, a3, gp, grad, d3, d2, d1, sb, yh, zh, zs,
           mfx, mfy, mfz, mbx, mby, mbz, sel,
           gwx, rx, ry, rz, sum_send, sum_recv,
           in_sem, cot_sem, out_sem, ysend, yrecv, zsend, zrecv, xsend, xrecv):
    nx, ny, nz, num_layers, num_taps, by_len, bz_len = sizes
    half = (num_taps - 1) // 2
    planes = a1.shape[0]
    rows = by_len * bz_len
    edge_y = half * bz_len
    edge_z = half * by_len
    nt = planes // PLANES
    part_x = w.shape[1] // nx
    part_y = part_x // ny
    part_z = part_y // nz
    my_x, my_y, my_z = lax.axis_index('gx'), lax.axis_index('gy'), lax.axis_index('gz')
    y_lo, y_hi = my_y > 0, my_y < ny - 1
    z_lo, z_hi = my_z > 0, my_z < nz - 1
    y_prev, y_next = {'gy': jnp.maximum(my_y - 1, 0)}, {'gy': jnp.minimum(my_y + 1, ny - 1)}
    z_prev, z_next = {'gz': jnp.maximum(my_z - 1, 0)}, {'gz': jnp.minimum(my_z + 1, nz - 1)}
    x_peer = {'gx': 1 - my_x}

    def x_of(j):
        return my_x * j + (1 - my_x) * (planes - 1 - j)

    def in_copy(j):
        return pltpu.make_async_copy(vol.at[x_of(j)], vols.at[0, j + half], in_sem.at[j])

    def cot_copy(j):
        return pltpu.make_async_copy(cot.at[x_of(j)], grad.at[j], cot_sem.at[j])

    def start_in(j, carry):
        in_copy(j).start()
        cot_copy(j).start()
        return carry

    lax.fori_loop(0, planes, start_in, 0)

    barrier = pltpu.get_barrier_semaphore()
    pl.semaphore_signal(barrier, inc=1, device_id=x_peer, device_id_type=MESH)
    for offset in range(1, ny):
        pl.semaphore_signal(barrier, inc=1, device_id={'gy': lax.rem(my_y + offset, ny)}, device_id_type=MESH)
    for offset in range(1, nz):
        pl.semaphore_signal(barrier, inc=1, device_id={'gz': lax.rem(my_z + offset, nz)}, device_id_type=MESH)

    half_y, half_rows = by_len // 2, rows // 2

    def iota(shape, axis):
        return lax.broadcasted_iota(jnp.int32, shape, axis)

    def banded(layer, axis, back, hop, inside):
        total = jnp.zeros(hop.shape, F32)
        for t in range(num_taps):
            tap = taps[layer, axis, num_taps - 1 - t if back else t]
            if axis == 0:
                tap = jnp.where(my_x == 1, tap, taps[layer, axis, t if back else num_taps - 1 - t])
            total = jnp.where(hop == t, tap, total)
        return jnp.where(inside, total, 0.0).astype(BF16)

    def build(layer, carry):
        i, k = iota((PLANES * GROUP, (PLANES + 2 * half) * GROUP), 0), iota((PLANES * GROUP, (PLANES + 2 * half) * GROUP), 1)
        hop, inside = k // GROUP - i // GROUP, k % GROUP == i % GROUP
        mfx[layer] = banded(layer, 0, False, hop, inside)
        mbx[layer] = banded(layer, 0, True, hop, inside)
        i, k = iota((half_rows, half_rows + 2 * edge_y), 0), iota((half_rows, half_rows + 2 * edge_y), 1)
        hop, inside = k // bz_len - i // bz_len, k % bz_len == i % bz_len
        mfy[layer, :half_rows] = banded(layer, 1, False, hop, inside)
        mby[layer] = banded(layer, 1, True, hop, inside)
        i, k = iota((edge_z, half_rows + 2 * edge_y), 0), iota((edge_z, half_rows + 2 * edge_y), 1)
        z_edge = i // half_y % half + i // (half * half_y) * (bz_len - half)
        mfy[layer, half_rows:] = banded(layer, 1, False, k // bz_len - i % half_y, k % bz_len == z_edge)
        i, k = iota((half_rows, half_rows), 0), iota((half_rows, half_rows), 1)
        hop, inside = k % bz_len - i % bz_len + half, k // bz_len == i // bz_len
        mfz[layer, :, :half_rows] = banded(layer, 2, False, hop, inside)
        mbz[layer, :, :half_rows] = banded(layer, 2, True, hop, inside)
        i, k = iota((half_rows, edge_z), 0), iota((half_rows, edge_z), 1)
        hop = k // half_y % half + k // (half * half_y) * (bz_len + half) - i % bz_len
        inside = k % half_y == i // bz_len
        mfz[layer, :, half_rows:] = banded(layer, 2, False, hop, inside)
        mbz[layer, :, half_rows:] = banded(layer, 2, True, hop, inside)
        return carry

    lax.fori_loop(0, num_layers, build, 0)
    i, k = iota((edge_z, half_rows), 0), iota((edge_z, half_rows), 1)
    z_edge = i // half_y % half + i // (half * half_y) * (bz_len - half)
    sel[...] = jnp.where((k // bz_len == i % half_y) & (k % bz_len == z_edge), 1.0, 0.0).astype(BF16)

    for layer in range(num_layers):
        vols[layer, planes + half:] = jnp.zeros((half,) + vols.shape[2:], BF16)
        d1[layer, planes + half:] = jnp.zeros((half,) + d1.shape[2:], BF16)

    def zero_halo(halo, where, side):
        @pl.when(where)
        def _():
            def clear(j, carry):
                for stage in range(2 * num_layers):
                    halo[stage, j, :, side] = jnp.zeros(halo.shape[2:3] + halo.shape[4:], BF16)
                return carry
            lax.fori_loop(0, planes, clear, 0)

    zero_halo(yh, my_y == 0, 0)
    zero_halo(yh, my_y == ny - 1, 1)
    zero_halo(zh, my_z == 0, 0)
    zero_halo(zh, my_z == nz - 1, 1)
    gwx[...] = jnp.zeros(gwx.shape, F32)

    pl.semaphore_wait(barrier, 1 + (ny - 1) + (nz - 1))

    def y_copies(src, stage, tau):
        at = pl.ds(tau * PLANES, PLANES)
        up = pltpu.make_async_remote_copy(
            src_ref=src.at[at, pl.ds(rows - edge_y, edge_y)], dst_ref=yh.at[stage, at, 0, 0],
            send_sem=ysend.at[stage, tau, 0], recv_sem=yrecv.at[stage, tau, 0], device_id=y_next, device_id_type=MESH)
        dn = pltpu.make_async_remote_copy(
            src_ref=src.at[at, pl.ds(0, edge_y)], dst_ref=yh.at[stage, at, 0, 1],
            send_sem=ysend.at[stage, tau, 1], recv_sem=yrecv.at[stage, tau, 1], device_id=y_prev, device_id_type=MESH)
        return up, dn, y_lo, y_hi

    def z_copies(stage, tau):
        at = pl.ds(tau * PLANES, PLANES)
        up = pltpu.make_async_remote_copy(
            src_ref=zs.at[stage, at, :, 1], dst_ref=zh.at[stage, at, :, 0],
            send_sem=zsend.at[stage, tau, 0], recv_sem=zrecv.at[stage, tau, 0], device_id=z_next, device_id_type=MESH)
        dn = pltpu.make_async_remote_copy(
            src_ref=zs.at[stage, at, :, 0], dst_ref=zh.at[stage, at, :, 1],
            send_sem=zsend.at[stage, tau, 1], recv_sem=zrecv.at[stage, tau, 1], device_id=z_prev, device_id_type=MESH)
        return up, dn, z_lo, z_hi

    def start(copies):
        up, dn, has_lo, has_hi = copies
        pl.when(has_hi)(up.start)
        pl.when(has_lo)(dn.start)

    def wait(copies):
        up, dn, has_lo, has_hi = copies

        @pl.when(has_hi)
        def _():
            up.wait_send()
            dn.wait_recv()

        @pl.when(has_lo)
        def _():
            dn.wait_send()
            up.wait_recv()

    def x_copy(buf, stage, layer, j):
        src = vol.at[x_of(j)] if stage == 0 else buf.at[layer, half + j]
        return pltpu.make_async_remote_copy(
            src_ref=src, dst_ref=buf.at[layer, half - 1 - j],
            send_sem=xsend.at[stage, j], recv_sem=xrecv.at[stage, j], device_id=x_peer, device_id_type=MESH)

    def start_x(buf, stage, layer, tau):
        for task in range(-(-half // PLANES)):
            @pl.when(tau == task)
            def _():
                for j in range(task * PLANES, min(half, (task + 1) * PLANES)):
                    x_copy(buf, stage, layer, j).start()

    def wait_x(buf, stage, layer, tau):
        @pl.when(tau == 0)
        def _():
            for j in range(half):
                x_copy(buf, stage, layer, j).wait()

    for j in range(half):
        x_copy(vols, 0, 0, j).start()

    def wait_in(j, carry):
        in_copy(j).wait()
        return carry

    lax.fori_loop(0, planes, wait_in, 0)

    def x_pass(matrix, buf, layer, tau, emit):
        for group in range(rows // GROUP):
            at = pl.ds(group * GROUP, GROUP)
            source = jnp.concatenate([buf[layer, tau * PLANES + p, at, :] for p in range(PLANES + 2 * half)], axis=0)
            total = dot(matrix[layer], source)
            for p in range(PLANES):
                emit(tau * PLANES + p, at, total[p * GROUP:(p + 1) * GROUP])

    def y_source(buf, stage, j, part):
        if part == 0:
            return jnp.concatenate([yh[stage, j, 0, 0], buf[j, :half_rows + edge_y]], axis=0)
        return jnp.concatenate([buf[j, half_rows - edge_y:], yh[stage, j, 0, 1]], axis=0)

    def z_source(buf, stage, j, part):
        halo = zh[stage, j, part]
        return jnp.concatenate([buf[j, part * half_rows:(part + 1) * half_rows], halo.reshape(edge_z, halo.shape[2])], axis=0)

    def put_z_edge(stage, j, part, value):
        zs[stage, j, part] = value.reshape(zs.shape[3:])

    def fx(layer, tau):
        wait_x(vols, layer, layer, tau)

        def emit(j, at, total):
            a1[j, at, :] = total.astype(BF16)

        x_pass(mfx, vols, layer, tau, emit)
        start(y_copies(a1, layer, tau))

    def fy(layer, tau):
        wait(y_copies(a1, layer, tau))
        for p in range(PLANES):
            j = tau * PLANES + p
            for part in range(2):
                total = dot(mfy[layer], y_source(a1, layer, j, part)).astype(BF16)
                a2[j, part * half_rows:(part + 1) * half_rows] = total[:half_rows]
                put_z_edge(layer, j, part, total[half_rows:])
        start(z_copies(layer, tau))

    def fz(layer, tau):
        wait(z_copies(layer, tau))
        bias = b[layer, :][None, :]
        for p in range(PLANES):
            j = tau * PLANES + p
            for part in range(2):
                at = slice(part * half_rows, (part + 1) * half_rows)
                filtered = dot(mfz[layer], z_source(a2, layer, j, part)).astype(BF16)
                a3[layer, j, at] = filtered
                pre = dot(filtered, w[layer])
                for first in range(0, half_rows, CHUNK):
                    at = slice(part * half_rows + first, part * half_rows + first + CHUNK)
                    z = pre[first:first + CHUNK] + bias
                    cdf = 0.5 * lax.erf(z * SQRT_HALF) + 0.5
                    gp[layer, j, at] = cdf + z * (jnp.exp2((z * z) * -HALF_LOG2_E) * INV_SQRT_2PI)
                    if layer + 1 < num_layers:
                        vols[layer + 1, j + half, at] = (vols[layer, j + half, at].astype(F32) + z * cdf).astype(BF16)
        if layer + 1 < num_layers:
            start_x(vols, layer + 1, layer + 1, tau)

    def bs(layer, tau):
        stage = num_layers + layer
        if layer == num_layers - 1:
            for p in range(PLANES):
                cot_copy(tau * PLANES + p).wait()
        total_b = gwx[layer, 0, part_x:]
        for p in range(PLANES):
            j = tau * PLANES + p
            for part in range(2):
                chunks = []
                for first in range(part * half_rows, (part + 1) * half_rows, CHUNK):
                    at = slice(first, first + CHUNK)
                    scaled = gp[layer, j, at] * grad[j, at].astype(F32)
                    total_b = total_b + jnp.sum(scaled.reshape(CHUNK // 8, 8, scaled.shape[1]), axis=0)
                    chunks.append(scaled.astype(BF16))
                    sb[p, at] = chunks[-1]
                at = slice(part * half_rows, (part + 1) * half_rows)
                rounded = jnp.concatenate(chunks, axis=0)
                mixed = lax.dot_general(rounded, w[layer], (((1,), (1,)), ((), ())), preferred_element_type=F32).astype(BF16)
                d3[j, at] = mixed
                put_z_edge(stage, j, part, dot(sel[...], mixed).astype(BF16))
        gwx[layer, 0, part_x:] = total_b
        start(z_copies(stage, tau))
        channels = w.shape[1]
        product = lax.dot_general(
            a3[layer, pl.ds(tau * PLANES, PLANES)].reshape(PLANES * rows, channels), sb[...].reshape(PLANES * rows, channels),
            (((0,), (0,)), ((), ())), preferred_element_type=F32)
        for side in range(nx):
            gwx[layer, side, :part_x] += product[side * part_x:(side + 1) * part_x]

    def bz(layer, tau):
        stage = num_layers + layer
        wait(z_copies(stage, tau))
        for p in range(PLANES):
            j = tau * PLANES + p
            for part in range(2):
                d2[j, part * half_rows:(part + 1) * half_rows] = dot(mbz[layer], z_source(d3, stage, j, part)).astype(BF16)
        start(y_copies(d2, stage, tau))

    def by(layer, tau):
        stage = num_layers + layer
        wait(y_copies(d2, stage, tau))
        for p in range(PLANES):
            j = tau * PLANES + p
            for part in range(2):
                d1[layer, j + half, part * half_rows:(part + 1) * half_rows] = dot(mby[layer], y_source(d2, stage, j, part)).astype(BF16)
        start_x(d1, stage, layer, tau)

    def out_copy(j):
        return pltpu.make_async_copy(grad.at[j], out.at[x_of(j)], out_sem.at[j])

    def bx(layer, tau):
        wait_x(d1, num_layers + layer, layer, tau)

        def emit(j, at, total):
            grad[j, at, :] = (grad[j, at, :].astype(F32) + total).astype(BF16)

        x_pass(mbx, d1, layer, tau, emit)
        if layer == 0:
            for p in range(PLANES):
                out_copy(tau * PLANES + p).start()

    def sum_copy(layer, phase, offset, src, dst, device):
        return pltpu.make_async_remote_copy(
            src_ref=src, dst_ref=dst, send_sem=sum_send.at[layer, phase, offset], recv_sem=sum_recv.at[layer, phase, offset],
            device_id=device, device_id_type=MESH)

    def phase_copies(layer, phase):
        base_x = my_x * part_x
        base_y = base_x + my_y * part_y
        base_z = base_y + my_z * part_z
        if phase == 0:
            return [sum_copy(layer, 0, 0, gwx.at[layer, 1 - my_x], rx.at[layer], x_peer)]
        if phase == 5:
            at = pl.ds(pl.multiple_of(base_x, part_x), part_x)
            return [sum_copy(layer, 5, 0, gw_out.at[layer, at], gw_out.at[layer, at], x_peer)]
        copies = []
        along_y = phase in (1, 4)
        count, me, name = (ny, my_y, 'gy') if along_y else (nz, my_z, 'gz')
        for offset in range(1, count):
            other = lax.rem(me + offset, count)
            if phase == 1:
                src, dst = ry.at[layer, 1, other], ry.at[layer, 0, me]
            elif phase == 2:
                src, dst = rz.at[layer, 1, other], rz.at[layer, 0, me]
            else:
                at = pl.ds(pl.multiple_of(base_z, part_z), part_z) if phase == 3 else pl.ds(pl.multiple_of(base_y, part_y), part_y)
                src, dst = gw_out.at[layer, at], gw_out.at[layer, at]
            copies.append(sum_copy(layer, phase, offset - 1, src, dst, {name: other}))
        return copies

    def start_phase(layer, phase):
        for copy in phase_copies(layer, phase):
            copy.start()

    def wait_phase(layer, phase):
        for copy in phase_copies(layer, phase):
            copy.wait()

    def r0(layer, tau):
        gwx[layer, 1, part_x:] = gwx[layer, 0, part_x:]
        start_phase(layer, 0)

    def spread(total, count, part, slots, layer, me):
        bias = total[count * part:]
        for k in range(count):
            slots[layer, 1, k, :part] = total[k * part:(k + 1) * part]
            slots[layer, 1, k, part:] = bias
        slots[layer, 0, me] = slots[layer, 1, me]

    def r1(layer, tau):
        wait_phase(layer, 0)
        spread(gwx[layer, my_x] + rx[layer], ny, part_y, ry, layer, my_y)
        start_phase(layer, 1)

    def gathered(slots, layer, count):
        total = slots[layer, 0, 0]
        for k in range(1, count):
            total = total + slots[layer, 0, k]
        return total

    def r2(layer, tau):
        wait_phase(layer, 1)
        spread(gathered(ry, layer, ny), nz, part_z, rz, layer, my_z)
        start_phase(layer, 2)

    def r3(layer, tau):
        wait_phase(layer, 2)
        total = gathered(rz, layer, nz)
        gw_out[layer, pl.ds(pl.multiple_of(my_x * part_x + my_y * part_y + my_z * part_z, part_z), part_z)] = total[:part_z]
        gb_out[layer, :] = jnp.sum(total[part_z:], axis=0)
        start_phase(layer, 3)

    def r4(layer, tau):
        wait_phase(layer, 3)
        start_phase(layer, 4)

    def r5(layer, tau):
        wait_phase(layer, 4)
        start_phase(layer, 5)

    def r6(layer, tau):
        wait_phase(layer, 5)

    tasks = {'r0': r0, 'r1': r1, 'r2': r2, 'r3': r3, 'r4': r4, 'r5': r5, 'r6': r6, 'fx': fx, 'fy': fy, 'fz': fz, 'bs': bs, 'bz': bz, 'by': by, 'bx': bx}
    stages, last = stage_list(num_layers, nt)

    def step(s, carry):
        for kind, layer, first in stages:
            tau = s - first

            @pl.when((tau >= 0) & (tau < (1 if kind[0] == 'r' else nt)))
            def _():
                tasks[kind](layer, tau)
        return carry

    lax.fori_loop(0, last, step, 0)

    def wait_out(j, carry):
        out_copy(j).wait()
        return carry

    lax.fori_loop(0, planes, wait_out, 0)


def solution(mesh):
    names = ('gx', 'gy', 'gz')
    nx, ny, nz = (mesh.shape[axis_name] for axis_name in names)
    assert nx == 2
    vol_spec = P('dp', 'gx', 'gy', 'gz')

    def local_step(volume, cot_out, filter_taps, w_mix, b_mix):
        channels, planes, by_len, bz_len = volume.shape
        num_layers, _, num_taps = filter_taps.shape
        half = (num_taps - 1) // 2
        rows = by_len * bz_len
        edge_y, edge_z = half * bz_len, half * by_len
        nt = planes // PLANES
        stages = 2 * num_layers
        part_x = channels // nx
        part_y = part_x // ny
        part_z = part_y // nz

        def to_rows(block):
            return jnp.transpose(block, (1, 2, 3, 0)).reshape(planes, rows, channels)

        any_spec = pl.BlockSpec(memory_space=pl.ANY)
        vmem_spec = pl.BlockSpec(memory_space=pltpu.VMEM)
        smem_spec = pl.BlockSpec(memory_space=pltpu.SMEM)
        block = (planes, rows, channels)
        dma = pltpu.SemaphoreType.DMA
        grad_rows, grad_w, grad_b = pl.pallas_call(
            functools.partial(kernel, (nx, ny, nz, num_layers, num_taps, by_len, bz_len)),
            out_shape=(
                jax.ShapeDtypeStruct(block, BF16),
                jax.ShapeDtypeStruct((num_layers, channels, channels), F32),
                jax.ShapeDtypeStruct((num_layers, channels), F32),
            ),
            in_specs=[any_spec, any_spec, smem_spec, vmem_spec, vmem_spec],
            out_specs=(any_spec, vmem_spec, vmem_spec),
            scratch_shapes=[
                pltpu.VMEM((num_layers, planes + 2 * half, rows, channels), BF16),
                pltpu.VMEM(block, BF16),
                pltpu.VMEM(block, BF16),
                pltpu.VMEM((num_layers,) + block, BF16),
                pltpu.VMEM((num_layers,) + block, F32),
                pltpu.VMEM(block, BF16),
                pltpu.VMEM(block, BF16),
                pltpu.VMEM(block, BF16),
                pltpu.VMEM((num_layers, planes + 2 * half, rows, channels), BF16),
                pltpu.VMEM((PLANES, rows, channels), BF16),
                pltpu.VMEM((stages, planes, 1, 2, edge_y, channels), BF16),
                pltpu.VMEM((stages, planes, 2, 2, edge_z // 2, channels), BF16),
                pltpu.VMEM((stages, planes, 2, 2, edge_z // 2, channels), BF16),
                pltpu.VMEM((num_layers, PLANES * GROUP, (PLANES + 2 * half) * GROUP), BF16),
                pltpu.VMEM((num_layers, rows // 2 + edge_z, rows // 2 + 2 * edge_y), BF16),
                pltpu.VMEM((num_layers, rows // 2, rows // 2 + edge_z), BF16),
                pltpu.VMEM((num_layers, PLANES * GROUP, (PLANES + 2 * half) * GROUP), BF16),
                pltpu.VMEM((num_layers, rows // 2, rows // 2 + 2 * edge_y), BF16),
                pltpu.VMEM((num_layers, rows // 2, rows // 2 + edge_z), BF16),
                pltpu.VMEM((edge_z, rows // 2), BF16),
                pltpu.VMEM((num_layers, nx, part_x + 8, channels), F32),
                pltpu.VMEM((num_layers, part_x + 8, channels), F32),
                pltpu.VMEM((num_layers, 2, ny, part_y + 8, channels), F32),
                pltpu.VMEM((num_layers, 2, nz, part_z + 8, channels), F32),
                dma((num_layers, 6, max(ny, nz, 2) - 1)), dma((num_layers, 6, max(ny, nz, 2) - 1)),
                dma((planes,)), dma((planes,)), dma((planes,)),
                dma((stages, nt, 2)), dma((stages, nt, 2)), dma((stages, nt, 2)), dma((stages, nt, 2)),
                dma((stages, half)), dma((stages, half)),
            ],
            compiler_params=pltpu.CompilerParams(
                collective_id=0, has_side_effects=True, vmem_limit_bytes=64000 * 1024),
            name='stack',
        )(to_rows(volume), to_rows(cot_out), filter_taps, w_mix, b_mix)
        grad_volume = jnp.transpose(grad_rows.reshape(planes, by_len, bz_len, channels), (3, 0, 1, 2))
        return grad_volume, grad_w, grad_b

    return jax.shard_map(local_step, mesh=mesh, in_specs=(vol_spec, vol_spec, P(), P(), P()), out_specs=(vol_spec, P('dp'), P('dp')), check_vma=False)
```

```python
import functools

import jax
import jax.numpy as jnp
from jax import lax
from jax.experimental import pallas as pl
from jax.experimental.pallas import tpu as pltpu
from jax.sharding import PartitionSpec as P

MESH = pl.DeviceIdType.MESH
PLANES = 2
LAG = 3
SUM_STEPS = (0, 2, 6, 10, 12)
LAST_SUM_STEPS = (0, 1, 6, 8, 9)
XLAG = 1
F32 = jnp.float32
BF16 = jnp.bfloat16
SQRT_HALF = 0.7071067811865476
HALF_LOG2_E = 0.7213475204444817
CHUNK = 16
GROUP = 32
INV_SQRT_2PI = 0.3989422804014327


def dot(a, b):
    return jnp.dot(a, b, preferred_element_type=F32)


def stage_list(num_layers, nt):
    stages = []
    start = 0
    for layer in range(num_layers):
        stages.append(('fx', layer, start))
        stages.append(('fy', layer, start + LAG))
        stages.append(('fz', layer, start + 2 * LAG))
        start += 2 * LAG + (XLAG if layer + 1 < num_layers else 0)
    for layer in reversed(range(num_layers)):
        stages.append(('bs', layer, start))
        stages.append(('bz', layer, start + LAG))
        stages.append(('by', layer, start + 2 * LAG))
        stages.append(('bx', layer, start + 2 * LAG + XLAG))
        start += 2 * LAG + XLAG
    for kind, layer, first in list(stages):
        if kind == 'bs':
            stages += [('r%d' % phase, layer, first + nt - 1 + (SUM_STEPS if layer else LAST_SUM_STEPS)[phase]) for phase in range(5)]
    return stages, max(first + (1 if kind[0] == 'r' else nt) for kind, _, first in stages)


def kernel(sizes, vol, cot, taps, w, b, out, gw_out, gb_out,
           vols, a1, a2, a3, gp, grad, d3, d2, d1, sb, yh, zh, zs,
           mfx, mfy, mfz, mbx, mby, mbz, sel,
           gwx, rx, rq, sum_send, sum_recv,
           in_sem, cot_sem, out_sem, ysend, yrecv, zsend, zrecv, xsend, xrecv):
    nx, ny, nz, num_layers, num_taps, by_len, bz_len = sizes
    half = (num_taps - 1) // 2
    planes = a1.shape[0]
    rows = by_len * bz_len
    edge_y = half * bz_len
    edge_z = half * by_len
    nt = planes // PLANES
    part_x = w.shape[1] // nx
    group = ny * nz
    part_q = part_x // group
    my_x, my_y, my_z = lax.axis_index('gx'), lax.axis_index('gy'), lax.axis_index('gz')
    y_lo, y_hi = my_y > 0, my_y < ny - 1
    z_lo, z_hi = my_z > 0, my_z < nz - 1
    y_prev, y_next = {'gy': jnp.maximum(my_y - 1, 0)}, {'gy': jnp.minimum(my_y + 1, ny - 1)}
    z_prev, z_next = {'gz': jnp.maximum(my_z - 1, 0)}, {'gz': jnp.minimum(my_z + 1, nz - 1)}
    x_peer = {'gx': 1 - my_x}

    def x_of(j):
        return my_x * j + (1 - my_x) * (planes - 1 - j)

    my_q = my_z * ny + my_y

    def chip(q):
        return {'gy': lax.rem(q, ny), 'gz': q // ny}

    barrier = pltpu.get_barrier_semaphore()
    pl.semaphore_signal(barrier, inc=1, device_id=x_peer, device_id_type=MESH)

    def signal_chip(offset, carry):
        pl.semaphore_signal(barrier, inc=1, device_id=chip(lax.rem(my_q + offset, group)), device_id_type=MESH)
        return carry

    lax.fori_loop(1, group, signal_chip, 0)

    def in_copy(j):
        return pltpu.make_async_copy(vol.at[x_of(j)], vols.at[0, j + half], in_sem.at[j])

    def cot_copy(j):
        return pltpu.make_async_copy(cot.at[x_of(j)], grad.at[j], cot_sem.at[j])

    def start_in(j, carry):
        in_copy(j).start()
        cot_copy(j).start()
        return carry

    lax.fori_loop(0, planes, start_in, 0)

    half_y, half_rows = by_len // 2, rows // 2

    def iota(shape, axis):
        return lax.broadcasted_iota(jnp.int32, shape, axis)

    def banded(layer, axis, back, hop, inside):
        total = jnp.zeros(hop.shape, F32)
        for t in range(num_taps):
            tap = taps[layer, axis, num_taps - 1 - t if back else t]
            if axis == 0:
                tap = jnp.where(my_x == 1, tap, taps[layer, axis, t if back else num_taps - 1 - t])
            total = jnp.where(hop == t, tap, total)
        return jnp.where(inside, total, 0.0).astype(BF16)

    def build(layer, carry):
        i, k = iota((PLANES * GROUP, (PLANES + 2 * half) * GROUP), 0), iota((PLANES * GROUP, (PLANES + 2 * half) * GROUP), 1)
        hop, inside = k // GROUP - i // GROUP, k % GROUP == i % GROUP
        mfx[layer] = banded(layer, 0, False, hop, inside)
        mbx[layer] = banded(layer, 0, True, hop, inside)
        i, k = iota((half_rows, half_rows + 2 * edge_y), 0), iota((half_rows, half_rows + 2 * edge_y), 1)
        hop, inside = k // bz_len - i // bz_len, k % bz_len == i % bz_len
        mfy[layer, :half_rows] = banded(layer, 1, False, hop, inside)
        mby[layer] = banded(layer, 1, True, hop, inside)
        i, k = iota((edge_z, half_rows + 2 * edge_y), 0), iota((edge_z, half_rows + 2 * edge_y), 1)
        z_edge = i // half_y % half + i // (half * half_y) * (bz_len - half)
        mfy[layer, half_rows:] = banded(layer, 1, False, k // bz_len - i % half_y, k % bz_len == z_edge)
        i, k = iota((half_rows, half_rows), 0), iota((half_rows, half_rows), 1)
        hop, inside = k % bz_len - i % bz_len + half, k // bz_len == i // bz_len
        mfz[layer, :, :half_rows] = banded(layer, 2, False, hop, inside)
        mbz[layer, :, :half_rows] = banded(layer, 2, True, hop, inside)
        i, k = iota((half_rows, edge_z), 0), iota((half_rows, edge_z), 1)
        hop = k // half_y % half + k // (half * half_y) * (bz_len + half) - i % bz_len
        inside = k % half_y == i // bz_len
        mfz[layer, :, half_rows:] = banded(layer, 2, False, hop, inside)
        mbz[layer, :, half_rows:] = banded(layer, 2, True, hop, inside)
        return carry

    lax.fori_loop(0, num_layers, build, 0)
    i, k = iota((edge_z, half_rows), 0), iota((edge_z, half_rows), 1)
    z_edge = i // half_y % half + i // (half * half_y) * (bz_len - half)
    sel[...] = jnp.where((k // bz_len == i % half_y) & (k % bz_len == z_edge), 1.0, 0.0).astype(BF16)

    for layer in range(num_layers):
        vols[layer, planes + half:] = jnp.zeros((half,) + vols.shape[2:], BF16)
        d1[layer, planes + half:] = jnp.zeros((half,) + d1.shape[2:], BF16)

    def zero_halo(halo, where, side):
        @pl.when(where)
        def _():
            def clear(j, carry):
                for stage in range(2 * num_layers):
                    halo[stage, j, :, side] = jnp.zeros(halo.shape[2:3] + halo.shape[4:], BF16)
                return carry
            lax.fori_loop(0, planes, clear, 0)

    zero_halo(yh, my_y == 0, 0)
    zero_halo(yh, my_y == ny - 1, 1)
    zero_halo(zh, my_z == 0, 0)
    zero_halo(zh, my_z == nz - 1, 1)
    gwx[...] = jnp.zeros(gwx.shape, F32)

    pl.semaphore_wait(barrier, group)

    def y_copies(src, stage, tau):
        at = pl.ds(tau * PLANES, PLANES)
        up = pltpu.make_async_remote_copy(
            src_ref=src.at[at, pl.ds(rows - edge_y, edge_y)], dst_ref=yh.at[stage, at, 0, 0],
            send_sem=ysend.at[stage, tau, 0], recv_sem=yrecv.at[stage, tau, 0], device_id=y_next, device_id_type=MESH)
        dn = pltpu.make_async_remote_copy(
            src_ref=src.at[at, pl.ds(0, edge_y)], dst_ref=yh.at[stage, at, 0, 1],
            send_sem=ysend.at[stage, tau, 1], recv_sem=yrecv.at[stage, tau, 1], device_id=y_prev, device_id_type=MESH)
        return up, dn, y_lo, y_hi

    def z_copies(stage, tau):
        at = pl.ds(tau * PLANES, PLANES)
        up = pltpu.make_async_remote_copy(
            src_ref=zs.at[stage, at, :, 1], dst_ref=zh.at[stage, at, :, 0],
            send_sem=zsend.at[stage, tau, 0], recv_sem=zrecv.at[stage, tau, 0], device_id=z_next, device_id_type=MESH)
        dn = pltpu.make_async_remote_copy(
            src_ref=zs.at[stage, at, :, 0], dst_ref=zh.at[stage, at, :, 1],
            send_sem=zsend.at[stage, tau, 1], recv_sem=zrecv.at[stage, tau, 1], device_id=z_prev, device_id_type=MESH)
        return up, dn, z_lo, z_hi

    def start(copies):
        up, dn, has_lo, has_hi = copies
        pl.when(has_hi)(up.start)
        pl.when(has_lo)(dn.start)

    def wait(copies):
        up, dn, has_lo, has_hi = copies

        @pl.when(has_hi)
        def _():
            up.wait_send()
            dn.wait_recv()

        @pl.when(has_lo)
        def _():
            dn.wait_send()
            up.wait_recv()

    def x_copy(buf, stage, layer, j):
        src = vol.at[x_of(j)] if stage == 0 else buf.at[layer, half + j]
        return pltpu.make_async_remote_copy(
            src_ref=src, dst_ref=buf.at[layer, half - 1 - j],
            send_sem=xsend.at[stage, j], recv_sem=xrecv.at[stage, j], device_id=x_peer, device_id_type=MESH)

    def start_x(buf, stage, layer, tau):
        for task in range(-(-half // PLANES)):
            @pl.when(tau == task)
            def _():
                for j in range(task * PLANES, min(half, (task + 1) * PLANES)):
                    x_copy(buf, stage, layer, j).start()

    def wait_x(buf, stage, layer, tau):
        @pl.when(tau == 0)
        def _():
            for j in range(half):
                x_copy(buf, stage, layer, j).wait()

    for j in range(half):
        x_copy(vols, 0, 0, j).start()

    def wait_in(j, carry):
        in_copy(j).wait()
        return carry

    lax.fori_loop(0, planes, wait_in, 0)

    def x_pass(matrix, buf, layer, tau, emit):
        for group in range(rows // GROUP):
            at = pl.ds(group * GROUP, GROUP)
            source = jnp.concatenate([buf[layer, tau * PLANES + p, at, :] for p in range(PLANES + 2 * half)], axis=0)
            total = dot(matrix[layer], source)
            for p in range(PLANES):
                emit(tau * PLANES + p, at, total[p * GROUP:(p + 1) * GROUP])

    def y_source(buf, stage, j, part):
        if part == 0:
            return jnp.concatenate([yh[stage, j, 0, 0], buf[j, :half_rows + edge_y]], axis=0)
        return jnp.concatenate([buf[j, half_rows - edge_y:], yh[stage, j, 0, 1]], axis=0)

    def z_source(buf, stage, j, part):
        halo = zh[stage, j, part]
        return jnp.concatenate([buf[j, part * half_rows:(part + 1) * half_rows], halo.reshape(edge_z, halo.shape[2])], axis=0)

    def put_z_edge(stage, j, part, value):
        zs[stage, j, part] = value.reshape(zs.shape[3:])

    def fx(layer, tau):
        wait_x(vols, layer, layer, tau)

        def emit(j, at, total):
            a1[j, at, :] = total.astype(BF16)

        x_pass(mfx, vols, layer, tau, emit)
        start(y_copies(a1, layer, tau))

    def fy(layer, tau):
        wait(y_copies(a1, layer, tau))
        for p in range(PLANES):
            j = tau * PLANES + p
            for part in range(2):
                total = dot(mfy[layer], y_source(a1, layer, j, part)).astype(BF16)
                a2[j, part * half_rows:(part + 1) * half_rows] = total[:half_rows]
                put_z_edge(layer, j, part, total[half_rows:])
        start(z_copies(layer, tau))

    def fz(layer, tau):
        wait(z_copies(layer, tau))
        bias = b[layer, :][None, :]
        for p in range(PLANES):
            j = tau * PLANES + p
            for part in range(2):
                at = slice(part * half_rows, (part + 1) * half_rows)
                filtered = dot(mfz[layer], z_source(a2, layer, j, part)).astype(BF16)
                a3[layer, j, at] = filtered
                pre = dot(filtered, w[layer])
                for first in range(0, half_rows, CHUNK):
                    at = slice(part * half_rows + first, part * half_rows + first + CHUNK)
                    z = pre[first:first + CHUNK] + bias
                    cdf = 0.5 * lax.erf(z * SQRT_HALF) + 0.5
                    gp[layer, j, at] = cdf + z * (jnp.exp2((z * z) * -HALF_LOG2_E) * INV_SQRT_2PI)
                    if layer + 1 < num_layers:
                        vols[layer + 1, j + half, at] = (vols[layer, j + half, at].astype(F32) + z * cdf).astype(BF16)
        if layer + 1 < num_layers:
            start_x(vols, layer + 1, layer + 1, tau)

    def bs(layer, tau):
        stage = num_layers + layer
        if layer == num_layers - 1:
            for p in range(PLANES):
                cot_copy(tau * PLANES + p).wait()
        total_b = gwx[layer, 0, part_x:]
        for p in range(PLANES):
            j = tau * PLANES + p
            for part in range(2):
                chunks = []
                for first in range(part * half_rows, (part + 1) * half_rows, CHUNK):
                    at = slice(first, first + CHUNK)
                    scaled = gp[layer, j, at] * grad[j, at].astype(F32)
                    total_b = total_b + jnp.sum(scaled.reshape(CHUNK // 8, 8, scaled.shape[1]), axis=0)
                    chunks.append(scaled.astype(BF16))
                    sb[p, at] = chunks[-1]
                at = slice(part * half_rows, (part + 1) * half_rows)
                rounded = jnp.concatenate(chunks, axis=0)
                mixed = lax.dot_general(rounded, w[layer], (((1,), (1,)), ((), ())), preferred_element_type=F32).astype(BF16)
                d3[j, at] = mixed
                put_z_edge(stage, j, part, dot(sel[...], mixed).astype(BF16))
        gwx[layer, 0, part_x:] = total_b
        start(z_copies(stage, tau))
        channels = w.shape[1]
        product = lax.dot_general(
            a3[layer, pl.ds(tau * PLANES, PLANES)].reshape(PLANES * rows, channels), sb[...].reshape(PLANES * rows, channels),
            (((0,), (0,)), ((), ())), preferred_element_type=F32)
        for side in range(nx):
            gwx[layer, side, :part_x] += product[side * part_x:(side + 1) * part_x]

    def bz(layer, tau):
        stage = num_layers + layer
        wait(z_copies(stage, tau))
        for p in range(PLANES):
            j = tau * PLANES + p
            for part in range(2):
                d2[j, part * half_rows:(part + 1) * half_rows] = dot(mbz[layer], z_source(d3, stage, j, part)).astype(BF16)
        start(y_copies(d2, stage, tau))

    def by(layer, tau):
        stage = num_layers + layer
        wait(y_copies(d2, stage, tau))
        for p in range(PLANES):
            j = tau * PLANES + p
            for part in range(2):
                d1[layer, j + half, part * half_rows:(part + 1) * half_rows] = dot(mby[layer], y_source(d2, stage, j, part)).astype(BF16)
        start_x(d1, stage, layer, tau)

    def out_copy(j):
        return pltpu.make_async_copy(grad.at[j], out.at[x_of(j)], out_sem.at[j])

    def bx(layer, tau):
        wait_x(d1, num_layers + layer, layer, tau)

        def emit(j, at, total):
            grad[j, at, :] = (grad[j, at, :].astype(F32) + total).astype(BF16)

        x_pass(mbx, d1, layer, tau, emit)
        if layer == 0:
            for p in range(PLANES):
                out_copy(tau * PLANES + p).start()

    def sum_copy(layer, phase, offset, src, dst, device):
        return pltpu.make_async_remote_copy(
            src_ref=src, dst_ref=dst, send_sem=sum_send.at[layer, phase, offset], recv_sem=sum_recv.at[layer, phase, offset],
            device_id=device, device_id_type=MESH)

    def core_copy(layer, phase):
        if phase == 0:
            return sum_copy(layer, 0, 0, gwx.at[layer, 1 - my_x], rx.at[layer], x_peer)
        at = pl.ds(pl.multiple_of(my_x * part_x, part_x), part_x)
        return sum_copy(layer, 3, 0, gw_out.at[layer, at], gw_out.at[layer, at], x_peer)

    def own_rows():
        return pl.ds(pl.multiple_of(my_x * part_x + my_q * part_q, part_q), part_q)

    def chip_copy(layer, phase, offset):
        other = lax.rem(my_q + offset, group)
        if phase == 1:
            return sum_copy(layer, 1, offset, rq.at[layer, 1, other], rq.at[layer, 0, my_q], chip(other))
        return sum_copy(layer, 2, offset, gw_out.at[layer, own_rows()], gw_out.at[layer, own_rows()], chip(other))

    def each_chip(layer, phase, act):
        def body(offset, carry):
            act(chip_copy(layer, phase, offset))
            return carry
        lax.fori_loop(1, group, body, 0)

    def r0(layer, tau):
        gwx[layer, 1, part_x:] = gwx[layer, 0, part_x:]
        core_copy(layer, 0).start()

    def r1(layer, tau):
        core_copy(layer, 0).wait()
        bias = gwx[layer, my_x, part_x:] + rx[layer, part_x:]
        for q in range(group):
            at = slice(q * part_q, (q + 1) * part_q)
            rq[layer, 1, q, :part_q] = gwx[layer, my_x, at] + rx[layer, at]
            rq[layer, 1, q, part_q:] = bias
        rq[layer, 0, my_q] = rq[layer, 1, my_q]
        each_chip(layer, 1, lambda copy: copy.start())

    def r2(layer, tau):
        each_chip(layer, 1, lambda copy: copy.wait())
        total = rq[layer, 0, 0]
        for q in range(1, group):
            total = total + rq[layer, 0, q]
        gw_out[layer, own_rows()] = total[:part_q]
        gb_out[layer, :] = jnp.sum(total[part_q:], axis=0)
        each_chip(layer, 2, lambda copy: copy.start())

    def r3(layer, tau):
        each_chip(layer, 2, lambda copy: copy.wait())
        core_copy(layer, 3).start()

    def r4(layer, tau):
        core_copy(layer, 3).wait()

    tasks = {'r0': r0, 'r1': r1, 'r2': r2, 'r3': r3, 'r4': r4, 'fx': fx, 'fy': fy, 'fz': fz, 'bs': bs, 'bz': bz, 'by': by, 'bx': bx}
    stages, last = stage_list(num_layers, nt)

    def step(s, carry):
        for kind, layer, first in stages:
            tau = s - first

            @pl.when((tau >= 0) & (tau < (1 if kind[0] == 'r' else nt)))
            def _():
                tasks[kind](layer, tau)
        return carry

    lax.fori_loop(0, last, step, 0)

    def wait_out(j, carry):
        out_copy(j).wait()
        return carry

    lax.fori_loop(0, planes, wait_out, 0)


def solution(mesh):
    names = ('gx', 'gy', 'gz')
    nx, ny, nz = (mesh.shape[axis_name] for axis_name in names)
    assert nx == 2
    vol_spec = P('dp', 'gx', 'gy', 'gz')

    def local_step(volume, cot_out, filter_taps, w_mix, b_mix):
        channels, planes, by_len, bz_len = volume.shape
        num_layers, _, num_taps = filter_taps.shape
        half = (num_taps - 1) // 2
        rows = by_len * bz_len
        edge_y, edge_z = half * bz_len, half * by_len
        nt = planes // PLANES
        stages = 2 * num_layers
        part_x = channels // nx
        part_q = part_x // (ny * nz)

        def to_rows(block):
            return jnp.transpose(block, (1, 2, 3, 0)).reshape(planes, rows, channels)

        any_spec = pl.BlockSpec(memory_space=pl.ANY)
        vmem_spec = pl.BlockSpec(memory_space=pltpu.VMEM)
        smem_spec = pl.BlockSpec(memory_space=pltpu.SMEM)
        block = (planes, rows, channels)
        dma = pltpu.SemaphoreType.DMA
        grad_rows, grad_w, grad_b = pl.pallas_call(
            functools.partial(kernel, (nx, ny, nz, num_layers, num_taps, by_len, bz_len)),
            out_shape=(
                jax.ShapeDtypeStruct(block, BF16),
                jax.ShapeDtypeStruct((num_layers, channels, channels), F32),
                jax.ShapeDtypeStruct((num_layers, channels), F32),
            ),
            in_specs=[any_spec, any_spec, smem_spec, vmem_spec, vmem_spec],
            out_specs=(any_spec, vmem_spec, vmem_spec),
            scratch_shapes=[
                pltpu.VMEM((num_layers, planes + 2 * half, rows, channels), BF16),
                pltpu.VMEM(block, BF16),
                pltpu.VMEM(block, BF16),
                pltpu.VMEM((num_layers,) + block, BF16),
                pltpu.VMEM((num_layers,) + block, F32),
                pltpu.VMEM(block, BF16),
                pltpu.VMEM(block, BF16),
                pltpu.VMEM(block, BF16),
                pltpu.VMEM((num_layers, planes + 2 * half, rows, channels), BF16),
                pltpu.VMEM((PLANES, rows, channels), BF16),
                pltpu.VMEM((stages, planes, 1, 2, edge_y, channels), BF16),
                pltpu.VMEM((stages, planes, 2, 2, edge_z // 2, channels), BF16),
                pltpu.VMEM((stages, planes, 2, 2, edge_z // 2, channels), BF16),
                pltpu.VMEM((num_layers, PLANES * GROUP, (PLANES + 2 * half) * GROUP), BF16),
                pltpu.VMEM((num_layers, rows // 2 + edge_z, rows // 2 + 2 * edge_y), BF16),
                pltpu.VMEM((num_layers, rows // 2, rows // 2 + edge_z), BF16),
                pltpu.VMEM((num_layers, PLANES * GROUP, (PLANES + 2 * half) * GROUP), BF16),
                pltpu.VMEM((num_layers, rows // 2, rows // 2 + 2 * edge_y), BF16),
                pltpu.VMEM((num_layers, rows // 2, rows // 2 + edge_z), BF16),
                pltpu.VMEM((edge_z, rows // 2), BF16),
                pltpu.VMEM((num_layers, nx, part_x + 8, channels), F32),
                pltpu.VMEM((num_layers, part_x + 8, channels), F32),
                pltpu.VMEM((num_layers, 2, ny * nz, part_q + 8, channels), F32),
                dma((num_layers, 4, ny * nz)), dma((num_layers, 4, ny * nz)),
                dma((planes,)), dma((planes,)), dma((planes,)),
                dma((stages, nt, 2)), dma((stages, nt, 2)), dma((stages, nt, 2)), dma((stages, nt, 2)),
                dma((stages, half)), dma((stages, half)),
            ],
            compiler_params=pltpu.CompilerParams(
                collective_id=0, has_side_effects=True, vmem_limit_bytes=64000 * 1024),
            name='stack',
        )(to_rows(volume), to_rows(cot_out), filter_taps, w_mix, b_mix)
        grad_volume = jnp.transpose(grad_rows.reshape(planes, by_len, bz_len, channels), (3, 0, 1, 2))
        return grad_volume, grad_w, grad_b

    return jax.shard_map(local_step, mesh=mesh, in_specs=(vol_spec, vol_spec, P(), P(), P()), out_specs=(vol_spec, P('dp'), P('dp')), check_vma=False)
```

```python
import functools

import jax
import jax.numpy as jnp
from jax import lax
from jax.experimental import pallas as pl
from jax.experimental.pallas import tpu as pltpu
from jax.sharding import PartitionSpec as P

MESH = pl.DeviceIdType.MESH
PLANES = 4
LAG = 2
SUM_STEPS = (0, 1, 3, 5, 6)
LAST_SUM_STEPS = (0, 1, 3, 5, 6)
XLAG = 1
F32 = jnp.float32
BF16 = jnp.bfloat16
SQRT_HALF = 0.7071067811865476
HALF_LOG2_E = 0.7213475204444817
CHUNK = 16
GROUP = 32
INV_SQRT_2PI = 0.3989422804014327


def dot(a, b):
    return jnp.dot(a, b, preferred_element_type=F32)


def stage_list(num_layers, nt):
    stages = []
    start = 0
    for layer in range(num_layers):
        stages.append(('fx', layer, start))
        stages.append(('fy', layer, start + LAG))
        stages.append(('fz', layer, start + 2 * LAG))
        start += 2 * LAG + (XLAG if layer + 1 < num_layers else 0)
    for layer in reversed(range(num_layers)):
        stages.append(('bs', layer, start))
        stages.append(('bz', layer, start + LAG))
        stages.append(('by', layer, start + 2 * LAG))
        stages.append(('bx', layer, start + 2 * LAG + XLAG))
        start += 2 * LAG + XLAG
    for kind, layer, first in list(stages):
        if kind == 'bs':
            stages += [('r%d' % phase, layer, first + nt - 1 + (SUM_STEPS if layer else LAST_SUM_STEPS)[phase]) for phase in range(5)]
    return stages, max(first + (1 if kind[0] == 'r' else nt) for kind, _, first in stages)


def kernel(sizes, vol, cot, taps, w, b, out, gw_out, gb_out,
           vols, a1, a2, a3, gp, grad, d3, d2, d1, sb, yh, zh, zs,
           mfx, mfy, mfz, mbx, mby, mbz, sel,
           gwx, rx, rq, sum_send, sum_recv,
           in_sem, cot_sem, out_sem, ysend, yrecv, zsend, zrecv, xsend, xrecv):
    nx, ny, nz, num_layers, num_taps, by_len, bz_len = sizes
    half = (num_taps - 1) // 2
    planes = a1.shape[0]
    rows = by_len * bz_len
    edge_y = half * bz_len
    edge_z = half * by_len
    nt = planes // PLANES
    part_x = w.shape[1] // nx
    group = ny * nz
    part_q = part_x // group
    my_x, my_y, my_z = lax.axis_index('gx'), lax.axis_index('gy'), lax.axis_index('gz')
    y_lo, y_hi = my_y > 0, my_y < ny - 1
    z_lo, z_hi = my_z > 0, my_z < nz - 1
    y_prev, y_next = {'gy': jnp.maximum(my_y - 1, 0)}, {'gy': jnp.minimum(my_y + 1, ny - 1)}
    z_prev, z_next = {'gz': jnp.maximum(my_z - 1, 0)}, {'gz': jnp.minimum(my_z + 1, nz - 1)}
    x_peer = {'gx': 1 - my_x}

    def x_of(j):
        return my_x * j + (1 - my_x) * (planes - 1 - j)

    my_q = my_z * ny + my_y

    def chip(q):
        return {'gy': lax.rem(q, ny), 'gz': q // ny}

    barrier = pltpu.get_barrier_semaphore()
    pl.semaphore_signal(barrier, inc=1, device_id=x_peer, device_id_type=MESH)

    def signal_chip(offset, carry):
        pl.semaphore_signal(barrier, inc=1, device_id=chip(lax.rem(my_q + offset, group)), device_id_type=MESH)
        return carry

    lax.fori_loop(1, group, signal_chip, 0)

    def in_copy(j):
        return pltpu.make_async_copy(vol.at[x_of(j)], vols.at[0, j + half], in_sem.at[j])

    def cot_copy(j):
        return pltpu.make_async_copy(cot.at[x_of(j)], grad.at[j], cot_sem.at[j])

    def start_in(j, carry):
        in_copy(j).start()
        cot_copy(j).start()
        return carry

    lax.fori_loop(0, planes, start_in, 0)

    half_y, half_rows = by_len // 2, rows // 2

    def iota(shape, axis):
        return lax.broadcasted_iota(jnp.int32, shape, axis)

    def banded(layer, axis, back, hop, inside):
        total = jnp.zeros(hop.shape, F32)
        for t in range(num_taps):
            tap = taps[layer, axis, num_taps - 1 - t if back else t]
            if axis == 0:
                tap = jnp.where(my_x == 1, tap, taps[layer, axis, t if back else num_taps - 1 - t])
            total = jnp.where(hop == t, tap, total)
        return jnp.where(inside, total, 0.0).astype(BF16)

    def build(layer, carry):
        i, k = iota((PLANES * GROUP, (PLANES + 2 * half) * GROUP), 0), iota((PLANES * GROUP, (PLANES + 2 * half) * GROUP), 1)
        hop, inside = k // GROUP - i // GROUP, k % GROUP == i % GROUP
        mfx[layer] = banded(layer, 0, False, hop, inside)
        mbx[layer] = banded(layer, 0, True, hop, inside)
        i, k = iota((half_rows, half_rows + 2 * edge_y), 0), iota((half_rows, half_rows + 2 * edge_y), 1)
        hop, inside = k // bz_len - i // bz_len, k % bz_len == i % bz_len
        mfy[layer, :half_rows] = banded(layer, 1, False, hop, inside)
        mby[layer] = banded(layer, 1, True, hop, inside)
        i, k = iota((edge_z, half_rows + 2 * edge_y), 0), iota((edge_z, half_rows + 2 * edge_y), 1)
        z_edge = i // half_y % half + i // (half * half_y) * (bz_len - half)
        mfy[layer, half_rows:] = banded(layer, 1, False, k // bz_len - i % half_y, k % bz_len == z_edge)
        i, k = iota((half_rows, half_rows), 0), iota((half_rows, half_rows), 1)
        hop, inside = k % bz_len - i % bz_len + half, k // bz_len == i // bz_len
        mfz[layer, :, :half_rows] = banded(layer, 2, False, hop, inside)
        mbz[layer, :, :half_rows] = banded(layer, 2, True, hop, inside)
        i, k = iota((half_rows, edge_z), 0), iota((half_rows, edge_z), 1)
        hop = k // half_y % half + k // (half * half_y) * (bz_len + half) - i % bz_len
        inside = k % half_y == i // bz_len
        mfz[layer, :, half_rows:] = banded(layer, 2, False, hop, inside)
        mbz[layer, :, half_rows:] = banded(layer, 2, True, hop, inside)
        return carry

    lax.fori_loop(0, num_layers, build, 0)
    i, k = iota((edge_z, half_rows), 0), iota((edge_z, half_rows), 1)
    z_edge = i // half_y % half + i // (half * half_y) * (bz_len - half)
    sel[...] = jnp.where((k // bz_len == i % half_y) & (k % bz_len == z_edge), 1.0, 0.0).astype(BF16)

    for layer in range(num_layers):
        vols[layer, planes + half:] = jnp.zeros((half,) + vols.shape[2:], BF16)
        d1[layer, planes + half:] = jnp.zeros((half,) + d1.shape[2:], BF16)

    def zero_halo(halo, where, side):
        @pl.when(where)
        def _():
            def clear(j, carry):
                for stage in range(2 * num_layers):
                    halo[stage, j, :, side] = jnp.zeros(halo.shape[2:3] + halo.shape[4:], BF16)
                return carry
            lax.fori_loop(0, planes, clear, 0)

    zero_halo(yh, my_y == 0, 0)
    zero_halo(yh, my_y == ny - 1, 1)
    zero_halo(zh, my_z == 0, 0)
    zero_halo(zh, my_z == nz - 1, 1)
    gwx[...] = jnp.zeros(gwx.shape, F32)

    pl.semaphore_wait(barrier, group)

    def y_copies(src, stage, tau):
        at = pl.ds(tau * PLANES, PLANES)
        up = pltpu.make_async_remote_copy(
            src_ref=src.at[at, pl.ds(rows - edge_y, edge_y)], dst_ref=yh.at[stage, at, 0, 0],
            send_sem=ysend.at[stage, tau, 0], recv_sem=yrecv.at[stage, tau, 0], device_id=y_next, device_id_type=MESH)
        dn = pltpu.make_async_remote_copy(
            src_ref=src.at[at, pl.ds(0, edge_y)], dst_ref=yh.at[stage, at, 0, 1],
            send_sem=ysend.at[stage, tau, 1], recv_sem=yrecv.at[stage, tau, 1], device_id=y_prev, device_id_type=MESH)
        return up, dn, y_lo, y_hi

    def z_copies(stage, tau):
        at = pl.ds(tau * PLANES, PLANES)
        up = pltpu.make_async_remote_copy(
            src_ref=zs.at[stage, at, :, 1], dst_ref=zh.at[stage, at, :, 0],
            send_sem=zsend.at[stage, tau, 0], recv_sem=zrecv.at[stage, tau, 0], device_id=z_next, device_id_type=MESH)
        dn = pltpu.make_async_remote_copy(
            src_ref=zs.at[stage, at, :, 0], dst_ref=zh.at[stage, at, :, 1],
            send_sem=zsend.at[stage, tau, 1], recv_sem=zrecv.at[stage, tau, 1], device_id=z_prev, device_id_type=MESH)
        return up, dn, z_lo, z_hi

    def start(copies):
        up, dn, has_lo, has_hi = copies
        pl.when(has_hi)(up.start)
        pl.when(has_lo)(dn.start)

    def wait(copies):
        up, dn, has_lo, has_hi = copies

        @pl.when(has_hi)
        def _():
            up.wait_send()
            dn.wait_recv()

        @pl.when(has_lo)
        def _():
            dn.wait_send()
            up.wait_recv()

    def x_copy(buf, stage, layer, j):
        src = vol.at[x_of(j)] if stage == 0 else buf.at[layer, half + j]
        return pltpu.make_async_remote_copy(
            src_ref=src, dst_ref=buf.at[layer, half - 1 - j],
            send_sem=xsend.at[stage, j], recv_sem=xrecv.at[stage, j], device_id=x_peer, device_id_type=MESH)

    def start_x(buf, stage, layer, tau):
        for task in range(-(-half // PLANES)):
            @pl.when(tau == task)
            def _():
                for j in range(task * PLANES, min(half, (task + 1) * PLANES)):
                    x_copy(buf, stage, layer, j).start()

    def wait_x(buf, stage, layer, tau):
        @pl.when(tau == 0)
        def _():
            for j in range(half):
                x_copy(buf, stage, layer, j).wait()

    for j in range(half):
        x_copy(vols, 0, 0, j).start()

    def wait_in(j, carry):
        in_copy(j).wait()
        return carry

    lax.fori_loop(0, planes, wait_in, 0)

    def x_pass(matrix, buf, layer, tau, emit):
        for group in range(rows // GROUP):
            at = pl.ds(group * GROUP, GROUP)
            source = jnp.concatenate([buf[layer, tau * PLANES + p, at, :] for p in range(PLANES + 2 * half)], axis=0)
            total = dot(matrix[layer], source)
            for p in range(PLANES):
                emit(tau * PLANES + p, at, total[p * GROUP:(p + 1) * GROUP])

    def y_source(buf, stage, j, part):
        if part == 0:
            return jnp.concatenate([yh[stage, j, 0, 0], buf[j, :half_rows + edge_y]], axis=0)
        return jnp.concatenate([buf[j, half_rows - edge_y:], yh[stage, j, 0, 1]], axis=0)

    def z_source(buf, stage, j, part):
        halo = zh[stage, j, part]
        return jnp.concatenate([buf[j, part * half_rows:(part + 1) * half_rows], halo.reshape(edge_z, halo.shape[2])], axis=0)

    def put_z_edge(stage, j, part, value):
        zs[stage, j, part] = value.reshape(zs.shape[3:])

    def fx(layer, tau):
        wait_x(vols, layer, layer, tau)

        def emit(j, at, total):
            a1[j, at, :] = total.astype(BF16)

        x_pass(mfx, vols, layer, tau, emit)
        start(y_copies(a1, layer, tau))

    def fy(layer, tau):
        wait(y_copies(a1, layer, tau))
        for p in range(PLANES):
            j = tau * PLANES + p
            for part in range(2):
                total = dot(mfy[layer], y_source(a1, layer, j, part)).astype(BF16)
                a2[j, part * half_rows:(part + 1) * half_rows] = total[:half_rows]
                put_z_edge(layer, j, part, total[half_rows:])
        start(z_copies(layer, tau))

    def fz(layer, tau):
        wait(z_copies(layer, tau))
        bias = b[layer, :][None, :]
        for p in range(PLANES):
            j = tau * PLANES + p
            for part in range(2):
                at = slice(part * half_rows, (part + 1) * half_rows)
                filtered = dot(mfz[layer], z_source(a2, layer, j, part)).astype(BF16)
                a3[layer, j, at] = filtered
                pre = dot(filtered, w[layer])
                for first in range(0, half_rows, CHUNK):
                    at = slice(part * half_rows + first, part * half_rows + first + CHUNK)
                    z = pre[first:first + CHUNK] + bias
                    cdf = 0.5 * lax.erf(z * SQRT_HALF) + 0.5
                    gp[layer, j, at] = cdf + z * (jnp.exp2((z * z) * -HALF_LOG2_E) * INV_SQRT_2PI)
                    if layer + 1 < num_layers:
                        vols[layer + 1, j + half, at] = (vols[layer, j + half, at].astype(F32) + z * cdf).astype(BF16)
        if layer + 1 < num_layers:
            start_x(vols, layer + 1, layer + 1, tau)

    def bs(layer, tau):
        stage = num_layers + layer
        if layer == num_layers - 1:
            for p in range(PLANES):
                cot_copy(tau * PLANES + p).wait()
        total_b = gwx[layer, 0, part_x:]
        for p in range(PLANES):
            j = tau * PLANES + p
            for part in range(2):
                chunks = []
                for first in range(part * half_rows, (part + 1) * half_rows, CHUNK):
                    at = slice(first, first + CHUNK)
                    scaled = gp[layer, j, at] * grad[j, at].astype(F32)
                    total_b = total_b + jnp.sum(scaled.reshape(CHUNK // 8, 8, scaled.shape[1]), axis=0)
                    chunks.append(scaled.astype(BF16))
                    sb[p, at] = chunks[-1]
                at = slice(part * half_rows, (part + 1) * half_rows)
                rounded = jnp.concatenate(chunks, axis=0)
                mixed = lax.dot_general(rounded, w[layer], (((1,), (1,)), ((), ())), preferred_element_type=F32).astype(BF16)
                d3[j, at] = mixed
                put_z_edge(stage, j, part, dot(sel[...], mixed).astype(BF16))
        gwx[layer, 0, part_x:] = total_b
        start(z_copies(stage, tau))
        channels = w.shape[1]
        product = lax.dot_general(
            a3[layer, pl.ds(tau * PLANES, PLANES)].reshape(PLANES * rows, channels), sb[...].reshape(PLANES * rows, channels),
            (((0,), (0,)), ((), ())), preferred_element_type=F32)
        for side in range(nx):
            gwx[layer, side, :part_x] += product[side * part_x:(side + 1) * part_x]

    def bz(layer, tau):
        stage = num_layers + layer
        wait(z_copies(stage, tau))
        for p in range(PLANES):
            j = tau * PLANES + p
            for part in range(2):
                d2[j, part * half_rows:(part + 1) * half_rows] = dot(mbz[layer], z_source(d3, stage, j, part)).astype(BF16)
        start(y_copies(d2, stage, tau))

    def by(layer, tau):
        stage = num_layers + layer
        wait(y_copies(d2, stage, tau))
        for p in range(PLANES):
            j = tau * PLANES + p
            for part in range(2):
                d1[layer, j + half, part * half_rows:(part + 1) * half_rows] = dot(mby[layer], y_source(d2, stage, j, part)).astype(BF16)
        start_x(d1, stage, layer, tau)

    def out_copy(j):
        return pltpu.make_async_copy(grad.at[j], out.at[x_of(j)], out_sem.at[j])

    def bx(layer, tau):
        wait_x(d1, num_layers + layer, layer, tau)

        def emit(j, at, total):
            grad[j, at, :] = (grad[j, at, :].astype(F32) + total).astype(BF16)

        x_pass(mbx, d1, layer, tau, emit)
        if layer == 0:
            for p in range(PLANES):
                out_copy(tau * PLANES + p).start()

    def sum_copy(layer, phase, offset, src, dst, device):
        return pltpu.make_async_remote_copy(
            src_ref=src, dst_ref=dst, send_sem=sum_send.at[layer, phase, offset], recv_sem=sum_recv.at[layer, phase, offset],
            device_id=device, device_id_type=MESH)

    def core_copy(layer, phase):
        if phase == 0:
            return sum_copy(layer, 0, 0, gwx.at[layer, 1 - my_x], rx.at[layer], x_peer)
        at = pl.ds(pl.multiple_of(my_x * part_x, part_x), part_x)
        return sum_copy(layer, 3, 0, gw_out.at[layer, at], gw_out.at[layer, at], x_peer)

    def own_rows():
        return pl.ds(pl.multiple_of(my_x * part_x + my_q * part_q, part_q), part_q)

    def chip_copy(layer, phase, offset):
        other = lax.rem(my_q + offset, group)
        if phase == 1:
            return sum_copy(layer, 1, offset, rq.at[layer, 1, other], rq.at[layer, 0, my_q], chip(other))
        return sum_copy(layer, 2, offset, gw_out.at[layer, own_rows()], gw_out.at[layer, own_rows()], chip(other))

    def each_chip(layer, phase, act):
        def body(offset, carry):
            act(chip_copy(layer, phase, offset))
            return carry
        lax.fori_loop(1, group, body, 0)

    def r0(layer, tau):
        gwx[layer, 1, part_x:] = gwx[layer, 0, part_x:]
        core_copy(layer, 0).start()

    def r1(layer, tau):
        core_copy(layer, 0).wait()
        bias = gwx[layer, my_x, part_x:] + rx[layer, part_x:]
        for q in range(group):
            at = slice(q * part_q, (q + 1) * part_q)
            rq[layer, 1, q, :part_q] = gwx[layer, my_x, at] + rx[layer, at]
            rq[layer, 1, q, part_q:] = bias
        rq[layer, 0, my_q] = rq[layer, 1, my_q]
        each_chip(layer, 1, lambda copy: copy.start())

    def r2(layer, tau):
        each_chip(layer, 1, lambda copy: copy.wait())
        total = rq[layer, 0, 0]
        for q in range(1, group):
            total = total + rq[layer, 0, q]
        gw_out[layer, own_rows()] = total[:part_q]
        gb_out[layer, :] = jnp.sum(total[part_q:], axis=0)
        each_chip(layer, 2, lambda copy: copy.start())

    def r3(layer, tau):
        each_chip(layer, 2, lambda copy: copy.wait())
        core_copy(layer, 3).start()

    def r4(layer, tau):
        core_copy(layer, 3).wait()

    tasks = {'r0': r0, 'r1': r1, 'r2': r2, 'r3': r3, 'r4': r4, 'fx': fx, 'fy': fy, 'fz': fz, 'bs': bs, 'bz': bz, 'by': by, 'bx': bx}
    stages, last = stage_list(num_layers, nt)

    def step(s, carry):
        for kind, layer, first in stages:
            tau = s - first

            @pl.when((tau >= 0) & (tau < (1 if kind[0] == 'r' else nt)))
            def _():
                tasks[kind](layer, tau)
        return carry

    lax.fori_loop(0, last, step, 0)

    def wait_out(j, carry):
        out_copy(j).wait()
        return carry

    lax.fori_loop(0, planes, wait_out, 0)


def solution(mesh):
    names = ('gx', 'gy', 'gz')
    nx, ny, nz = (mesh.shape[axis_name] for axis_name in names)
    assert nx == 2
    vol_spec = P('dp', 'gx', 'gy', 'gz')

    def local_step(volume, cot_out, filter_taps, w_mix, b_mix):
        channels, planes, by_len, bz_len = volume.shape
        num_layers, _, num_taps = filter_taps.shape
        half = (num_taps - 1) // 2
        rows = by_len * bz_len
        edge_y, edge_z = half * bz_len, half * by_len
        nt = planes // PLANES
        stages = 2 * num_layers
        part_x = channels // nx
        part_q = part_x // (ny * nz)

        def to_rows(block):
            return jnp.transpose(block, (1, 2, 3, 0)).reshape(planes, rows, channels)

        any_spec = pl.BlockSpec(memory_space=pl.ANY)
        vmem_spec = pl.BlockSpec(memory_space=pltpu.VMEM)
        smem_spec = pl.BlockSpec(memory_space=pltpu.SMEM)
        block = (planes, rows, channels)
        dma = pltpu.SemaphoreType.DMA
        grad_rows, grad_w, grad_b = pl.pallas_call(
            functools.partial(kernel, (nx, ny, nz, num_layers, num_taps, by_len, bz_len)),
            out_shape=(
                jax.ShapeDtypeStruct(block, BF16),
                jax.ShapeDtypeStruct((num_layers, channels, channels), F32),
                jax.ShapeDtypeStruct((num_layers, channels), F32),
            ),
            in_specs=[any_spec, any_spec, smem_spec, vmem_spec, vmem_spec],
            out_specs=(any_spec, vmem_spec, vmem_spec),
            scratch_shapes=[
                pltpu.VMEM((num_layers, planes + 2 * half, rows, channels), BF16),
                pltpu.VMEM(block, BF16),
                pltpu.VMEM(block, BF16),
                pltpu.VMEM((num_layers,) + block, BF16),
                pltpu.VMEM((num_layers,) + block, F32),
                pltpu.VMEM(block, BF16),
                pltpu.VMEM(block, BF16),
                pltpu.VMEM(block, BF16),
                pltpu.VMEM((num_layers, planes + 2 * half, rows, channels), BF16),
                pltpu.VMEM((PLANES, rows, channels), BF16),
                pltpu.VMEM((stages, planes, 1, 2, edge_y, channels), BF16),
                pltpu.VMEM((stages, planes, 2, 2, edge_z // 2, channels), BF16),
                pltpu.VMEM((stages, planes, 2, 2, edge_z // 2, channels), BF16),
                pltpu.VMEM((num_layers, PLANES * GROUP, (PLANES + 2 * half) * GROUP), BF16),
                pltpu.VMEM((num_layers, rows // 2 + edge_z, rows // 2 + 2 * edge_y), BF16),
                pltpu.VMEM((num_layers, rows // 2, rows // 2 + edge_z), BF16),
                pltpu.VMEM((num_layers, PLANES * GROUP, (PLANES + 2 * half) * GROUP), BF16),
                pltpu.VMEM((num_layers, rows // 2, rows // 2 + 2 * edge_y), BF16),
                pltpu.VMEM((num_layers, rows // 2, rows // 2 + edge_z), BF16),
                pltpu.VMEM((edge_z, rows // 2), BF16),
                pltpu.VMEM((num_layers, nx, part_x + 8, channels), F32),
                pltpu.VMEM((num_layers, part_x + 8, channels), F32),
                pltpu.VMEM((num_layers, 2, ny * nz, part_q + 8, channels), F32),
                dma((num_layers, 4, ny * nz)), dma((num_layers, 4, ny * nz)),
                dma((planes,)), dma((planes,)), dma((planes,)),
                dma((stages, nt, 2)), dma((stages, nt, 2)), dma((stages, nt, 2)), dma((stages, nt, 2)),
                dma((stages, half)), dma((stages, half)),
            ],
            compiler_params=pltpu.CompilerParams(
                collective_id=0, has_side_effects=True, vmem_limit_bytes=64000 * 1024),
            name='stack',
        )(to_rows(volume), to_rows(cot_out), filter_taps, w_mix, b_mix)
        grad_volume = jnp.transpose(grad_rows.reshape(planes, by_len, bz_len, channels), (3, 0, 1, 2))
        return grad_volume, grad_w, grad_b

    return jax.shard_map(local_step, mesh=mesh, in_specs=(vol_spec, vol_spec, P(), P(), P()), out_specs=(vol_spec, P('dp'), P('dp')), check_vma=False)
```

```python
import functools

import jax
import jax.numpy as jnp
from jax import lax
from jax.experimental import pallas as pl
from jax.experimental.pallas import tpu as pltpu
from jax.sharding import PartitionSpec as P

MESH = pl.DeviceIdType.MESH
PLANES = 4
LAG = 2
SUM_STEPS = ((0, 1, 2, 3, 4), (0, 2, 5, 7, 8), (0, 2, 5, 7, 9))
XLAG = 1
F32 = jnp.float32
BF16 = jnp.bfloat16
SQRT_HALF = 0.7071067811865476
HALF_LOG2_E = 0.7213475204444817
CHUNK = 16
INV_SQRT_2PI = 0.3989422804014327


def dot(a, b):
    return jnp.dot(a, b, preferred_element_type=F32)


def stage_list(num_layers, nt):
    stages = []
    start = 0
    for layer in range(num_layers):
        stages.append(('fx', layer, start))
        stages.append(('fz', layer, start + LAG))
        start += LAG + (XLAG if layer + 1 < num_layers else 0)
    for layer in reversed(range(num_layers)):
        stages.append(('bs', layer, start))
        stages.append(('by', layer, start + LAG))
        stages.append(('bx', layer, start + LAG + XLAG))
        start += LAG + XLAG
    stages[1:1] = [('m', layer, layer) for layer in range(num_layers)]
    for kind, layer, first in list(stages):
        if kind == 'bs':
            stages += [('r%d' % phase, layer, first + nt - 1 + SUM_STEPS[min(layer, 2)][phase]) for phase in range(5)]
    return stages, max(first + (1 if kind[0] in 'rm' else nt) for kind, _, first in stages)


def kernel(sizes, vol, cot, taps, w, b, out, gw_out, gb_out,
           vols, a1, a3, gp, grad, d3, d1, sb, second, yh, zh, zs, wt,
           mfx, mfy, mfyh, mfz, mbx, mby, mbz, mbzh, sel,
           gwx, rx, rq, sum_send, sum_recv,
           in_sem, cot_sem, out_sem, send_sem, recv_sem, xsend, xrecv):
    nx, ny, nz, num_layers, num_taps, by_len, bz_len = sizes
    half = (num_taps - 1) // 2
    planes = a1.shape[0]
    rows = by_len * bz_len
    edge_y = half * bz_len
    pairs = by_len // half
    edge = PLANES * half * half
    nt = planes // PLANES
    part_x = w.shape[1] // nx
    group = ny * nz
    part_q = part_x // group
    my_x, my_y, my_z = lax.axis_index('gx'), lax.axis_index('gy'), lax.axis_index('gz')
    y_lo, y_hi = my_y > 0, my_y < ny - 1
    z_lo, z_hi = my_z > 0, my_z < nz - 1
    x_peer = {'gx': 1 - my_x}

    def x_of(j):
        return my_x * j + (1 - my_x) * (planes - 1 - j)

    my_q = my_z * ny + my_y

    def chip(q):
        return {'gy': lax.rem(q, ny), 'gz': q // ny}

    barrier = pltpu.get_barrier_semaphore()
    pl.semaphore_signal(barrier, inc=1, device_id=x_peer, device_id_type=MESH)

    def signal_chip(offset, carry):
        pl.semaphore_signal(barrier, inc=1, device_id=chip(lax.rem(my_q + offset, group)), device_id_type=MESH)
        return carry

    lax.fori_loop(1, group, signal_chip, 0)

    def in_copy(j):
        return pltpu.make_async_copy(vol.at[x_of(j)], vols.at[0, j + half], in_sem.at[j])

    def cot_copy(j):
        return pltpu.make_async_copy(cot.at[x_of(j)], grad.at[j], cot_sem.at[j])

    def start_in(j, carry):
        in_copy(j).start()
        cot_copy(j).start()
        return carry

    lax.fori_loop(0, planes, start_in, 0)

    half_y, half_rows = by_len // 2, rows // 2

    def iota(shape, axis):
        return lax.broadcasted_iota(jnp.int32, shape, axis)

    def banded(layer, axis, back, hop, inside):
        total = jnp.zeros(hop.shape, F32)
        for t in range(num_taps):
            tap = taps[layer, axis, num_taps - 1 - t if back else t]
            if axis == 0:
                tap = jnp.where(my_x == 1, tap, taps[layer, axis, t if back else num_taps - 1 - t])
            total = jnp.where(hop == t, tap, total)
        return jnp.where(inside, total, 0.0).astype(BF16)

    def edge_index(e):
        return e // edge, e % edge // (half * half), e % (half * half) // half, e % half

    def grid(row_count, column_count):
        return iota((row_count, column_count), 0), iota((row_count, column_count), 1)

    def build_forward(layer, carry):
        i, k = grid(PLANES * edge_y, (PLANES + 2 * half) * edge_y)
        mfx[layer, :PLANES * edge_y] = banded(layer, 0, False, k // edge_y - i // edge_y, k % edge_y == i % edge_y)
        i, k = grid(2 * edge, (PLANES + 2 * half) * edge_y)
        side, plane, depth, y = edge_index(i)
        z = depth + side * (bz_len - half)
        mfx[layer, PLANES * edge_y:] = banded(layer, 0, False, k // edge_y - plane, k % edge_y == y * bz_len + z)
        i, k = grid(half_rows, half_rows + 2 * edge_y)
        mfy[layer] = banded(layer, 1, False, k // bz_len - i // bz_len, k % bz_len == i % bz_len)
        i, k = grid(PLANES * half * by_len, (pairs + 2) * edge)
        side, plane, depth, y = edge_index(k % edge)
        y = (k // edge - 1) * half + y
        i_y = i // (half * half_y) % 2 * half_y + i % half_y
        inside = (plane == i // (half * by_len)) & (depth == i // half_y % half)
        mfyh[layer] = banded(layer, 1, False, y - i_y + half, inside)
        i, k = grid(half_rows, half_rows)
        mfz[layer, :, :half_rows] = banded(layer, 2, False, k % bz_len - i % bz_len + half, k // bz_len == i // bz_len)
        i, k = grid(half_rows, half * by_len)
        hop = k // half_y % half + k // (half * half_y) * (bz_len + half) - i % bz_len
        mfz[layer, :, half_rows:] = banded(layer, 2, False, hop, k % half_y == i // bz_len)
        return carry

    def build_backward(layer, tau):
        i, k = grid(PLANES * edge_y, (PLANES + 2 * half) * edge_y)
        mbx[layer] = banded(layer, 0, True, k // edge_y - i // edge_y, k % edge_y == i % edge_y)
        i, k = grid(half_rows, half_rows + 2 * edge_y)
        mby[layer] = banded(layer, 1, True, k // bz_len - i // bz_len, k % bz_len == i % bz_len)
        i, k = grid(half_rows, half_rows)
        own_back = banded(layer, 2, True, k % bz_len - i % bz_len + half, k // bz_len == i // bz_len)
        i, k = grid(half_rows, pairs * edge)
        side, (_, plane, depth, y) = k // (pairs * edge // 2), edge_index(k % edge)
        y = k // edge % (pairs // 2) * half + y
        hop = depth + side * (bz_len + half) - i % bz_len
        for p in range(PLANES):
            mbz[layer, p, :, :half_rows] = own_back
            mbz[layer, p, :, half_rows:] = banded(layer, 2, True, hop, (y == i // bz_len) & (plane == p))
        i, k = grid(PLANES * edge_y, PLANES * edge_y)
        mbzh[layer, :, :PLANES * edge_y] = banded(layer, 2, True, k % bz_len - i % bz_len + half, k // bz_len == i // bz_len)
        i, k = grid(PLANES * edge_y, 2 * edge)
        side, plane, depth, y = edge_index(k)
        hop = depth + side * (bz_len + half) - i % bz_len
        mbzh[layer, :, PLANES * edge_y:] = banded(layer, 2, True, hop, (plane == i // edge_y) & (y == i // bz_len % half))
        wt[layer] = jnp.transpose(w[layer].astype(F32)).astype(BF16)

    lax.fori_loop(0, num_layers, build_forward, 0)
    i, k = grid(2 * edge, PLANES * edge_y)
    side, plane, depth, y = edge_index(i)
    z = depth + side * (bz_len - half)
    sel[...] = jnp.where((k // edge_y == plane) & (k % edge_y == y * bz_len + z), 1.0, 0.0).astype(BF16)

    for layer in range(num_layers):
        vols[layer, planes + half:] = jnp.zeros((half,) + vols.shape[2:], BF16)
        d1[layer, planes + half:] = jnp.zeros((half,) + d1.shape[2:], BF16)

    def zero_halo(where, clear):
        @pl.when(where)
        def _():
            def body(stage, carry):
                clear(stage)
                return carry
            lax.fori_loop(0, 2 * num_layers, body, 0)

    def clear_y(side):
        def clear(stage):
            yh[stage, :, side] = jnp.zeros(yh.shape[1:2] + yh.shape[3:], BF16)
            zh[stage, :, :, side * (pairs + 1)] = jnp.zeros(zh.shape[1:3] + zh.shape[4:], BF16)
        return clear

    def clear_z(side):
        def clear(stage):
            zh[stage, :, side] = jnp.zeros(zh.shape[1:2] + zh.shape[3:], BF16)
        return clear

    zero_halo(my_y == 0, clear_y(0))
    zero_halo(my_y == ny - 1, clear_y(1))
    zero_halo(my_z == 0, clear_z(0))
    zero_halo(my_z == nz - 1, clear_z(1))
    gwx[...] = jnp.zeros(gwx.shape, F32)

    pl.semaphore_wait(barrier, group)

    def exchange(src, stage, tau):
        at = pl.ds(tau * PLANES, PLANES)
        y_near, z_near = {0: None, 1: y_hi, -1: y_lo}, {0: None, 1: z_hi, -1: z_lo}
        entries = []
        for dy, dz in ((1, 0), (-1, 0), (0, 1), (0, -1), (1, 1), (1, -1), (-1, 1), (-1, -1)):
            device = {}
            if dy:
                device['gy'] = jnp.clip(my_y + dy, 0, ny - 1)
            if dz:
                device['gz'] = jnp.clip(my_z + dz, 0, nz - 1)
            if dz == 0:
                source = src.at[at, pl.ds(rows - edge_y if dy > 0 else 0, edge_y)]
                target = yh.at[stage, at, 0 if dy > 0 else 1]
            else:
                from_side, to_side = (1, 0) if dz > 0 else (0, 1)
                if dy == 0:
                    source, target = zs.at[stage, tau, from_side], zh.at[stage, tau, to_side, pl.ds(1, pairs)]
                else:
                    source = zs.at[stage, tau, from_side, pairs - 1 if dy > 0 else 0]
                    target = zh.at[stage, tau, to_side, 0 if dy > 0 else pairs + 1]
            copy = pltpu.make_async_remote_copy(
                src_ref=source, dst_ref=target, send_sem=send_sem.at[stage, tau, len(entries)],
                recv_sem=recv_sem.at[stage, tau, len(entries)], device_id=device, device_id_type=MESH)
            sends = [near for near in (y_near[dy], z_near[dz]) if near is not None]
            receives = [near for near in (y_near[-dy], z_near[-dz]) if near is not None]
            entries.append((copy, functools.reduce(jnp.logical_and, sends), functools.reduce(jnp.logical_and, receives)))
        return entries

    def start(entries):
        for copy, sends, _ in entries:
            pl.when(sends)(copy.start)

    def wait(entries):
        for copy, sends, receives in entries:
            pl.when(sends)(copy.wait_send)
            pl.when(receives)(copy.wait_recv)

    def x_copy(buf, stage, layer, j):
        src = vol.at[x_of(j)] if stage == 0 else buf.at[layer, half + j]
        return pltpu.make_async_remote_copy(
            src_ref=src, dst_ref=buf.at[layer, half - 1 - j],
            send_sem=xsend.at[stage, j], recv_sem=xrecv.at[stage, j], device_id=x_peer, device_id_type=MESH)

    def start_x(buf, stage, layer, tau):
        for task in range(-(-half // PLANES)):
            @pl.when(tau == task)
            def _():
                for j in range(task * PLANES, min(half, (task + 1) * PLANES)):
                    x_copy(buf, stage, layer, j).start()

    def wait_x(buf, stage, layer, tau):
        @pl.when(tau == 0)
        def _():
            for j in range(half):
                x_copy(buf, stage, layer, j).wait()

    for j in range(half):
        x_copy(vols, 0, 0, j).start()

    def wait_in(j, carry):
        in_copy(j).wait()
        return carry

    lax.fori_loop(0, planes, wait_in, 0)

    def x_source(buf, layer, tau, group):
        at = pl.ds(group * edge_y, edge_y)
        return jnp.concatenate([buf[layer, tau * PLANES + p, at, :] for p in range(PLANES + 2 * half)], axis=0)

    def fx(layer, tau):
        wait_x(vols, layer, layer, tau)
        for group in range(pairs):
            total = dot(mfx[layer], x_source(vols, layer, tau, group)).astype(BF16)
            for p in range(PLANES):
                a1[tau * PLANES + p, group * edge_y:(group + 1) * edge_y] = total[p * edge_y:(p + 1) * edge_y]
            for side in range(2):
                first = PLANES * edge_y + side * edge
                zs[layer, tau, side, group] = total[first:first + edge]
        start(exchange(a1, layer, tau))

    def fz(layer, tau):
        wait(exchange(a1, layer, tau))
        bias = b[layer, :][None, :]
        channels = w.shape[1]
        z_halo = [dot(mfyh[layer], zh[layer, tau, side].reshape((pairs + 2) * edge, channels)).astype(BF16) for side in range(2)]
        for p in range(PLANES):
            j = tau * PLANES + p
            for part in range(2):
                if part == 0:
                    source = jnp.concatenate([yh[layer, j, 0], a1[j, :half_rows + edge_y]], axis=0)
                else:
                    source = jnp.concatenate([a1[j, half_rows - edge_y:], yh[layer, j, 1]], axis=0)
                second[p, part] = dot(mfy[layer], source).astype(BF16)
        for p in range(PLANES):
            for part in range(2):
                size = half * half_y
                first = (p * 2 + part) * size
                source = jnp.concatenate([second[p, part]] + [halo[first:first + size] for halo in z_halo], axis=0)
                a3[layer, tau * PLANES + p, part * half_rows:(part + 1) * half_rows] = dot(mfz[layer], source).astype(BF16)
        for p in range(PLANES):
            j = tau * PLANES + p
            for part in range(2):
                pre = dot(a3[layer, j, part * half_rows:(part + 1) * half_rows], w[layer])
                for first in range(0, half_rows, CHUNK):
                    at = slice(part * half_rows + first, part * half_rows + first + CHUNK)
                    z = pre[first:first + CHUNK] + bias
                    cdf = 0.5 * lax.erf(z * SQRT_HALF) + 0.5
                    gp[layer, j, at] = cdf + z * (jnp.exp2((z * z) * -HALF_LOG2_E) * INV_SQRT_2PI)
                    if layer + 1 < num_layers:
                        vols[layer + 1, j + half, at] = (vols[layer, j + half, at].astype(F32) + z * cdf).astype(BF16)
        if layer + 1 < num_layers:
            start_x(vols, layer + 1, layer + 1, tau)

    def bs(layer, tau):
        stage = num_layers + layer
        channels = w.shape[1]
        if layer == num_layers - 1:
            for p in range(PLANES):
                cot_copy(tau * PLANES + p).wait()
        total_b = gwx[layer, 0, part_x:]
        for group in range(pairs):
            chunks = []
            for p in range(PLANES):
                j = tau * PLANES + p
                at = slice(group * edge_y, (group + 1) * edge_y)
                scaled = gp[layer, j, at] * grad[j, at].astype(F32)
                total_b = total_b + jnp.sum(scaled.reshape(edge_y // 8, 8, channels), axis=0)
                chunks.append(scaled.astype(BF16))
                sb[p, at] = chunks[-1]
            mixed = dot(jnp.concatenate(chunks, axis=0), wt[layer]).astype(BF16)
            for p in range(PLANES):
                d3[tau * PLANES + p, group * edge_y:(group + 1) * edge_y] = mixed[p * edge_y:(p + 1) * edge_y]
        for group in range(pairs):
            mixed = jnp.concatenate([d3[tau * PLANES + p, group * edge_y:(group + 1) * edge_y] for p in range(PLANES)], axis=0)
            edges = dot(sel[...], mixed).astype(BF16)
            for side in range(2):
                zs[stage, tau, side, group] = edges[side * edge:(side + 1) * edge]
        gwx[layer, 0, part_x:] = total_b
        start(exchange(d3, stage, tau))
        product = lax.dot_general(
            a3[layer, pl.ds(tau * PLANES, PLANES)].reshape(PLANES * rows, channels), sb[...].reshape(PLANES * rows, channels),
            (((0,), (0,)), ((), ())), preferred_element_type=F32)
        for side in range(nx):
            gwx[layer, side, :part_x] += product[side * part_x:(side + 1) * part_x]

    def by(layer, tau):
        stage = num_layers + layer
        channels = w.shape[1]
        wait(exchange(d3, stage, tau))
        y_halo = []
        for side in range(2):
            corner = side * (pairs + 1)
            source = jnp.concatenate(
                [yh[stage, tau * PLANES + p, side] for p in range(PLANES)] + [zh[stage, tau, z_side, corner] for z_side in range(2)], axis=0)
            y_halo.append(dot(mbzh[layer], source).astype(BF16))
        for p in range(PLANES):
            j = tau * PLANES + p
            for part in range(2):
                halves = [zh[stage, tau, side, pl.ds(1 + part * (pairs // 2), pairs // 2)] for side in range(2)]
                source = jnp.concatenate(
                    [d3[j, part * half_rows:(part + 1) * half_rows]] + [halo.reshape(pairs // 2 * edge, channels) for halo in halves], axis=0)
                second[p, part] = dot(mbz[layer, p], source).astype(BF16)
        for p in range(PLANES):
            j = tau * PLANES + p
            at = slice(p * edge_y, (p + 1) * edge_y)
            for part in range(2):
                if part == 0:
                    source = jnp.concatenate([y_halo[0][at], second[p, 0], second[p, 1, :edge_y]], axis=0)
                else:
                    source = jnp.concatenate([second[p, 0, half_rows - edge_y:], second[p, 1], y_halo[1][at]], axis=0)
                d1[layer, j + half, part * half_rows:(part + 1) * half_rows] = dot(mby[layer], source).astype(BF16)
        start_x(d1, stage, layer, tau)

    def out_copy(j):
        return pltpu.make_async_copy(grad.at[j], out.at[x_of(j)], out_sem.at[j])

    def bx(layer, tau):
        wait_x(d1, num_layers + layer, layer, tau)

        for group in range(pairs):
            at = slice(group * edge_y, (group + 1) * edge_y)
            total = dot(mbx[layer], x_source(d1, layer, tau, group))
            for p in range(PLANES):
                j = tau * PLANES + p
                grad[j, at] = (grad[j, at].astype(F32) + total[p * edge_y:(p + 1) * edge_y]).astype(BF16)
        if layer == 0:
            for p in range(PLANES):
                out_copy(tau * PLANES + p).start()

    def sum_copy(layer, phase, offset, src, dst, device):
        return pltpu.make_async_remote_copy(
            src_ref=src, dst_ref=dst, send_sem=sum_send.at[layer, phase, offset], recv_sem=sum_recv.at[layer, phase, offset],
            device_id=device, device_id_type=MESH)

    def core_copy(layer, phase):
        if phase == 0:
            return sum_copy(layer, 0, 0, gwx.at[layer, 1 - my_x], rx.at[layer], x_peer)
        at = pl.ds(pl.multiple_of(my_x * part_x, part_x), part_x)
        return sum_copy(layer, 3, 0, gw_out.at[layer, at], gw_out.at[layer, at], x_peer)

    def own_rows():
        return pl.ds(pl.multiple_of(my_x * part_x + my_q * part_q, part_q), part_q)

    def chip_copy(layer, phase, offset):
        other = lax.rem(my_q + offset, group)
        if phase == 1:
            return sum_copy(layer, 1, offset, rq.at[layer, 1, other], rq.at[layer, 0, my_q], chip(other))
        return sum_copy(layer, 2, offset, gw_out.at[layer, own_rows()], gw_out.at[layer, own_rows()], chip(other))

    def each_chip(layer, phase, act):
        def body(offset, carry):
            act(chip_copy(layer, phase, offset))
            return carry
        lax.fori_loop(1, group, body, 0)

    def r0(layer, tau):
        gwx[layer, 1, part_x:] = gwx[layer, 0, part_x:]
        core_copy(layer, 0).start()

    def r1(layer, tau):
        core_copy(layer, 0).wait()
        bias = gwx[layer, my_x, part_x:] + rx[layer, part_x:]
        for q in range(group):
            at = slice(q * part_q, (q + 1) * part_q)
            rq[layer, 1, q, :part_q] = gwx[layer, my_x, at] + rx[layer, at]
            rq[layer, 1, q, part_q:] = bias
        rq[layer, 0, my_q] = rq[layer, 1, my_q]
        each_chip(layer, 1, lambda copy: copy.start())

    def r2(layer, tau):
        each_chip(layer, 1, lambda copy: copy.wait())
        total = rq[layer, 0, 0]
        for q in range(1, group):
            total = total + rq[layer, 0, q]
        gw_out[layer, own_rows()] = total[:part_q]
        gb_out[layer, :] = jnp.sum(total[part_q:], axis=0)
        each_chip(layer, 2, lambda copy: copy.start())

    def r3(layer, tau):
        each_chip(layer, 2, lambda copy: copy.wait())
        core_copy(layer, 3).start()

    def r4(layer, tau):
        core_copy(layer, 3).wait()

    tasks = {'r0': r0, 'r1': r1, 'r2': r2, 'r3': r3, 'r4': r4, 'm': build_backward, 'fx': fx, 'fz': fz, 'bs': bs, 'by': by, 'bx': bx}
    stages, last = stage_list(num_layers, nt)

    def step(s, carry):
        for kind, layer, first in stages:
            tau = s - first

            @pl.when((tau >= 0) & (tau < (1 if kind[0] in 'rm' else nt)))
            def _():
                tasks[kind](layer, tau)
        return carry

    lax.fori_loop(0, last, step, 0)

    def wait_out(j, carry):
        out_copy(j).wait()
        return carry

    lax.fori_loop(0, planes, wait_out, 0)


def solution(mesh):
    names = ('gx', 'gy', 'gz')
    nx, ny, nz = (mesh.shape[axis_name] for axis_name in names)
    assert nx == 2
    vol_spec = P('dp', 'gx', 'gy', 'gz')

    def local_step(volume, cot_out, filter_taps, w_mix, b_mix):
        channels, planes, by_len, bz_len = volume.shape
        num_layers, _, num_taps = filter_taps.shape
        half = (num_taps - 1) // 2
        rows = by_len * bz_len
        edge_y, pairs, edge = half * bz_len, by_len // half, PLANES * half * half
        half_rows = rows // 2
        nt = planes // PLANES
        stages = 2 * num_layers
        part_x = channels // nx
        part_q = part_x // (ny * nz)

        def to_rows(block):
            return jnp.transpose(block, (1, 2, 3, 0)).reshape(planes, rows, channels)

        any_spec = pl.BlockSpec(memory_space=pl.ANY)
        vmem_spec = pl.BlockSpec(memory_space=pltpu.VMEM)
        smem_spec = pl.BlockSpec(memory_space=pltpu.SMEM)
        block = (planes, rows, channels)
        dma = pltpu.SemaphoreType.DMA
        grad_rows, grad_w, grad_b = pl.pallas_call(
            functools.partial(kernel, (nx, ny, nz, num_layers, num_taps, by_len, bz_len)),
            out_shape=(
                jax.ShapeDtypeStruct(block, BF16),
                jax.ShapeDtypeStruct((num_layers, channels, channels), F32),
                jax.ShapeDtypeStruct((num_layers, channels), F32),
            ),
            in_specs=[any_spec, any_spec, smem_spec, vmem_spec, vmem_spec],
            out_specs=(any_spec, vmem_spec, vmem_spec),
            scratch_shapes=[
                pltpu.VMEM((num_layers, planes + 2 * half, rows, channels), BF16),
                pltpu.VMEM(block, BF16),
                pltpu.VMEM((num_layers,) + block, BF16),
                pltpu.VMEM((num_layers,) + block, F32),
                pltpu.VMEM(block, BF16),
                pltpu.VMEM(block, BF16),
                pltpu.VMEM((num_layers, planes + 2 * half, rows, channels), BF16),
                pltpu.VMEM((PLANES, rows, channels), BF16),
                pltpu.VMEM((PLANES, 2, half_rows, channels), BF16),
                pltpu.VMEM((stages, planes, 2, edge_y, channels), BF16),
                pltpu.VMEM((stages, nt, 2, pairs + 2, edge, channels), BF16),
                pltpu.VMEM((stages, nt, 2, pairs, edge, channels), BF16),
                pltpu.VMEM((num_layers, channels, channels), BF16),
                pltpu.VMEM((num_layers, PLANES * edge_y + 2 * edge, (PLANES + 2 * half) * edge_y), BF16),
                pltpu.VMEM((num_layers, half_rows, half_rows + 2 * edge_y), BF16),
                pltpu.VMEM((num_layers, PLANES * half * by_len, (pairs + 2) * edge), BF16),
                pltpu.VMEM((num_layers, half_rows, half_rows + half * by_len), BF16),
                pltpu.VMEM((num_layers, PLANES * edge_y, (PLANES + 2 * half) * edge_y), BF16),
                pltpu.VMEM((num_layers, half_rows, half_rows + 2 * edge_y), BF16),
                pltpu.VMEM((num_layers, PLANES, half_rows, half_rows + pairs * edge), BF16),
                pltpu.VMEM((num_layers, PLANES * edge_y, PLANES * edge_y + 2 * edge), BF16),
                pltpu.VMEM((2 * edge, PLANES * edge_y), BF16),
                pltpu.VMEM((num_layers, nx, part_x + 8, channels), F32),
                pltpu.VMEM((num_layers, part_x + 8, channels), F32),
                pltpu.VMEM((num_layers, 2, ny * nz, part_q + 8, channels), F32),
                dma((num_layers, 4, ny * nz)), dma((num_layers, 4, ny * nz)),
                dma((planes,)), dma((planes,)), dma((planes,)),
                dma((stages, nt, 8)), dma((stages, nt, 8)),
                dma((stages, half)), dma((stages, half)),
            ],
            compiler_params=pltpu.CompilerParams(
                collective_id=0, has_side_effects=True, vmem_limit_bytes=64000 * 1024),
            name='stack',
        )(to_rows(volume), to_rows(cot_out), filter_taps, w_mix, b_mix)
        grad_volume = jnp.transpose(grad_rows.reshape(planes, by_len, bz_len, channels), (3, 0, 1, 2))
        return grad_volume, grad_w, grad_b

    return jax.shard_map(local_step, mesh=mesh, in_specs=(vol_spec, vol_spec, P(), P(), P()), out_specs=(vol_spec, P('dp'), P('dp')), check_vma=False)
```

```python
import functools

import jax
import jax.numpy as jnp
from jax import lax
from jax.experimental import pallas as pl
from jax.experimental.pallas import tpu as pltpu
from jax.sharding import PartitionSpec as P

MESH = pl.DeviceIdType.MESH
PLANES = 4
LAG = 3
SUM_STEPS = ((0, 1, 3, 5, 6), (0, 2, 6, 9, 10), (0, 2, 6, 9, 10))
XLAG = 1
F32 = jnp.float32
BF16 = jnp.bfloat16
SQRT_HALF = 0.7071067811865476
HALF_LOG2_E = 0.7213475204444817
CHUNK = 16
INV_SQRT_2PI = 0.3989422804014327


def dot(a, b):
    return jnp.dot(a, b, preferred_element_type=F32)


def stage_list(num_layers, nt):
    stages = []
    start = 0
    for layer in range(num_layers):
        stages.append(('fx', layer, start))
        stages.append(('fz', layer, start + LAG))
        start += LAG + (XLAG if layer + 1 < num_layers else 0)
    for layer in reversed(range(num_layers)):
        stages.append(('bs', layer, start))
        stages.append(('by', layer, start + LAG))
        stages.append(('bx', layer, start + LAG + XLAG))
        start += LAG + XLAG
    stages[1:1] = [('m', layer, layer) for layer in range(num_layers)]
    for kind, layer, first in list(stages):
        if kind == 'bs':
            stages += [('r%d' % phase, layer, first + nt - 1 + SUM_STEPS[min(layer, 2)][phase]) for phase in range(5)]
    return stages, max(first + (1 if kind[0] in 'rm' else nt) for kind, _, first in stages)


def kernel(sizes, vol, cot, taps, w, b, grad, gw_out, gb_out,
           vols, a1, a3, gp, d3, d1, sb, second, yh, zh, zs, wt,
           mfx, mfy, mfyh, mfz, mbx, mby, mbz, mbzh, sel,
           gwx, gb_acc, rx, rq, sum_send, sum_recv,
           in_sem, cot_sem, send_sem, recv_sem, xsend, xrecv):
    nx, ny, nz, num_layers, num_taps, by_len, bz_len = sizes
    half = (num_taps - 1) // 2
    planes = a1.shape[0]
    rows = by_len * bz_len
    edge_y = half * bz_len
    pairs = by_len // half
    edge = PLANES * half * half
    nt = planes // PLANES
    part_x = w.shape[1] // nx
    group = ny * nz
    part_q = part_x // group
    my_x, my_y, my_z = lax.axis_index('gx'), lax.axis_index('gy'), lax.axis_index('gz')
    y_lo, y_hi = my_y > 0, my_y < ny - 1
    z_lo, z_hi = my_z > 0, my_z < nz - 1
    x_peer = {'gx': 1 - my_x}

    def x_of(j):
        return my_x * j + (1 - my_x) * (planes - 1 - j)

    my_q = my_z * ny + my_y

    def chip(q):
        return {'gy': lax.rem(q, ny), 'gz': q // ny}

    barrier = pltpu.get_barrier_semaphore()
    pl.semaphore_signal(barrier, inc=1, device_id=x_peer, device_id_type=MESH)

    def signal_chip(offset, carry):
        pl.semaphore_signal(barrier, inc=1, device_id=chip(lax.rem(my_q + offset, group)), device_id_type=MESH)
        return carry

    lax.fori_loop(1, group, signal_chip, 0)

    def in_copy(j):
        return pltpu.make_async_copy(vol.at[x_of(j)], vols.at[0, j + half], in_sem.at[j])

    cot_copy = pltpu.make_async_copy(cot, grad, cot_sem)

    def start_in(j, carry):
        in_copy(j).start()
        return carry

    lax.fori_loop(0, planes, start_in, 0)
    cot_copy.start()

    half_y, half_rows = by_len // 2, rows // 2

    def iota(shape, axis):
        return lax.broadcasted_iota(jnp.int32, shape, axis)

    def banded(layer, axis, back, hop, inside):
        total = jnp.zeros(hop.shape, F32)
        for t in range(num_taps):
            tap = taps[layer, axis, num_taps - 1 - t if back else t]
            if axis == 0:
                tap = jnp.where(my_x == 1, tap, taps[layer, axis, t if back else num_taps - 1 - t])
            total = jnp.where(hop == t, tap, total)
        return jnp.where(inside, total, 0.0).astype(BF16)

    def edge_index(e):
        return e // edge, e % edge // (half * half), e % (half * half) // half, e % half

    def grid(row_count, column_count):
        return iota((row_count, column_count), 0), iota((row_count, column_count), 1)

    def build_forward(layer, carry):
        i, k = grid(PLANES * edge_y, (PLANES + 2 * half) * edge_y)
        mfx[layer, :PLANES * edge_y] = banded(layer, 0, False, k // edge_y - i // edge_y, k % edge_y == i % edge_y)
        i, k = grid(2 * edge, (PLANES + 2 * half) * edge_y)
        side, plane, depth, y = edge_index(i)
        z = depth + side * (bz_len - half)
        mfx[layer, PLANES * edge_y:] = banded(layer, 0, False, k // edge_y - plane, k % edge_y == y * bz_len + z)
        i, k = grid(half_rows, half_rows + 2 * edge_y)
        mfy[layer] = banded(layer, 1, False, k // bz_len - i // bz_len, k % bz_len == i % bz_len)
        i, k = grid(PLANES * half * by_len, (pairs + 2) * edge)
        side, plane, depth, y = edge_index(k % edge)
        y = (k // edge - 1) * half + y
        i_y = i // (half * half_y) % 2 * half_y + i % half_y
        inside = (plane == i // (half * by_len)) & (depth == i // half_y % half)
        mfyh[layer] = banded(layer, 1, False, y - i_y + half, inside)
        i, k = grid(half_rows, half_rows)
        mfz[layer, :, :half_rows] = banded(layer, 2, False, k % bz_len - i % bz_len + half, k // bz_len == i // bz_len)
        i, k = grid(half_rows, half * by_len)
        hop = k // half_y % half + k // (half * half_y) * (bz_len + half) - i % bz_len
        mfz[layer, :, half_rows:] = banded(layer, 2, False, hop, k % half_y == i // bz_len)
        return carry

    def build_backward(layer, tau):
        i, k = grid(PLANES * edge_y, (PLANES + 2 * half) * edge_y)
        mbx[layer] = banded(layer, 0, True, k // edge_y - i // edge_y, k % edge_y == i % edge_y)
        i, k = grid(half_rows, half_rows + 2 * edge_y)
        mby[layer] = banded(layer, 1, True, k // bz_len - i // bz_len, k % bz_len == i % bz_len)
        i, k = grid(half_rows, half_rows)
        own_back = banded(layer, 2, True, k % bz_len - i % bz_len + half, k // bz_len == i // bz_len)
        i, k = grid(half_rows, pairs * edge)
        side, (_, plane, depth, y) = k // (pairs * edge // 2), edge_index(k % edge)
        y = k // edge % (pairs // 2) * half + y
        hop = depth + side * (bz_len + half) - i % bz_len
        for p in range(PLANES):
            mbz[layer, p, :, :half_rows] = own_back
            mbz[layer, p, :, half_rows:] = banded(layer, 2, True, hop, (y == i // bz_len) & (plane == p))
        i, k = grid(PLANES * edge_y, PLANES * edge_y)
        mbzh[layer, :, :PLANES * edge_y] = banded(layer, 2, True, k % bz_len - i % bz_len + half, k // bz_len == i // bz_len)
        i, k = grid(PLANES * edge_y, 2 * edge)
        side, plane, depth, y = edge_index(k)
        hop = depth + side * (bz_len + half) - i % bz_len
        mbzh[layer, :, PLANES * edge_y:] = banded(layer, 2, True, hop, (plane == i // edge_y) & (y == i // bz_len % half))
        wt[layer] = jnp.transpose(w[layer].astype(F32)).astype(BF16)

    lax.fori_loop(0, num_layers, build_forward, 0)
    i, k = grid(2 * edge, PLANES * edge_y)
    side, plane, depth, y = edge_index(i)
    z = depth + side * (bz_len - half)
    sel[...] = jnp.where((k // edge_y == plane) & (k % edge_y == y * bz_len + z), 1.0, 0.0).astype(BF16)

    for layer in range(num_layers):
        vols[layer, planes + half:] = jnp.zeros((half,) + vols.shape[2:], BF16)
        d1[layer, planes + half:] = jnp.zeros((half,) + d1.shape[2:], BF16)

    def zero_halo(where, clear):
        @pl.when(where)
        def _():
            def body(stage, carry):
                clear(stage)
                return carry
            lax.fori_loop(0, 2 * num_layers, body, 0)

    def clear_y(side):
        def clear(stage):
            yh[stage, :, side] = jnp.zeros(yh.shape[1:2] + yh.shape[3:], BF16)
            zh[stage, :, :, side * (pairs + 1)] = jnp.zeros(zh.shape[1:3] + zh.shape[4:], BF16)
        return clear

    def clear_z(side):
        def clear(stage):
            zh[stage, :, side] = jnp.zeros(zh.shape[1:2] + zh.shape[3:], BF16)
        return clear

    zero_halo(my_y == 0, clear_y(0))
    zero_halo(my_y == ny - 1, clear_y(1))
    zero_halo(my_z == 0, clear_z(0))
    zero_halo(my_z == nz - 1, clear_z(1))
    gwx[...] = jnp.zeros(gwx.shape, F32)
    gb_acc[...] = jnp.zeros(gb_acc.shape, F32)

    pl.semaphore_wait(barrier, group)

    def exchange(src, stage, tau):
        at = pl.ds(tau * PLANES, PLANES)
        y_near, z_near = {0: None, 1: y_hi, -1: y_lo}, {0: None, 1: z_hi, -1: z_lo}
        entries = []
        for dy, dz in ((1, 0), (-1, 0), (0, 1), (0, -1), (1, 1), (1, -1), (-1, 1), (-1, -1)):
            device = {}
            if dy:
                device['gy'] = jnp.clip(my_y + dy, 0, ny - 1)
            if dz:
                device['gz'] = jnp.clip(my_z + dz, 0, nz - 1)
            if dz == 0:
                source = src.at[at, pl.ds(rows - edge_y if dy > 0 else 0, edge_y)]
                target = yh.at[stage, at, 0 if dy > 0 else 1]
            else:
                from_side, to_side = (1, 0) if dz > 0 else (0, 1)
                if dy == 0:
                    source, target = zs.at[stage, tau, from_side], zh.at[stage, tau, to_side, pl.ds(1, pairs)]
                else:
                    source = zs.at[stage, tau, from_side, pairs - 1 if dy > 0 else 0]
                    target = zh.at[stage, tau, to_side, 0 if dy > 0 else pairs + 1]
            copy = pltpu.make_async_remote_copy(
                src_ref=source, dst_ref=target, send_sem=send_sem.at[stage, tau, len(entries)],
                recv_sem=recv_sem.at[stage, tau, len(entries)], device_id=device, device_id_type=MESH)
            sends = [near for near in (y_near[dy], z_near[dz]) if near is not None]
            receives = [near for near in (y_near[-dy], z_near[-dz]) if near is not None]
            entries.append((copy, functools.reduce(jnp.logical_and, sends), functools.reduce(jnp.logical_and, receives)))
        return entries

    def start(entries):
        for copy, sends, _ in entries:
            pl.when(sends)(copy.start)

    def wait(entries):
        for copy, sends, receives in entries:
            pl.when(sends)(copy.wait_send)
            pl.when(receives)(copy.wait_recv)

    def x_copy(buf, stage, layer, j):
        src = vol.at[x_of(j)] if stage == 0 else buf.at[layer, half + j]
        return pltpu.make_async_remote_copy(
            src_ref=src, dst_ref=buf.at[layer, half - 1 - j],
            send_sem=xsend.at[stage, j], recv_sem=xrecv.at[stage, j], device_id=x_peer, device_id_type=MESH)

    def start_x(buf, stage, layer, tau):
        for task in range(-(-half // PLANES)):
            @pl.when(tau == task)
            def _():
                for j in range(task * PLANES, min(half, (task + 1) * PLANES)):
                    x_copy(buf, stage, layer, j).start()

    def wait_x(buf, stage, layer, tau):
        @pl.when(tau == 0)
        def _():
            for j in range(half):
                x_copy(buf, stage, layer, j).wait()

    for j in range(half):
        x_copy(vols, 0, 0, j).start()

    def wait_in(j, carry):
        in_copy(j).wait()
        return carry

    lax.fori_loop(0, planes, wait_in, 0)

    def x_source(buf, layer, tau, group):
        at = pl.ds(group * edge_y, edge_y)
        return jnp.concatenate([buf[layer, tau * PLANES + p, at, :] for p in range(PLANES + 2 * half)], axis=0)

    def fx(layer, tau):
        wait_x(vols, layer, layer, tau)
        for group in range(pairs):
            total = dot(mfx[layer], x_source(vols, layer, tau, group)).astype(BF16)
            for p in range(PLANES):
                a1[tau * PLANES + p, group * edge_y:(group + 1) * edge_y] = total[p * edge_y:(p + 1) * edge_y]
            for side in range(2):
                first = PLANES * edge_y + side * edge
                zs[layer, tau, side, group] = total[first:first + edge]
        start(exchange(a1, layer, tau))

    def fz(layer, tau):
        wait(exchange(a1, layer, tau))
        bias = b[layer, :][None, :]
        channels = w.shape[1]
        z_halo = [dot(mfyh[layer], zh[layer, tau, side].reshape((pairs + 2) * edge, channels)).astype(BF16) for side in range(2)]
        for p in range(PLANES):
            j = tau * PLANES + p
            for part in range(2):
                if part == 0:
                    source = jnp.concatenate([yh[layer, j, 0], a1[j, :half_rows + edge_y]], axis=0)
                else:
                    source = jnp.concatenate([a1[j, half_rows - edge_y:], yh[layer, j, 1]], axis=0)
                second[p, part] = dot(mfy[layer], source).astype(BF16)
        for p in range(PLANES):
            for part in range(2):
                size = half * half_y
                first = (p * 2 + part) * size
                source = jnp.concatenate([second[p, part]] + [halo[first:first + size] for halo in z_halo], axis=0)
                a3[layer, tau * PLANES + p, part * half_rows:(part + 1) * half_rows] = dot(mfz[layer], source).astype(BF16)
        for p in range(PLANES):
            j = tau * PLANES + p
            for part in range(2):
                pre = dot(a3[layer, j, part * half_rows:(part + 1) * half_rows], w[layer])
                for first in range(0, half_rows, CHUNK):
                    at = slice(part * half_rows + first, part * half_rows + first + CHUNK)
                    z = pre[first:first + CHUNK] + bias
                    cdf = 0.5 * lax.erf(z * SQRT_HALF) + 0.5
                    gp[layer, j, at] = cdf + z * (jnp.exp2((z * z) * -HALF_LOG2_E) * INV_SQRT_2PI)
                    if layer + 1 < num_layers:
                        vols[layer + 1, j + half, at] = (vols[layer, j + half, at].astype(F32) + z * cdf).astype(BF16)
        if layer + 1 < num_layers:
            start_x(vols, layer + 1, layer + 1, tau)

    def bs(layer, tau):
        stage = num_layers + layer
        channels = w.shape[1]
        if layer == num_layers - 1:
            pl.when(tau == 0)(cot_copy.wait)
        total_b = gb_acc[layer]
        for group in range(pairs):
            chunks = []
            for p in range(PLANES):
                j = tau * PLANES + p
                at = slice(group * edge_y, (group + 1) * edge_y)
                scaled = gp[layer, j, at] * grad[x_of(j), at].astype(F32)
                total_b = total_b + jnp.sum(scaled.reshape(edge_y // 8, 8, channels), axis=0)
                chunks.append(scaled.astype(BF16))
                sb[p, at] = chunks[-1]
            mixed = dot(jnp.concatenate(chunks, axis=0), wt[layer]).astype(BF16)
            for p in range(PLANES):
                d3[tau * PLANES + p, group * edge_y:(group + 1) * edge_y] = mixed[p * edge_y:(p + 1) * edge_y]
        for group in range(pairs):
            mixed = jnp.concatenate([d3[tau * PLANES + p, group * edge_y:(group + 1) * edge_y] for p in range(PLANES)], axis=0)
            edges = dot(sel[...], mixed).astype(BF16)
            for side in range(2):
                zs[stage, tau, side, group] = edges[side * edge:(side + 1) * edge]
        gb_acc[layer] = total_b
        start(exchange(d3, stage, tau))
        product = lax.dot_general(
            a3[layer, pl.ds(tau * PLANES, PLANES)].reshape(PLANES * rows, channels), sb[...].reshape(PLANES * rows, channels),
            (((0,), (0,)), ((), ())), preferred_element_type=F32)
        for side in range(nx):
            gwx[layer, side, :part_x] += product[side * part_x:(side + 1) * part_x]

    def by(layer, tau):
        stage = num_layers + layer
        channels = w.shape[1]
        wait(exchange(d3, stage, tau))
        y_halo = []
        for side in range(2):
            corner = side * (pairs + 1)
            source = jnp.concatenate(
                [yh[stage, tau * PLANES + p, side] for p in range(PLANES)] + [zh[stage, tau, z_side, corner] for z_side in range(2)], axis=0)
            y_halo.append(dot(mbzh[layer], source).astype(BF16))
        for p in range(PLANES):
            j = tau * PLANES + p
            for part in range(2):
                halves = [zh[stage, tau, side, pl.ds(1 + part * (pairs // 2), pairs // 2)] for side in range(2)]
                source = jnp.concatenate(
                    [d3[j, part * half_rows:(part + 1) * half_rows]] + [halo.reshape(pairs // 2 * edge, channels) for halo in halves], axis=0)
                second[p, part] = dot(mbz[layer, p], source).astype(BF16)
        for p in range(PLANES):
            j = tau * PLANES + p
            at = slice(p * edge_y, (p + 1) * edge_y)
            for part in range(2):
                if part == 0:
                    source = jnp.concatenate([y_halo[0][at], second[p, 0], second[p, 1, :edge_y]], axis=0)
                else:
                    source = jnp.concatenate([second[p, 0, half_rows - edge_y:], second[p, 1], y_halo[1][at]], axis=0)
                d1[layer, j + half, part * half_rows:(part + 1) * half_rows] = dot(mby[layer], source).astype(BF16)
        start_x(d1, stage, layer, tau)

    def bx(layer, tau):
        wait_x(d1, num_layers + layer, layer, tau)

        for group in range(pairs):
            at = slice(group * edge_y, (group + 1) * edge_y)
            total = dot(mbx[layer], x_source(d1, layer, tau, group))
            for p in range(PLANES):
                x = x_of(tau * PLANES + p)
                grad[x, at] = (grad[x, at].astype(F32) + total[p * edge_y:(p + 1) * edge_y]).astype(BF16)
    def sum_copy(layer, phase, offset, src, dst, device):
        return pltpu.make_async_remote_copy(
            src_ref=src, dst_ref=dst, send_sem=sum_send.at[layer, phase, offset], recv_sem=sum_recv.at[layer, phase, offset],
            device_id=device, device_id_type=MESH)

    def bias_rows(layer):
        return 0 if layer else 8

    def core_copy(layer, phase):
        if phase == 0:
            at = pl.ds(0, part_x + bias_rows(layer))
            return sum_copy(layer, 0, 0, gwx.at[layer, 1 - my_x, at], rx.at[layer, at], x_peer)
        at = pl.ds(pl.multiple_of(my_x * part_x, part_x), part_x)
        return sum_copy(layer, 3, 0, gw_out.at[layer, at], gw_out.at[layer, at], x_peer)

    def own_rows():
        return pl.ds(pl.multiple_of(my_x * part_x + my_q * part_q, part_q), part_q)

    def chip_copy(layer, phase, offset):
        other = lax.rem(my_q + offset, group)
        if phase == 1:
            at = pl.ds(0, part_q + bias_rows(layer))
            return sum_copy(layer, 1, offset, rq.at[layer, 1, other, at], rq.at[layer, 0, my_q, at], chip(other))
        return sum_copy(layer, 2, offset, gw_out.at[layer, own_rows()], gw_out.at[layer, own_rows()], chip(other))

    def each_chip(layer, phase, act):
        def body(offset, carry):
            act(chip_copy(layer, phase, offset))
            return carry
        lax.fori_loop(1, group, body, 0)

    def r0(layer, tau):
        if bias_rows(layer):
            for side in range(nx):
                for row in range(num_layers):
                    gwx[layer, side, part_x + row, :] = jnp.sum(gb_acc[row], axis=0)
        core_copy(layer, 0).start()

    def r1(layer, tau):
        core_copy(layer, 0).wait()
        extra = bias_rows(layer)
        for q in range(group):
            at = slice(q * part_q, (q + 1) * part_q)
            rq[layer, 1, q, :part_q] = gwx[layer, my_x, at] + rx[layer, at]
            if extra:
                rq[layer, 1, q, part_q:] = gwx[layer, my_x, part_x:] + rx[layer, part_x:]
        rq[layer, 0, my_q, :part_q + extra] = rq[layer, 1, my_q, :part_q + extra]
        each_chip(layer, 1, lambda copy: copy.start())

    def r2(layer, tau):
        each_chip(layer, 1, lambda copy: copy.wait())
        count = part_q + bias_rows(layer)
        total = rq[layer, 0, 0, :count]
        for q in range(1, group):
            total = total + rq[layer, 0, q, :count]
        gw_out[layer, own_rows()] = total[:part_q]
        if bias_rows(layer):
            gb_out[...] = total[part_q:part_q + num_layers]
        each_chip(layer, 2, lambda copy: copy.start())

    def r3(layer, tau):
        each_chip(layer, 2, lambda copy: copy.wait())
        core_copy(layer, 3).start()

    def r4(layer, tau):
        core_copy(layer, 3).wait()

    tasks = {'r0': r0, 'r1': r1, 'r2': r2, 'r3': r3, 'r4': r4, 'm': build_backward, 'fx': fx, 'fz': fz, 'bs': bs, 'by': by, 'bx': bx}
    stages, last = stage_list(num_layers, nt)

    def step(s, carry):
        for kind, layer, first in stages:
            tau = s - first

            @pl.when((tau >= 0) & (tau < (1 if kind[0] in 'rm' else nt)))
            def _():
                tasks[kind](layer, tau)
        return carry

    lax.fori_loop(0, last, step, 0)


def solution(mesh):
    names = ('gx', 'gy', 'gz')
    nx, ny, nz = (mesh.shape[axis_name] for axis_name in names)
    assert nx == 2
    vol_spec = P('dp', 'gx', 'gy', 'gz')

    def local_step(volume, cot_out, filter_taps, w_mix, b_mix):
        channels, planes, by_len, bz_len = volume.shape
        num_layers, _, num_taps = filter_taps.shape
        half = (num_taps - 1) // 2
        rows = by_len * bz_len
        edge_y, pairs, edge = half * bz_len, by_len // half, PLANES * half * half
        half_rows = rows // 2
        nt = planes // PLANES
        stages = 2 * num_layers
        part_x = channels // nx
        part_q = part_x // (ny * nz)

        def to_rows(block):
            return jnp.transpose(block, (1, 2, 3, 0)).reshape(planes, rows, channels)

        any_spec = pl.BlockSpec(memory_space=pl.ANY)
        vmem_spec = pl.BlockSpec(memory_space=pltpu.VMEM)
        smem_spec = pl.BlockSpec(memory_space=pltpu.SMEM)
        block = (planes, rows, channels)
        dma = pltpu.SemaphoreType.DMA
        grad_rows, grad_w, grad_b = pl.pallas_call(
            functools.partial(kernel, (nx, ny, nz, num_layers, num_taps, by_len, bz_len)),
            out_shape=(
                pltpu.VMEM(block, BF16),
                pltpu.VMEM((num_layers, channels, channels), F32),
                pltpu.VMEM((num_layers, channels), F32),
            ),
            in_specs=[any_spec, any_spec, smem_spec, vmem_spec, vmem_spec],
            out_specs=(vmem_spec, vmem_spec, vmem_spec),
            scratch_shapes=[
                pltpu.VMEM((num_layers, planes + 2 * half, rows, channels), BF16),
                pltpu.VMEM(block, BF16),
                pltpu.VMEM((num_layers,) + block, BF16),
                pltpu.VMEM((num_layers,) + block, F32),
                pltpu.VMEM(block, BF16),
                pltpu.VMEM((num_layers, planes + 2 * half, rows, channels), BF16),
                pltpu.VMEM((PLANES, rows, channels), BF16),
                pltpu.VMEM((PLANES, 2, half_rows, channels), BF16),
                pltpu.VMEM((stages, planes, 2, edge_y, channels), BF16),
                pltpu.VMEM((stages, nt, 2, pairs + 2, edge, channels), BF16),
                pltpu.VMEM((stages, nt, 2, pairs, edge, channels), BF16),
                pltpu.VMEM((num_layers, channels, channels), BF16),
                pltpu.VMEM((num_layers, PLANES * edge_y + 2 * edge, (PLANES + 2 * half) * edge_y), BF16),
                pltpu.VMEM((num_layers, half_rows, half_rows + 2 * edge_y), BF16),
                pltpu.VMEM((num_layers, PLANES * half * by_len, (pairs + 2) * edge), BF16),
                pltpu.VMEM((num_layers, half_rows, half_rows + half * by_len), BF16),
                pltpu.VMEM((num_layers, PLANES * edge_y, (PLANES + 2 * half) * edge_y), BF16),
                pltpu.VMEM((num_layers, half_rows, half_rows + 2 * edge_y), BF16),
                pltpu.VMEM((num_layers, PLANES, half_rows, half_rows + pairs * edge), BF16),
                pltpu.VMEM((num_layers, PLANES * edge_y, PLANES * edge_y + 2 * edge), BF16),
                pltpu.VMEM((2 * edge, PLANES * edge_y), BF16),
                pltpu.VMEM((num_layers, nx, part_x + 8, channels), F32),
                pltpu.VMEM((num_layers, 8, channels), F32),
                pltpu.VMEM((num_layers, part_x + 8, channels), F32),
                pltpu.VMEM((num_layers, 2, ny * nz, part_q + 8, channels), F32),
                dma((num_layers, 4, ny * nz)), dma((num_layers, 4, ny * nz)),
                dma((planes,)), dma,
                dma((stages, nt, 8)), dma((stages, nt, 8)),
                dma((stages, half)), dma((stages, half)),
            ],
            compiler_params=pltpu.CompilerParams(
                collective_id=0, has_side_effects=True, vmem_limit_bytes=59000 * 1024),
            name='stack',
        )(to_rows(volume), to_rows(cot_out), filter_taps, w_mix, b_mix)
        grad_volume = jnp.transpose(grad_rows.reshape(planes, by_len, bz_len, channels), (3, 0, 1, 2))
        return grad_volume, grad_w, grad_b

    return jax.shard_map(local_step, mesh=mesh, in_specs=(vol_spec, vol_spec, P(), P(), P()), out_specs=(vol_spec, P('dp'), P('dp')), check_vma=False)
```

```python
import functools

import jax
import jax.numpy as jnp
from jax import lax
from jax.experimental import pallas as pl
from jax.experimental.pallas import tpu as pltpu
from jax.sharding import PartitionSpec as P

MESH = pl.DeviceIdType.MESH
PLANES = 4
LAST_LAG = 4
LAG = 3
SUM_STEPS = ((0, 0, 4, 7, 9), (0, 2, 6, 10, 11), (0, 2, 9, 13, 15))
XLAG = 1
F32 = jnp.float32
BF16 = jnp.bfloat16
SQRT_HALF = 0.7071067811865476
HALF_LOG2_E = 0.7213475204444817
CHUNK = 16
INV_SQRT_2PI = 0.3989422804014327


def dot(a, b):
    return jnp.dot(a, b, preferred_element_type=F32)


def stage_list(num_layers, nt):
    stages = []
    start = 0
    for layer in range(num_layers):
        stages.append(('fx', layer, start))
        stages.append(('fz', layer, start + LAG))
        start += LAG + (XLAG if layer + 1 < num_layers else 0)
    for layer in reversed(range(num_layers)):
        stages.append(('bs', layer, start))
        lag = LAG if layer else LAST_LAG
        stages.append(('by', layer, start + lag))
        stages.append(('bx', layer, start + lag + XLAG))
        start += lag + XLAG
    stages[1:1] = [('m', layer, layer) for layer in range(num_layers)]
    for kind, layer, first in list(stages):
        if kind == 'bs':
            stages += [('r%d' % phase, layer, first + nt - 1 + SUM_STEPS[min(layer, 2)][phase]) for phase in range(5)]
    return stages, max(first + (1 if kind[0] in 'rm' else nt) for kind, _, first in stages)


def kernel(sizes, vol, cot, taps, w, b, grad, gw_out, gb_out,
           vols, a1, a3, gp, d3, d1, sb, second, yh, zh, zs, wt,
           mfx, mfy, mfyh, mfz, mbx, mby, mbz, mbzh, sel,
           gwx, gb_acc, rx, rq, sum_send, sum_recv,
           in_sem, cot_sem, send_sem, recv_sem, xsend, xrecv):
    nx, ny, nz, num_layers, num_taps, by_len, bz_len = sizes
    half = (num_taps - 1) // 2
    planes = a1.shape[0]
    rows = by_len * bz_len
    edge_y = half * bz_len
    pairs = by_len // half
    edge = PLANES * half * half
    nt = planes // PLANES
    part_x = w.shape[1] // nx
    group = ny * nz
    part_q = part_x // group
    my_x, my_y, my_z = lax.axis_index('gx'), lax.axis_index('gy'), lax.axis_index('gz')
    y_lo, y_hi = my_y > 0, my_y < ny - 1
    z_lo, z_hi = my_z > 0, my_z < nz - 1
    x_peer = {'gx': 1 - my_x}

    def x_of(j):
        return my_x * j + (1 - my_x) * (planes - 1 - j)

    my_q = my_z * ny + my_y

    other_y = [lax.rem(my_y + offset, ny) for offset in range(ny)]
    other_z = [lax.rem(my_z + offset, nz) for offset in range(nz)]
    others = [(y, z) for z in range(nz) for y in range(ny)][1:]

    barrier = pltpu.get_barrier_semaphore()
    pl.semaphore_signal(barrier, inc=1, device_id=x_peer, device_id_type=MESH)
    for y, z in others:
        pl.semaphore_signal(barrier, inc=1, device_id={'gy': other_y[y], 'gz': other_z[z]}, device_id_type=MESH)

    def in_copy(j):
        return pltpu.make_async_copy(vol.at[x_of(j)], vols.at[0, j + half], in_sem.at[j])

    cot_copy = pltpu.make_async_copy(cot, grad, cot_sem)

    def start_in(j, carry):
        in_copy(j).start()
        return carry

    lax.fori_loop(0, planes, start_in, 0)
    cot_copy.start()

    half_y, half_rows = by_len // 2, rows // 2

    def iota(shape, axis):
        return lax.broadcasted_iota(jnp.int32, shape, axis)

    def banded(layer, axis, back, hop, inside):
        total = jnp.zeros(hop.shape, F32)
        for t in range(num_taps):
            tap = taps[layer, axis, num_taps - 1 - t if back else t]
            if axis == 0:
                tap = jnp.where(my_x == 1, tap, taps[layer, axis, t if back else num_taps - 1 - t])
            total = jnp.where(hop == t, tap, total)
        return jnp.where(inside, total, 0.0).astype(BF16)

    def edge_index(e):
        return e // edge, e % edge // (half * half), e % (half * half) // half, e % half

    def grid(row_count, column_count):
        return iota((row_count, column_count), 0), iota((row_count, column_count), 1)

    def build_forward(layer, carry):
        i, k = grid(PLANES * edge_y, (PLANES + 2 * half) * edge_y)
        mfx[layer, :PLANES * edge_y] = banded(layer, 0, False, k // edge_y - i // edge_y, k % edge_y == i % edge_y)
        i, k = grid(2 * edge, (PLANES + 2 * half) * edge_y)
        side, plane, depth, y = edge_index(i)
        z = depth + side * (bz_len - half)
        mfx[layer, PLANES * edge_y:] = banded(layer, 0, False, k // edge_y - plane, k % edge_y == y * bz_len + z)
        i, k = grid(half_rows, half_rows + 2 * edge_y)
        mfy[layer] = banded(layer, 1, False, k // bz_len - i // bz_len, k % bz_len == i % bz_len)
        i, k = grid(PLANES * half * by_len, (pairs + 2) * edge)
        side, plane, depth, y = edge_index(k % edge)
        y = (k // edge - 1) * half + y
        i_y = i // (half * half_y) % 2 * half_y + i % half_y
        inside = (plane == i // (half * by_len)) & (depth == i // half_y % half)
        mfyh[layer] = banded(layer, 1, False, y - i_y + half, inside)
        i, k = grid(half_rows, half_rows)
        mfz[layer, :, :half_rows] = banded(layer, 2, False, k % bz_len - i % bz_len + half, k // bz_len == i // bz_len)
        i, k = grid(half_rows, half * by_len)
        hop = k // half_y % half + k // (half * half_y) * (bz_len + half) - i % bz_len
        mfz[layer, :, half_rows:] = banded(layer, 2, False, hop, k % half_y == i // bz_len)
        return carry

    def build_backward(layer, tau):
        i, k = grid(PLANES * edge_y, (PLANES + 2 * half) * edge_y)
        mbx[layer] = banded(layer, 0, True, k // edge_y - i // edge_y, k % edge_y == i % edge_y)
        i, k = grid(half_rows, half_rows + 2 * edge_y)
        mby[layer] = banded(layer, 1, True, k // bz_len - i // bz_len, k % bz_len == i % bz_len)
        i, k = grid(half_rows, half_rows)
        own_back = banded(layer, 2, True, k % bz_len - i % bz_len + half, k // bz_len == i // bz_len)
        i, k = grid(half_rows, pairs * edge)
        side, (_, plane, depth, y) = k // (pairs * edge // 2), edge_index(k % edge)
        y = k // edge % (pairs // 2) * half + y
        hop = depth + side * (bz_len + half) - i % bz_len
        for p in range(PLANES):
            mbz[layer, p, :, :half_rows] = own_back
            mbz[layer, p, :, half_rows:] = banded(layer, 2, True, hop, (y == i // bz_len) & (plane == p))
        i, k = grid(PLANES * edge_y, PLANES * edge_y)
        mbzh[layer, :, :PLANES * edge_y] = banded(layer, 2, True, k % bz_len - i % bz_len + half, k // bz_len == i // bz_len)
        i, k = grid(PLANES * edge_y, 2 * edge)
        side, plane, depth, y = edge_index(k)
        hop = depth + side * (bz_len + half) - i % bz_len
        mbzh[layer, :, PLANES * edge_y:] = banded(layer, 2, True, hop, (plane == i // edge_y) & (y == i // bz_len % half))
        wt[layer] = jnp.transpose(w[layer].astype(F32)).astype(BF16)

    lax.fori_loop(0, num_layers, build_forward, 0)
    i, k = grid(2 * edge, PLANES * edge_y)
    side, plane, depth, y = edge_index(i)
    z = depth + side * (bz_len - half)
    sel[...] = jnp.where((k // edge_y == plane) & (k % edge_y == y * bz_len + z), 1.0, 0.0).astype(BF16)

    pl.semaphore_wait(barrier, group)

    def exchange(src, stage, tau):
        at = pl.ds(tau * PLANES, PLANES)
        y_near, z_near = {0: None, 1: y_hi, -1: y_lo}, {0: None, 1: z_hi, -1: z_lo}
        entries = []
        for dy, dz in ((1, 0), (-1, 0), (0, 1), (0, -1), (1, 1), (1, -1), (-1, 1), (-1, -1)):
            device = {}
            if dy:
                device['gy'] = jnp.clip(my_y + dy, 0, ny - 1)
            if dz:
                device['gz'] = jnp.clip(my_z + dz, 0, nz - 1)
            if dz == 0:
                source = src.at[at, pl.ds(rows - edge_y if dy > 0 else 0, edge_y)]
                target = yh.at[stage, at, 0 if dy > 0 else 1]
            else:
                from_side, to_side = (1, 0) if dz > 0 else (0, 1)
                if dy == 0:
                    source, target = zs.at[stage, tau, from_side], zh.at[stage, tau, to_side, pl.ds(1, pairs)]
                else:
                    source = zs.at[stage, tau, from_side, pairs - 1 if dy > 0 else 0]
                    target = zh.at[stage, tau, to_side, 0 if dy > 0 else pairs + 1]
            copy = pltpu.make_async_remote_copy(
                src_ref=source, dst_ref=target, send_sem=send_sem.at[stage, tau, len(entries)],
                recv_sem=recv_sem.at[stage, tau, len(entries)], device_id=device, device_id_type=MESH)
            sends = [near for near in (y_near[dy], z_near[dz]) if near is not None]
            receives = [near for near in (y_near[-dy], z_near[-dz]) if near is not None]
            entries.append((copy, functools.reduce(jnp.logical_and, sends), functools.reduce(jnp.logical_and, receives)))
        return entries

    def start(entries):
        for copy, sends, _ in entries:
            pl.when(sends)(copy.start)

    def wait(entries):
        for copy, sends, receives in entries:
            pl.when(sends)(copy.wait_send)
            pl.when(receives)(copy.wait_recv)

    def x_copy(buf, stage, layer, j):
        src = vol.at[x_of(j)] if stage == 0 else buf.at[layer, half + j]
        return pltpu.make_async_remote_copy(
            src_ref=src, dst_ref=buf.at[layer, half - 1 - j],
            send_sem=xsend.at[stage, j], recv_sem=xrecv.at[stage, j], device_id=x_peer, device_id_type=MESH)

    def start_x(buf, stage, layer, tau):
        for task in range(-(-half // PLANES)):
            @pl.when(tau == task)
            def _():
                for j in range(task * PLANES, min(half, (task + 1) * PLANES)):
                    x_copy(buf, stage, layer, j).start()

    def wait_x(buf, stage, layer, tau):
        @pl.when(tau == 0)
        def _():
            for j in range(half):
                x_copy(buf, stage, layer, j).wait()

    for j in range(half):
        x_copy(vols, 0, 0, j).start()

    for layer in range(num_layers):
        vols[layer, planes + half:] = jnp.zeros((half,) + vols.shape[2:], BF16)
        d1[layer, planes + half:] = jnp.zeros((half,) + d1.shape[2:], BF16)

    def zero_halo(where, clear):
        @pl.when(where)
        def _():
            def body(stage, carry):
                clear(stage)
                return carry
            lax.fori_loop(0, 2 * num_layers, body, 0)

    def clear_y(side):
        def clear(stage):
            yh[stage, :, side] = jnp.zeros(yh.shape[1:2] + yh.shape[3:], BF16)
            zh[stage, :, :, side * (pairs + 1)] = jnp.zeros(zh.shape[1:3] + zh.shape[4:], BF16)
        return clear

    def clear_z(side):
        def clear(stage):
            zh[stage, :, side] = jnp.zeros(zh.shape[1:2] + zh.shape[3:], BF16)
        return clear

    zero_halo(my_y == 0, clear_y(0))
    zero_halo(my_y == ny - 1, clear_y(1))
    zero_halo(my_z == 0, clear_z(0))
    zero_halo(my_z == nz - 1, clear_z(1))
    gwx[...] = jnp.zeros(gwx.shape, F32)
    gb_acc[...] = jnp.zeros(gb_acc.shape, F32)

    def wait_in(j, carry):
        in_copy(j).wait()
        return carry

    lax.fori_loop(0, planes, wait_in, 0)

    def x_source(buf, layer, tau, group):
        at = pl.ds(group * edge_y, edge_y)
        return jnp.concatenate([buf[layer, tau * PLANES + p, at, :] for p in range(PLANES + 2 * half)], axis=0)

    def fx(layer, tau):
        wait_x(vols, layer, layer, tau)
        for group in range(pairs):
            total = dot(mfx[layer], x_source(vols, layer, tau, group)).astype(BF16)
            for p in range(PLANES):
                a1[tau * PLANES + p, group * edge_y:(group + 1) * edge_y] = total[p * edge_y:(p + 1) * edge_y]
            for side in range(2):
                first = PLANES * edge_y + side * edge
                zs[layer, tau, side, group] = total[first:first + edge]
        start(exchange(a1, layer, tau))

    def fz(layer, tau):
        wait(exchange(a1, layer, tau))
        bias = b[layer, :][None, :]
        channels = w.shape[1]
        z_halo = [dot(mfyh[layer], zh[layer, tau, side].reshape((pairs + 2) * edge, channels)).astype(BF16) for side in range(2)]
        for p in range(PLANES):
            j = tau * PLANES + p
            for part in range(2):
                if part == 0:
                    source = jnp.concatenate([yh[layer, j, 0], a1[j, :half_rows + edge_y]], axis=0)
                else:
                    source = jnp.concatenate([a1[j, half_rows - edge_y:], yh[layer, j, 1]], axis=0)
                second[p, part] = dot(mfy[layer], source).astype(BF16)
        for p in range(PLANES):
            for part in range(2):
                size = half * half_y
                first = (p * 2 + part) * size
                source = jnp.concatenate([second[p, part]] + [halo[first:first + size] for halo in z_halo], axis=0)
                a3[layer, tau * PLANES + p, part * half_rows:(part + 1) * half_rows] = dot(mfz[layer], source).astype(BF16)
        for p in range(PLANES):
            j = tau * PLANES + p
            for part in range(2):
                pre = dot(a3[layer, j, part * half_rows:(part + 1) * half_rows], w[layer])
                for first in range(0, half_rows, CHUNK):
                    at = slice(part * half_rows + first, part * half_rows + first + CHUNK)
                    z = pre[first:first + CHUNK] + bias
                    cdf = 0.5 * lax.erf(z * SQRT_HALF) + 0.5
                    gp[layer, j, at] = cdf + z * (jnp.exp2((z * z) * -HALF_LOG2_E) * INV_SQRT_2PI)
                    if layer + 1 < num_layers:
                        vols[layer + 1, j + half, at] = (vols[layer, j + half, at].astype(F32) + z * cdf).astype(BF16)
        if layer + 1 < num_layers:
            start_x(vols, layer + 1, layer + 1, tau)

    def bs(layer, tau):
        stage = num_layers + layer
        channels = w.shape[1]
        if layer == num_layers - 1:
            pl.when(tau == 0)(cot_copy.wait)
        total_b = gb_acc[layer]
        for group in range(pairs):
            chunks = []
            for p in range(PLANES):
                j = tau * PLANES + p
                at = slice(group * edge_y, (group + 1) * edge_y)
                scaled = gp[layer, j, at] * grad[x_of(j), at].astype(F32)
                total_b = total_b + jnp.sum(scaled.reshape(edge_y // 8, 8, channels), axis=0)
                chunks.append(scaled.astype(BF16))
                sb[p, at] = chunks[-1]
            mixed = dot(jnp.concatenate(chunks, axis=0), wt[layer]).astype(BF16)
            for p in range(PLANES):
                d3[tau * PLANES + p, group * edge_y:(group + 1) * edge_y] = mixed[p * edge_y:(p + 1) * edge_y]
        for group in range(pairs):
            mixed = jnp.concatenate([d3[tau * PLANES + p, group * edge_y:(group + 1) * edge_y] for p in range(PLANES)], axis=0)
            edges = dot(sel[...], mixed).astype(BF16)
            for side in range(2):
                zs[stage, tau, side, group] = edges[side * edge:(side + 1) * edge]
        gb_acc[layer] = total_b
        start(exchange(d3, stage, tau))
        product = lax.dot_general(
            a3[layer, pl.ds(tau * PLANES, PLANES)].reshape(PLANES * rows, channels), sb[...].reshape(PLANES * rows, channels),
            (((0,), (0,)), ((), ())), preferred_element_type=F32)
        for side in range(nx):
            gwx[layer, side, :part_x] += product[side * part_x:(side + 1) * part_x]

    def by(layer, tau):
        stage = num_layers + layer
        channels = w.shape[1]
        wait(exchange(d3, stage, tau))
        y_halo = []
        for side in range(2):
            corner = side * (pairs + 1)
            source = jnp.concatenate(
                [yh[stage, tau * PLANES + p, side] for p in range(PLANES)] + [zh[stage, tau, z_side, corner] for z_side in range(2)], axis=0)
            y_halo.append(dot(mbzh[layer], source).astype(BF16))
        for p in range(PLANES):
            j = tau * PLANES + p
            for part in range(2):
                halves = [zh[stage, tau, side, pl.ds(1 + part * (pairs // 2), pairs // 2)] for side in range(2)]
                source = jnp.concatenate(
                    [d3[j, part * half_rows:(part + 1) * half_rows]] + [halo.reshape(pairs // 2 * edge, channels) for halo in halves], axis=0)
                second[p, part] = dot(mbz[layer, p], source).astype(BF16)
        for p in range(PLANES):
            j = tau * PLANES + p
            at = slice(p * edge_y, (p + 1) * edge_y)
            for part in range(2):
                if part == 0:
                    source = jnp.concatenate([y_halo[0][at], second[p, 0], second[p, 1, :edge_y]], axis=0)
                else:
                    source = jnp.concatenate([second[p, 0, half_rows - edge_y:], second[p, 1], y_halo[1][at]], axis=0)
                d1[layer, j + half, part * half_rows:(part + 1) * half_rows] = dot(mby[layer], source).astype(BF16)
        start_x(d1, stage, layer, tau)

    def bx(layer, tau):
        wait_x(d1, num_layers + layer, layer, tau)

        for group in range(pairs):
            at = slice(group * edge_y, (group + 1) * edge_y)
            total = dot(mbx[layer], x_source(d1, layer, tau, group))
            for p in range(PLANES):
                x = x_of(tau * PLANES + p)
                grad[x, at] = (grad[x, at].astype(F32) + total[p * edge_y:(p + 1) * edge_y]).astype(BF16)
    def sum_copy(layer, phase, offset, src, dst, device):
        return pltpu.make_async_remote_copy(
            src_ref=src, dst_ref=dst, send_sem=sum_send.at[layer, phase, offset], recv_sem=sum_recv.at[layer, phase, offset],
            device_id=device, device_id_type=MESH)

    def bias_rows(layer):
        return 0 if layer else 8

    def core_copy(layer, phase):
        if phase == 0:
            at = pl.ds(0, part_x + bias_rows(layer))
            return sum_copy(layer, 0, 0, gwx.at[layer, 1 - my_x, at], rx.at[layer, at], x_peer)
        at = pl.ds(pl.multiple_of(my_x * part_x, part_x), part_x)
        return sum_copy(layer, 3, 0, gw_out.at[layer, at], gw_out.at[layer, at], x_peer)

    def own_rows():
        return pl.ds(pl.multiple_of(my_x * part_x + my_q * part_q, part_q), part_q)

    def chip_copy(layer, phase, offset):
        y, z = others[offset]
        device = {'gy': other_y[y], 'gz': other_z[z]}
        if phase == 1:
            at = pl.ds(0, part_q + bias_rows(layer))
            source = rq.at[layer, 1, other_z[z] * ny + other_y[y], at]
            return sum_copy(layer, 1, offset, source, rq.at[layer, 0, my_q, at], device)
        return sum_copy(layer, 2, offset, gw_out.at[layer, own_rows()], gw_out.at[layer, own_rows()], device)

    def each_chip(layer, phase, act):
        for offset in range(group - 1):
            act(chip_copy(layer, phase, offset))

    def r0(layer, tau):
        if bias_rows(layer):
            for side in range(nx):
                for row in range(num_layers):
                    gwx[layer, side, part_x + row, :] = jnp.sum(gb_acc[row], axis=0)
        core_copy(layer, 0).start()

    def r1(layer, tau):
        core_copy(layer, 0).wait()
        extra = bias_rows(layer)
        for q in range(group):
            at = slice(q * part_q, (q + 1) * part_q)
            rq[layer, 1, q, :part_q] = gwx[layer, my_x, at] + rx[layer, at]
            if extra:
                rq[layer, 1, q, part_q:] = gwx[layer, my_x, part_x:] + rx[layer, part_x:]
        rq[layer, 0, my_q, :part_q + extra] = rq[layer, 1, my_q, :part_q + extra]
        each_chip(layer, 1, lambda copy: copy.start())

    def r2(layer, tau):
        each_chip(layer, 1, lambda copy: copy.wait())
        count = part_q + bias_rows(layer)
        total = rq[layer, 0, 0, :count]
        for q in range(1, group):
            total = total + rq[layer, 0, q, :count]
        gw_out[layer, own_rows()] = total[:part_q]
        if bias_rows(layer):
            gb_out[...] = total[part_q:part_q + num_layers]
        each_chip(layer, 2, lambda copy: copy.start())

    def r3(layer, tau):
        each_chip(layer, 2, lambda copy: copy.wait())
        core_copy(layer, 3).start()

    def r4(layer, tau):
        core_copy(layer, 3).wait()

    tasks = {'r0': r0, 'r1': r1, 'r2': r2, 'r3': r3, 'r4': r4, 'm': build_backward, 'fx': fx, 'fz': fz, 'bs': bs, 'by': by, 'bx': bx}
    stages, last = stage_list(num_layers, nt)

    def step(s, carry):
        for kind, layer, first in stages:
            tau = s - first

            @pl.when((tau >= 0) & (tau < (1 if kind[0] in 'rm' else nt)))
            def _():
                tasks[kind](layer, tau)
        return carry

    lax.fori_loop(0, last, step, 0)


def write_kernel(count, grad, gw, gb, grad_out, gw_out, gb_out, sems):
    part = grad.shape[0] // count
    copies = [pltpu.make_async_copy(grad.at[pl.ds(k * part, part)], grad_out.at[pl.ds(k * part, part)], sems.at[k]) for k in range(count)]
    copies += [pltpu.make_async_copy(gw.at[k], gw_out.at[k], sems.at[count + k]) for k in range(gw.shape[0])]
    copies.append(pltpu.make_async_copy(gb, gb_out, sems.at[count + gw.shape[0]]))
    for copy in copies:
        copy.start()
    for copy in copies:
        copy.wait()


def solution(mesh):
    names = ('gx', 'gy', 'gz')
    nx, ny, nz = (mesh.shape[axis_name] for axis_name in names)
    assert nx == 2
    vol_spec = P('dp', 'gx', 'gy', 'gz')

    def local_step(volume, cot_out, filter_taps, w_mix, b_mix):
        channels, planes, by_len, bz_len = volume.shape
        num_layers, _, num_taps = filter_taps.shape
        half = (num_taps - 1) // 2
        rows = by_len * bz_len
        edge_y, pairs, edge = half * bz_len, by_len // half, PLANES * half * half
        half_rows = rows // 2
        nt = planes // PLANES
        stages = 2 * num_layers
        part_x = channels // nx
        part_q = part_x // (ny * nz)

        def to_rows(block):
            return jnp.transpose(block, (1, 2, 3, 0)).reshape(planes, rows, channels)

        any_spec = pl.BlockSpec(memory_space=pl.ANY)
        vmem_spec = pl.BlockSpec(memory_space=pltpu.VMEM)
        smem_spec = pl.BlockSpec(memory_space=pltpu.SMEM)
        block = (planes, rows, channels)
        dma = pltpu.SemaphoreType.DMA
        grad_rows, grad_w, grad_b = pl.pallas_call(
            functools.partial(kernel, (nx, ny, nz, num_layers, num_taps, by_len, bz_len)),
            out_shape=(
                pltpu.VMEM(block, BF16),
                pltpu.VMEM((num_layers, channels, channels), F32),
                pltpu.VMEM((num_layers, channels), F32),
            ),
            in_specs=[any_spec, any_spec, smem_spec, vmem_spec, vmem_spec],
            out_specs=(vmem_spec, vmem_spec, vmem_spec),
            scratch_shapes=[
                pltpu.VMEM((num_layers, planes + 2 * half, rows, channels), BF16),
                pltpu.VMEM(block, BF16),
                pltpu.VMEM((num_layers,) + block, BF16),
                pltpu.VMEM((num_layers,) + block, F32),
                pltpu.VMEM(block, BF16),
                pltpu.VMEM((num_layers, planes + 2 * half, rows, channels), BF16),
                pltpu.VMEM((PLANES, rows, channels), BF16),
                pltpu.VMEM((PLANES, 2, half_rows, channels), BF16),
                pltpu.VMEM((stages, planes, 2, edge_y, channels), BF16),
                pltpu.VMEM((stages, nt, 2, pairs + 2, edge, channels), BF16),
                pltpu.VMEM((stages, nt, 2, pairs, edge, channels), BF16),
                pltpu.VMEM((num_layers, channels, channels), BF16),
                pltpu.VMEM((num_layers, PLANES * edge_y + 2 * edge, (PLANES + 2 * half) * edge_y), BF16),
                pltpu.VMEM((num_layers, half_rows, half_rows + 2 * edge_y), BF16),
                pltpu.VMEM((num_layers, PLANES * half * by_len, (pairs + 2) * edge), BF16),
                pltpu.VMEM((num_layers, half_rows, half_rows + half * by_len), BF16),
                pltpu.VMEM((num_layers, PLANES * edge_y, (PLANES + 2 * half) * edge_y), BF16),
                pltpu.VMEM((num_layers, half_rows, half_rows + 2 * edge_y), BF16),
                pltpu.VMEM((num_layers, PLANES, half_rows, half_rows + pairs * edge), BF16),
                pltpu.VMEM((num_layers, PLANES * edge_y, PLANES * edge_y + 2 * edge), BF16),
                pltpu.VMEM((2 * edge, PLANES * edge_y), BF16),
                pltpu.VMEM((num_layers, nx, part_x + 8, channels), F32),
                pltpu.VMEM((num_layers, 8, channels), F32),
                pltpu.VMEM((num_layers, part_x + 8, channels), F32),
                pltpu.VMEM((num_layers, 2, ny * nz, part_q + 8, channels), F32),
                dma((num_layers, 4, ny * nz)), dma((num_layers, 4, ny * nz)),
                dma((planes,)), dma,
                dma((stages, nt, 8)), dma((stages, nt, 8)),
                dma((stages, half)), dma((stages, half)),
            ],
            compiler_params=pltpu.CompilerParams(
                collective_id=0, has_side_effects=True, vmem_limit_bytes=59000 * 1024),
            name='stack',
        )(to_rows(volume), to_rows(cot_out), filter_taps, w_mix, b_mix)
        count = 4
        grad_rows, grad_w, grad_b = pl.pallas_call(
            functools.partial(write_kernel, count),
            out_shape=(
                jax.ShapeDtypeStruct(block, BF16),
                jax.ShapeDtypeStruct((num_layers, channels, channels), F32),
                jax.ShapeDtypeStruct((num_layers, channels), F32),
            ),
            in_specs=[vmem_spec] * 3,
            out_specs=(any_spec,) * 3,
            scratch_shapes=[dma((count + num_layers + 1,))],
            compiler_params=pltpu.CompilerParams(vmem_limit_bytes=1024 * 1024),
            name='write',
        )(*(pltpu.with_memory_space_constraint(value, pltpu.VMEM) for value in (grad_rows, grad_w, grad_b)))
        grad_volume = jnp.transpose(grad_rows.reshape(planes, by_len, bz_len, channels), (3, 0, 1, 2))
        return grad_volume, grad_w, grad_b

    return jax.shard_map(local_step, mesh=mesh, in_specs=(vol_spec, vol_spec, P(), P(), P()), out_specs=(vol_spec, P('dp'), P('dp')), check_vma=False)
```

```python
import functools

import jax
import jax.numpy as jnp
from jax import lax
from jax.experimental import pallas as pl
from jax.experimental.pallas import tpu as pltpu
from jax.sharding import PartitionSpec as P

MESH = pl.DeviceIdType.MESH
PLANES = 4
LAST_LAG = 4
LAG = 3
SUM_STEPS = ((0, 0, 4, 7, 9), (0, 2, 6, 10, 11), (0, 2, 9, 13, 15))
XLAG = 1
F32 = jnp.float32
BF16 = jnp.bfloat16
SQRT_HALF = 0.7071067811865476
HALF_LOG2_E = 0.7213475204444817
CHUNK = 16
INV_SQRT_2PI = 0.3989422804014327


def dot(a, b):
    return jnp.dot(a, b, preferred_element_type=F32)


def stage_list(num_layers, nt):
    stages = []
    start = 0
    for layer in range(num_layers):
        stages.append(('fx', layer, start))
        stages.append(('fz', layer, start + LAG))
        start += LAG + (XLAG if layer + 1 < num_layers else 0)
    for layer in reversed(range(num_layers)):
        stages.append(('bs', layer, start))
        lag = LAG if layer else LAST_LAG
        stages.append(('by', layer, start + lag))
        stages.append(('bx', layer, start + lag + XLAG))
        start += lag + XLAG
    stages[1:1] = [('m', layer, layer) for layer in range(num_layers)]
    for kind, layer, first in list(stages):
        if kind == 'bs':
            stages += [('r%d' % phase, layer, first + nt - 1 + SUM_STEPS[min(layer, 2)][phase]) for phase in range(5)]
    return stages, max(first + (1 if kind[0] in 'rm' else nt) for kind, _, first in stages)


def kernel(sizes, vol, cot, taps, w, b, grad, gw_out, gb_out,
           vols, a1, a3, gp, d3, d1, sb, second, yh, zh, zs, wt,
           mfx, mfy, mfyh, mfz, mbx, mby, mbz, mbzh, sel,
           gwx, gb_acc, rx, rq, sum_send, sum_recv,
           in_sem, cot_sem, send_sem, recv_sem, xsend, xrecv):
    nx, ny, nz, num_layers, num_taps, by_len, bz_len = sizes
    half = (num_taps - 1) // 2
    planes = a1.shape[0]
    rows = by_len * bz_len
    edge_y = half * bz_len
    half_y, half_rows = by_len // 2, rows // 2
    pairs = by_len // half
    edge = PLANES * half * half
    nt = planes // PLANES
    part_x = w.shape[1] // nx
    group = ny * nz
    part_q = part_x // group
    my_x, my_y, my_z = lax.axis_index('gx'), lax.axis_index('gy'), lax.axis_index('gz')
    y_lo, y_hi = my_y > 0, my_y < ny - 1
    z_lo, z_hi = my_z > 0, my_z < nz - 1
    x_peer = {'gx': 1 - my_x}

    def x_of(j):
        return my_x * j + (1 - my_x) * (planes - 1 - j)

    my_q = my_z * ny + my_y

    other_y = [lax.rem(my_y + offset, ny) for offset in range(ny)]
    other_z = [lax.rem(my_z + offset, nz) for offset in range(nz)]
    others = [(y, z) for z in range(nz) for y in range(ny)][1:]

    barrier = pltpu.get_barrier_semaphore()
    pl.semaphore_signal(barrier, inc=1, device_id=x_peer, device_id_type=MESH)
    for y, z in others:
        pl.semaphore_signal(barrier, inc=1, device_id={'gy': other_y[y], 'gz': other_z[z]}, device_id_type=MESH)

    def in_copy(j):
        return pltpu.make_async_copy(vol.at[x_of(j)], vols.at[0, j + half], in_sem.at[j])

    cot_copy = pltpu.make_async_copy(cot, grad, cot_sem)

    def start_in(j, carry):
        in_copy(j).start()
        return carry

    lax.fori_loop(0, planes, start_in, 0)
    cot_copy.start()

    pl.semaphore_wait(barrier, group)

    def exchange(src, stage, tau):
        at = pl.ds(tau * PLANES, PLANES)
        y_near, z_near = {0: None, 1: y_hi, -1: y_lo}, {0: None, 1: z_hi, -1: z_lo}
        entries = []
        for dy, dz in ((1, 1), (1, -1), (-1, 1), (-1, -1), (1, 0), (-1, 0), (0, 1), (0, -1)):
            device = {}
            if dy:
                device['gy'] = jnp.clip(my_y + dy, 0, ny - 1)
            if dz:
                device['gz'] = jnp.clip(my_z + dz, 0, nz - 1)
            if dz == 0:
                source = src.at[at, pl.ds(rows - edge_y if dy > 0 else 0, edge_y)]
                target = yh.at[stage, at, 0 if dy > 0 else 1]
            else:
                from_side, to_side = (1, 0) if dz > 0 else (0, 1)
                if dy == 0:
                    source, target = zs.at[stage, tau, from_side], zh.at[stage, tau, to_side, pl.ds(1, pairs)]
                else:
                    source = zs.at[stage, tau, from_side, pairs - 1 if dy > 0 else 0]
                    target = zh.at[stage, tau, to_side, 0 if dy > 0 else pairs + 1]
            copy = pltpu.make_async_remote_copy(
                src_ref=source, dst_ref=target, send_sem=send_sem.at[stage, tau, len(entries)],
                recv_sem=recv_sem.at[stage, tau, len(entries)], device_id=device, device_id_type=MESH)
            sends = [near for near in (y_near[dy], z_near[dz]) if near is not None]
            receives = [near for near in (y_near[-dy], z_near[-dz]) if near is not None]
            entries.append((copy, functools.reduce(jnp.logical_and, sends), functools.reduce(jnp.logical_and, receives)))
        return entries

    def start(entries):
        for copy, sends, _ in entries:
            pl.when(sends)(copy.start)

    def wait(entries):
        for copy, sends, receives in entries:
            pl.when(sends)(copy.wait_send)
            pl.when(receives)(copy.wait_recv)

    def x_copy(buf, stage, layer, j):
        src = vol.at[x_of(j)] if stage == 0 else buf.at[layer, half + j]
        return pltpu.make_async_remote_copy(
            src_ref=src, dst_ref=buf.at[layer, half - 1 - j],
            send_sem=xsend.at[stage, j], recv_sem=xrecv.at[stage, j], device_id=x_peer, device_id_type=MESH)

    def start_x(buf, stage, layer, tau):
        for task in range(-(-half // PLANES)):
            @pl.when(tau == task)
            def _():
                for j in range(task * PLANES, min(half, (task + 1) * PLANES)):
                    x_copy(buf, stage, layer, j).start()

    def wait_x(buf, stage, layer, tau):
        @pl.when(tau == 0)
        def _():
            for j in range(half):
                x_copy(buf, stage, layer, j).wait()

    for j in range(half):
        x_copy(vols, 0, 0, j).start()

    def iota(shape, axis):
        return lax.broadcasted_iota(jnp.int32, shape, axis)

    def banded(layer, axis, back, hop, inside):
        total = jnp.zeros(hop.shape, F32)
        for t in range(num_taps):
            tap = taps[layer, axis, num_taps - 1 - t if back else t]
            if axis == 0:
                tap = jnp.where(my_x == 1, tap, taps[layer, axis, t if back else num_taps - 1 - t])
            total = jnp.where(hop == t, tap, total)
        return jnp.where(inside, total, 0.0).astype(BF16)

    def edge_index(e):
        return e // edge, e % edge // (half * half), e % (half * half) // half, e % half

    def grid(row_count, column_count):
        return iota((row_count, column_count), 0), iota((row_count, column_count), 1)

    def build_forward(layer, carry):
        i, k = grid(PLANES * edge_y, (PLANES + 2 * half) * edge_y)
        mfx[layer, :PLANES * edge_y] = banded(layer, 0, False, k // edge_y - i // edge_y, k % edge_y == i % edge_y)
        i, k = grid(2 * edge, (PLANES + 2 * half) * edge_y)
        side, plane, depth, y = edge_index(i)
        z = depth + side * (bz_len - half)
        mfx[layer, PLANES * edge_y:] = banded(layer, 0, False, k // edge_y - plane, k % edge_y == y * bz_len + z)
        i, k = grid(half_rows, half_rows + 2 * edge_y)
        mfy[layer] = banded(layer, 1, False, k // bz_len - i // bz_len, k % bz_len == i % bz_len)
        i, k = grid(PLANES * half * by_len, (pairs + 2) * edge)
        side, plane, depth, y = edge_index(k % edge)
        y = (k // edge - 1) * half + y
        i_y = i // (half * half_y) % 2 * half_y + i % half_y
        inside = (plane == i // (half * by_len)) & (depth == i // half_y % half)
        mfyh[layer] = banded(layer, 1, False, y - i_y + half, inside)
        i, k = grid(half_rows, half_rows)
        mfz[layer, :, :half_rows] = banded(layer, 2, False, k % bz_len - i % bz_len + half, k // bz_len == i // bz_len)
        i, k = grid(half_rows, half * by_len)
        hop = k // half_y % half + k // (half * half_y) * (bz_len + half) - i % bz_len
        mfz[layer, :, half_rows:] = banded(layer, 2, False, hop, k % half_y == i // bz_len)
        return carry

    def build_backward(layer, tau):
        i, k = grid(PLANES * edge_y, (PLANES + 2 * half) * edge_y)
        mbx[layer] = banded(layer, 0, True, k // edge_y - i // edge_y, k % edge_y == i % edge_y)
        i, k = grid(half_rows, half_rows + 2 * edge_y)
        mby[layer] = banded(layer, 1, True, k // bz_len - i // bz_len, k % bz_len == i % bz_len)
        i, k = grid(half_rows, half_rows)
        own_back = banded(layer, 2, True, k % bz_len - i % bz_len + half, k // bz_len == i // bz_len)
        i, k = grid(half_rows, pairs * edge)
        side, (_, plane, depth, y) = k // (pairs * edge // 2), edge_index(k % edge)
        y = k // edge % (pairs // 2) * half + y
        hop = depth + side * (bz_len + half) - i % bz_len
        for p in range(PLANES):
            mbz[layer, p, :, :half_rows] = own_back
            mbz[layer, p, :, half_rows:] = banded(layer, 2, True, hop, (y == i // bz_len) & (plane == p))
        i, k = grid(PLANES * edge_y, PLANES * edge_y)
        mbzh[layer, :, :PLANES * edge_y] = banded(layer, 2, True, k % bz_len - i % bz_len + half, k // bz_len == i // bz_len)
        i, k = grid(PLANES * edge_y, 2 * edge)
        side, plane, depth, y = edge_index(k)
        hop = depth + side * (bz_len + half) - i % bz_len
        mbzh[layer, :, PLANES * edge_y:] = banded(layer, 2, True, hop, (plane == i // edge_y) & (y == i // bz_len % half))
        wt[layer] = jnp.transpose(w[layer].astype(F32)).astype(BF16)

    lax.fori_loop(0, num_layers, build_forward, 0)
    i, k = grid(2 * edge, PLANES * edge_y)
    side, plane, depth, y = edge_index(i)
    z = depth + side * (bz_len - half)
    sel[...] = jnp.where((k // edge_y == plane) & (k % edge_y == y * bz_len + z), 1.0, 0.0).astype(BF16)

    for layer in range(num_layers):
        vols[layer, planes + half:] = jnp.zeros((half,) + vols.shape[2:], BF16)
        d1[layer, planes + half:] = jnp.zeros((half,) + d1.shape[2:], BF16)

    def zero_halo(where, clear):
        @pl.when(where)
        def _():
            def body(stage, carry):
                clear(stage)
                return carry
            lax.fori_loop(0, 2 * num_layers, body, 0)

    def clear_y(side):
        def clear(stage):
            yh[stage, :, side] = jnp.zeros(yh.shape[1:2] + yh.shape[3:], BF16)
            zh[stage, :, :, side * (pairs + 1)] = jnp.zeros(zh.shape[1:3] + zh.shape[4:], BF16)
        return clear

    def clear_z(side):
        def clear(stage):
            zh[stage, :, side] = jnp.zeros(zh.shape[1:2] + zh.shape[3:], BF16)
        return clear

    zero_halo(my_y == 0, clear_y(0))
    zero_halo(my_y == ny - 1, clear_y(1))
    zero_halo(my_z == 0, clear_z(0))
    zero_halo(my_z == nz - 1, clear_z(1))
    gwx[...] = jnp.zeros(gwx.shape, F32)
    gb_acc[...] = jnp.zeros(gb_acc.shape, F32)

    def wait_in(j, carry):
        in_copy(j).wait()
        return carry

    lax.fori_loop(0, planes, wait_in, 0)

    def x_source(buf, layer, tau, group):
        at = pl.ds(group * edge_y, edge_y)
        return jnp.concatenate([buf[layer, tau * PLANES + p, at, :] for p in range(PLANES + 2 * half)], axis=0)

    def fx(layer, tau):
        wait_x(vols, layer, layer, tau)
        for group in range(pairs):
            total = dot(mfx[layer], x_source(vols, layer, tau, group)).astype(BF16)
            for p in range(PLANES):
                a1[tau * PLANES + p, group * edge_y:(group + 1) * edge_y] = total[p * edge_y:(p + 1) * edge_y]
            for side in range(2):
                first = PLANES * edge_y + side * edge
                zs[layer, tau, side, group] = total[first:first + edge]
        start(exchange(a1, layer, tau))

    def fz(layer, tau):
        wait(exchange(a1, layer, tau))
        bias = b[layer, :][None, :]
        channels = w.shape[1]
        z_halo = [dot(mfyh[layer], zh[layer, tau, side].reshape((pairs + 2) * edge, channels)).astype(BF16) for side in range(2)]
        for p in range(PLANES):
            j = tau * PLANES + p
            for part in range(2):
                if part == 0:
                    source = jnp.concatenate([yh[layer, j, 0], a1[j, :half_rows + edge_y]], axis=0)
                else:
                    source = jnp.concatenate([a1[j, half_rows - edge_y:], yh[layer, j, 1]], axis=0)
                second[p, part] = dot(mfy[layer], source).astype(BF16)
        for p in range(PLANES):
            for part in range(2):
                size = half * half_y
                first = (p * 2 + part) * size
                source = jnp.concatenate([second[p, part]] + [halo[first:first + size] for halo in z_halo], axis=0)
                a3[layer, tau * PLANES + p, part * half_rows:(part + 1) * half_rows] = dot(mfz[layer], source).astype(BF16)
        for p in range(PLANES):
            j = tau * PLANES + p
            for part in range(2):
                pre = dot(a3[layer, j, part * half_rows:(part + 1) * half_rows], w[layer])
                for first in range(0, half_rows, CHUNK):
                    at = slice(part * half_rows + first, part * half_rows + first + CHUNK)
                    z = pre[first:first + CHUNK] + bias
                    cdf = 0.5 * lax.erf(z * SQRT_HALF) + 0.5
                    gp[layer, j, at] = cdf + z * (jnp.exp2((z * z) * -HALF_LOG2_E) * INV_SQRT_2PI)
                    if layer + 1 < num_layers:
                        vols[layer + 1, j + half, at] = (vols[layer, j + half, at].astype(F32) + z * cdf).astype(BF16)
        if layer + 1 < num_layers:
            start_x(vols, layer + 1, layer + 1, tau)

    def bs(layer, tau):
        stage = num_layers + layer
        channels = w.shape[1]
        if layer == num_layers - 1:
            pl.when(tau == 0)(cot_copy.wait)
        total_b = gb_acc[layer]
        for group in range(pairs):
            chunks = []
            for p in range(PLANES):
                j = tau * PLANES + p
                at = slice(group * edge_y, (group + 1) * edge_y)
                scaled = gp[layer, j, at] * grad[x_of(j), at].astype(F32)
                total_b = total_b + jnp.sum(scaled.reshape(edge_y // 8, 8, channels), axis=0)
                chunks.append(scaled.astype(BF16))
                sb[p, at] = chunks[-1]
            mixed = dot(jnp.concatenate(chunks, axis=0), wt[layer]).astype(BF16)
            for p in range(PLANES):
                d3[tau * PLANES + p, group * edge_y:(group + 1) * edge_y] = mixed[p * edge_y:(p + 1) * edge_y]
        for group in range(pairs):
            mixed = jnp.concatenate([d3[tau * PLANES + p, group * edge_y:(group + 1) * edge_y] for p in range(PLANES)], axis=0)
            edges = dot(sel[...], mixed).astype(BF16)
            for side in range(2):
                zs[stage, tau, side, group] = edges[side * edge:(side + 1) * edge]
        gb_acc[layer] = total_b
        start(exchange(d3, stage, tau))
        product = lax.dot_general(
            a3[layer, pl.ds(tau * PLANES, PLANES)].reshape(PLANES * rows, channels), sb[...].reshape(PLANES * rows, channels),
            (((0,), (0,)), ((), ())), preferred_element_type=F32)
        for side in range(nx):
            gwx[layer, side, :part_x] += product[side * part_x:(side + 1) * part_x]

    def by(layer, tau):
        stage = num_layers + layer
        channels = w.shape[1]
        wait(exchange(d3, stage, tau))
        y_halo = []
        for side in range(2):
            corner = side * (pairs + 1)
            source = jnp.concatenate(
                [yh[stage, tau * PLANES + p, side] for p in range(PLANES)] + [zh[stage, tau, z_side, corner] for z_side in range(2)], axis=0)
            y_halo.append(dot(mbzh[layer], source).astype(BF16))
        for p in range(PLANES):
            j = tau * PLANES + p
            for part in range(2):
                halves = [zh[stage, tau, side, pl.ds(1 + part * (pairs // 2), pairs // 2)] for side in range(2)]
                source = jnp.concatenate(
                    [d3[j, part * half_rows:(part + 1) * half_rows]] + [halo.reshape(pairs // 2 * edge, channels) for halo in halves], axis=0)
                second[p, part] = dot(mbz[layer, p], source).astype(BF16)
        for p in range(PLANES):
            j = tau * PLANES + p
            at = slice(p * edge_y, (p + 1) * edge_y)
            for part in range(2):
                if part == 0:
                    source = jnp.concatenate([y_halo[0][at], second[p, 0], second[p, 1, :edge_y]], axis=0)
                else:
                    source = jnp.concatenate([second[p, 0, half_rows - edge_y:], second[p, 1], y_halo[1][at]], axis=0)
                d1[layer, j + half, part * half_rows:(part + 1) * half_rows] = dot(mby[layer], source).astype(BF16)
        start_x(d1, stage, layer, tau)

    def bx(layer, tau):
        wait_x(d1, num_layers + layer, layer, tau)

        for group in range(pairs):
            at = slice(group * edge_y, (group + 1) * edge_y)
            total = dot(mbx[layer], x_source(d1, layer, tau, group))
            for p in range(PLANES):
                x = x_of(tau * PLANES + p)
                grad[x, at] = (grad[x, at].astype(F32) + total[p * edge_y:(p + 1) * edge_y]).astype(BF16)
    def sum_copy(layer, phase, offset, src, dst, device):
        return pltpu.make_async_remote_copy(
            src_ref=src, dst_ref=dst, send_sem=sum_send.at[layer, phase, offset], recv_sem=sum_recv.at[layer, phase, offset],
            device_id=device, device_id_type=MESH)

    def bias_rows(layer):
        return 0 if layer else 8

    def core_copy(layer, phase):
        if phase == 0:
            at = pl.ds(0, part_x + bias_rows(layer))
            return sum_copy(layer, 0, 0, gwx.at[layer, 1 - my_x, at], rx.at[layer, at], x_peer)
        at = pl.ds(pl.multiple_of(my_x * part_x, part_x), part_x)
        return sum_copy(layer, 3, 0, gw_out.at[layer, at], gw_out.at[layer, at], x_peer)

    def own_rows():
        return pl.ds(pl.multiple_of(my_x * part_x + my_q * part_q, part_q), part_q)

    def chip_copy(layer, phase, offset):
        y, z = others[offset]
        device = {'gy': other_y[y], 'gz': other_z[z]}
        if phase == 1:
            at = pl.ds(0, part_q + bias_rows(layer))
            source = rq.at[layer, 1, other_z[z] * ny + other_y[y], at]
            return sum_copy(layer, 1, offset, source, rq.at[layer, 0, my_q, at], device)
        return sum_copy(layer, 2, offset, gw_out.at[layer, own_rows()], gw_out.at[layer, own_rows()], device)

    def each_chip(layer, phase, act):
        for offset in range(group - 1):
            act(chip_copy(layer, phase, offset))

    def r0(layer, tau):
        if bias_rows(layer):
            for side in range(nx):
                for row in range(num_layers):
                    gwx[layer, side, part_x + row, :] = jnp.sum(gb_acc[row], axis=0)
        core_copy(layer, 0).start()

    def r1(layer, tau):
        core_copy(layer, 0).wait()
        extra = bias_rows(layer)
        for q in range(group):
            at = slice(q * part_q, (q + 1) * part_q)
            rq[layer, 1, q, :part_q] = gwx[layer, my_x, at] + rx[layer, at]
            if extra:
                rq[layer, 1, q, part_q:] = gwx[layer, my_x, part_x:] + rx[layer, part_x:]
        rq[layer, 0, my_q, :part_q + extra] = rq[layer, 1, my_q, :part_q + extra]
        each_chip(layer, 1, lambda copy: copy.start())

    def r2(layer, tau):
        each_chip(layer, 1, lambda copy: copy.wait())
        count = part_q + bias_rows(layer)
        total = rq[layer, 0, 0, :count]
        for q in range(1, group):
            total = total + rq[layer, 0, q, :count]
        gw_out[layer, own_rows()] = total[:part_q]
        if bias_rows(layer):
            gb_out[...] = total[part_q:part_q + num_layers]
        each_chip(layer, 2, lambda copy: copy.start())

    def r3(layer, tau):
        each_chip(layer, 2, lambda copy: copy.wait())
        core_copy(layer, 3).start()

    def r4(layer, tau):
        core_copy(layer, 3).wait()

    tasks = {'r0': r0, 'r1': r1, 'r2': r2, 'r3': r3, 'r4': r4, 'm': build_backward, 'fx': fx, 'fz': fz, 'bs': bs, 'by': by, 'bx': bx}
    stages, last = stage_list(num_layers, nt)

    def step(s, carry):
        for kind, layer, first in stages:
            tau = s - first

            @pl.when((tau >= 0) & (tau < (1 if kind[0] in 'rm' else nt)))
            def _():
                tasks[kind](layer, tau)
        return carry

    lax.fori_loop(0, last, step, 0)


def write_kernel(count, grad, gw, gb, grad_out, gw_out, gb_out, sems):
    part = grad.shape[0] // count
    copies = [pltpu.make_async_copy(grad.at[pl.ds(k * part, part)], grad_out.at[pl.ds(k * part, part)], sems.at[k]) for k in range(count)]
    copies += [pltpu.make_async_copy(gw.at[k], gw_out.at[k], sems.at[count + k]) for k in range(gw.shape[0])]
    copies.append(pltpu.make_async_copy(gb, gb_out, sems.at[count + gw.shape[0]]))
    for copy in copies:
        copy.start()
    for copy in copies:
        copy.wait()


def solution(mesh):
    names = ('gx', 'gy', 'gz')
    nx, ny, nz = (mesh.shape[axis_name] for axis_name in names)
    assert nx == 2
    vol_spec = P('dp', 'gx', 'gy', 'gz')

    def local_step(volume, cot_out, filter_taps, w_mix, b_mix):
        channels, planes, by_len, bz_len = volume.shape
        num_layers, _, num_taps = filter_taps.shape
        half = (num_taps - 1) // 2
        rows = by_len * bz_len
        edge_y, pairs, edge = half * bz_len, by_len // half, PLANES * half * half
        half_rows = rows // 2
        nt = planes // PLANES
        stages = 2 * num_layers
        part_x = channels // nx
        part_q = part_x // (ny * nz)

        def to_rows(block):
            return jnp.transpose(block, (1, 2, 3, 0)).reshape(planes, rows, channels)

        any_spec = pl.BlockSpec(memory_space=pl.ANY)
        vmem_spec = pl.BlockSpec(memory_space=pltpu.VMEM)
        smem_spec = pl.BlockSpec(memory_space=pltpu.SMEM)
        block = (planes, rows, channels)
        dma = pltpu.SemaphoreType.DMA
        grad_rows, grad_w, grad_b = pl.pallas_call(
            functools.partial(kernel, (nx, ny, nz, num_layers, num_taps, by_len, bz_len)),
            out_shape=(
                pltpu.VMEM(block, BF16),
                pltpu.VMEM((num_layers, channels, channels), F32),
                pltpu.VMEM((num_layers, channels), F32),
            ),
            in_specs=[any_spec, any_spec, smem_spec, vmem_spec, vmem_spec],
            out_specs=(vmem_spec, vmem_spec, vmem_spec),
            scratch_shapes=[
                pltpu.VMEM((num_layers, planes + 2 * half, rows, channels), BF16),
                pltpu.VMEM(block, BF16),
                pltpu.VMEM((num_layers,) + block, BF16),
                pltpu.VMEM((num_layers,) + block, F32),
                pltpu.VMEM(block, BF16),
                pltpu.VMEM((num_layers, planes + 2 * half, rows, channels), BF16),
                pltpu.VMEM((PLANES, rows, channels), BF16),
                pltpu.VMEM((PLANES, 2, half_rows, channels), BF16),
                pltpu.VMEM((stages, planes, 2, edge_y, channels), BF16),
                pltpu.VMEM((stages, nt, 2, pairs + 2, edge, channels), BF16),
                pltpu.VMEM((stages, nt, 2, pairs, edge, channels), BF16),
                pltpu.VMEM((num_layers, channels, channels), BF16),
                pltpu.VMEM((num_layers, PLANES * edge_y + 2 * edge, (PLANES + 2 * half) * edge_y), BF16),
                pltpu.VMEM((num_layers, half_rows, half_rows + 2 * edge_y), BF16),
                pltpu.VMEM((num_layers, PLANES * half * by_len, (pairs + 2) * edge), BF16),
                pltpu.VMEM((num_layers, half_rows, half_rows + half * by_len), BF16),
                pltpu.VMEM((num_layers, PLANES * edge_y, (PLANES + 2 * half) * edge_y), BF16),
                pltpu.VMEM((num_layers, half_rows, half_rows + 2 * edge_y), BF16),
                pltpu.VMEM((num_layers, PLANES, half_rows, half_rows + pairs * edge), BF16),
                pltpu.VMEM((num_layers, PLANES * edge_y, PLANES * edge_y + 2 * edge), BF16),
                pltpu.VMEM((2 * edge, PLANES * edge_y), BF16),
                pltpu.VMEM((num_layers, nx, part_x + 8, channels), F32),
                pltpu.VMEM((num_layers, 8, channels), F32),
                pltpu.VMEM((num_layers, part_x + 8, channels), F32),
                pltpu.VMEM((num_layers, 2, ny * nz, part_q + 8, channels), F32),
                dma((num_layers, 4, ny * nz)), dma((num_layers, 4, ny * nz)),
                dma((planes,)), dma,
                dma((stages, nt, 8)), dma((stages, nt, 8)),
                dma((stages, half)), dma((stages, half)),
            ],
            compiler_params=pltpu.CompilerParams(
                collective_id=0, has_side_effects=True, vmem_limit_bytes=59000 * 1024),
            name='stack',
        )(to_rows(volume), to_rows(cot_out), filter_taps, w_mix, b_mix)
        count = 4
        grad_rows, grad_w, grad_b = pl.pallas_call(
            functools.partial(write_kernel, count),
            out_shape=(
                jax.ShapeDtypeStruct(block, BF16),
                jax.ShapeDtypeStruct((num_layers, channels, channels), F32),
                jax.ShapeDtypeStruct((num_layers, channels), F32),
            ),
            in_specs=[vmem_spec] * 3,
            out_specs=(any_spec,) * 3,
            scratch_shapes=[dma((count + num_layers + 1,))],
            compiler_params=pltpu.CompilerParams(vmem_limit_bytes=1024 * 1024),
            name='write',
        )(*(pltpu.with_memory_space_constraint(value, pltpu.VMEM) for value in (grad_rows, grad_w, grad_b)))
        grad_volume = jnp.transpose(grad_rows.reshape(planes, by_len, bz_len, channels), (3, 0, 1, 2))
        return grad_volume, grad_w, grad_b

    return jax.shard_map(local_step, mesh=mesh, in_specs=(vol_spec, vol_spec, P(), P(), P()), out_specs=(vol_spec, P('dp'), P('dp')), check_vma=False)
```

```python
import functools

import jax
import jax.numpy as jnp
from jax import lax
from jax.experimental import pallas as pl
from jax.experimental.pallas import tpu as pltpu
from jax.sharding import PartitionSpec as P

MESH = pl.DeviceIdType.MESH
PLANES = 4
LAST_LAG = 4
LAG = 3
SUM_STEPS = ((0, 0, 4, 7, 9), (0, 2, 6, 10, 11), (0, 2, 9, 13, 15))
XLAG = 1
F32 = jnp.float32
BF16 = jnp.bfloat16
SQRT_HALF = 0.7071067811865476
HALF_LOG2_E = 0.7213475204444817
CHUNK = 16
INV_SQRT_2PI = 0.3989422804014327


def dot(a, b):
    return jnp.dot(a, b, preferred_element_type=F32)


def stage_list(num_layers, nt):
    stages = []
    start = 0
    for layer in range(num_layers):
        stages.append(('fx', layer, start))
        stages.append(('fz', layer, start + LAG))
        start += LAG + (XLAG if layer + 1 < num_layers else 0)
    for layer in reversed(range(num_layers)):
        stages.append(('bs', layer, start))
        lag = LAG if layer else LAST_LAG
        stages.append(('by', layer, start + lag))
        stages.append(('bx', layer, start + lag + XLAG))
        start += lag + XLAG
    stages[1:1] = [('m', layer, layer) for layer in range(num_layers)]
    for kind, layer, first in list(stages):
        if kind == 'bs':
            stages += [('r%d' % phase, layer, first + nt - 1 + SUM_STEPS[min(layer, 2)][phase]) for phase in range(5)]
    return stages, max(first + (1 if kind[0] in 'rm' else nt) for kind, _, first in stages)


def kernel(sizes, vol, cot, taps, w, b, grad, gw_out, gb_out,
           vols, a1, a3, gp, d3, d1, sb, second, yh, zh, zs, wt,
           mfx, mfy, mfyh, mfz, mbx, mby, mbz, mbzh, sel,
           gwx, gb_acc, rx, rq, sum_send, sum_recv,
           in_sem, cot_sem, send_sem, recv_sem, xsend, xrecv):
    nx, ny, nz, num_layers, num_taps, by_len, bz_len = sizes
    half = (num_taps - 1) // 2
    planes = a1.shape[0]
    rows = by_len * bz_len
    edge_y = half * bz_len
    half_y, half_rows = by_len // 2, rows // 2
    pairs = by_len // half
    edge = PLANES * half * half
    nt = planes // PLANES
    part_x = w.shape[1] // nx
    group = ny * nz
    part_q = part_x // group
    my_x, my_y, my_z = lax.axis_index('gx'), lax.axis_index('gy'), lax.axis_index('gz')
    y_lo, y_hi = my_y > 0, my_y < ny - 1
    z_lo, z_hi = my_z > 0, my_z < nz - 1
    x_peer = {'gx': 1 - my_x}

    def x_of(j):
        return my_x * j + (1 - my_x) * (planes - 1 - j)

    my_q = my_z * ny + my_y

    other_y = [lax.rem(my_y + offset, ny) for offset in range(ny)]
    other_z = [lax.rem(my_z + offset, nz) for offset in range(nz)]
    others = [(y, z) for z in range(nz) for y in range(ny)][1:]

    barrier = pltpu.get_barrier_semaphore()
    pl.semaphore_signal(barrier, inc=1, device_id=x_peer, device_id_type=MESH)
    for y, z in others:
        pl.semaphore_signal(barrier, inc=1, device_id={'gy': other_y[y], 'gz': other_z[z]}, device_id_type=MESH)

    def in_copy(j):
        return pltpu.make_async_copy(vol.at[x_of(j)], vols.at[0, j + half], in_sem.at[j])

    cot_copy = pltpu.make_async_copy(cot, grad, cot_sem)

    def start_in(j, carry):
        in_copy(j).start()
        return carry

    lax.fori_loop(0, planes, start_in, 0)
    cot_copy.start()

    pl.semaphore_wait(barrier, group)

    def exchange(src, stage, tau):
        at = pl.ds(tau * PLANES, PLANES)
        y_near, z_near = {0: None, 1: y_hi, -1: y_lo}, {0: None, 1: z_hi, -1: z_lo}
        entries = []
        for dy, dz in ((1, 1), (1, -1), (-1, 1), (-1, -1), (1, 0), (-1, 0), (0, 1), (0, -1)):
            device = {}
            if dy:
                device['gy'] = jnp.clip(my_y + dy, 0, ny - 1)
            if dz:
                device['gz'] = jnp.clip(my_z + dz, 0, nz - 1)
            if dz == 0:
                source = src.at[at, pl.ds(rows - edge_y if dy > 0 else 0, edge_y)]
                target = yh.at[stage, at, 0 if dy > 0 else 1]
            else:
                from_side, to_side = (1, 0) if dz > 0 else (0, 1)
                if dy == 0:
                    source, target = zs.at[stage, tau, from_side], zh.at[stage, tau, to_side, pl.ds(1, pairs)]
                else:
                    source = zs.at[stage, tau, from_side, pairs - 1 if dy > 0 else 0]
                    target = zh.at[stage, tau, to_side, 0 if dy > 0 else pairs + 1]
            copy = pltpu.make_async_remote_copy(
                src_ref=source, dst_ref=target, send_sem=send_sem.at[stage, tau, len(entries)],
                recv_sem=recv_sem.at[stage, tau, len(entries)], device_id=device, device_id_type=MESH)
            sends = [near for near in (y_near[dy], z_near[dz]) if near is not None]
            receives = [near for near in (y_near[-dy], z_near[-dz]) if near is not None]
            entries.append((copy, functools.reduce(jnp.logical_and, sends), functools.reduce(jnp.logical_and, receives)))
        return entries

    def start(entries):
        for copy, sends, _ in entries:
            pl.when(sends)(copy.start)

    def wait(entries):
        for copy, sends, receives in entries:
            pl.when(sends)(copy.wait_send)
            pl.when(receives)(copy.wait_recv)

    def x_copy(buf, stage, layer, j):
        src = vol.at[x_of(j)] if stage == 0 else buf.at[layer, half + j]
        return pltpu.make_async_remote_copy(
            src_ref=src, dst_ref=buf.at[layer, half - 1 - j],
            send_sem=xsend.at[stage, j], recv_sem=xrecv.at[stage, j], device_id=x_peer, device_id_type=MESH)

    def start_x(buf, stage, layer, tau):
        for task in range(-(-half // PLANES)):
            @pl.when(tau == task)
            def _():
                for j in range(task * PLANES, min(half, (task + 1) * PLANES)):
                    x_copy(buf, stage, layer, j).start()

    def wait_x(buf, stage, layer, tau):
        @pl.when(tau == 0)
        def _():
            for j in range(half):
                x_copy(buf, stage, layer, j).wait()

    for j in range(half):
        x_copy(vols, 0, 0, j).start()

    def iota(shape, axis):
        return lax.broadcasted_iota(jnp.int32, shape, axis)

    def banded(layer, axis, back, hop, inside):
        total = jnp.zeros(hop.shape, F32)
        for t in range(num_taps):
            tap = taps[layer, axis, num_taps - 1 - t if back else t]
            if axis == 0:
                tap = jnp.where(my_x == 1, tap, taps[layer, axis, t if back else num_taps - 1 - t])
            total = jnp.where(hop == t, tap, total)
        return jnp.where(inside, total, 0.0).astype(BF16)

    def edge_index(e):
        return e // edge, e % edge // (half * half), e % (half * half) // half, e % half

    def grid(row_count, column_count):
        return iota((row_count, column_count), 0), iota((row_count, column_count), 1)

    def build_forward(layer, carry):
        i, k = grid(PLANES * edge_y, (PLANES + 2 * half) * edge_y)
        mfx[layer, :PLANES * edge_y] = banded(layer, 0, False, k // edge_y - i // edge_y, k % edge_y == i % edge_y)
        i, k = grid(2 * edge, (PLANES + 2 * half) * edge_y)
        side, plane, depth, y = edge_index(i)
        z = depth + side * (bz_len - half)
        mfx[layer, PLANES * edge_y:] = banded(layer, 0, False, k // edge_y - plane, k % edge_y == y * bz_len + z)
        i, k = grid(half_rows, half_rows + 2 * edge_y)
        mfy[layer] = banded(layer, 1, False, k // bz_len - i // bz_len, k % bz_len == i % bz_len)
        i, k = grid(PLANES * half * by_len, (pairs + 2) * edge)
        side, plane, depth, y = edge_index(k % edge)
        y = (k // edge - 1) * half + y
        i_y = i // (half * half_y) % 2 * half_y + i % half_y
        inside = (plane == i // (half * by_len)) & (depth == i // half_y % half)
        mfyh[layer] = banded(layer, 1, False, y - i_y + half, inside)
        i, k = grid(half_rows, half_rows)
        mfz[layer, :, :half_rows] = banded(layer, 2, False, k % bz_len - i % bz_len + half, k // bz_len == i // bz_len)
        i, k = grid(half_rows, half * by_len)
        hop = k // half_y % half + k // (half * half_y) * (bz_len + half) - i % bz_len
        mfz[layer, :, half_rows:] = banded(layer, 2, False, hop, k % half_y == i // bz_len)
        return carry

    def build_backward(layer, tau):
        i, k = grid(PLANES * edge_y, (PLANES + 2 * half) * edge_y)
        mbx[layer] = banded(layer, 0, True, k // edge_y - i // edge_y, k % edge_y == i % edge_y)
        i, k = grid(half_rows, half_rows + 2 * edge_y)
        mby[layer] = banded(layer, 1, True, k // bz_len - i // bz_len, k % bz_len == i % bz_len)
        i, k = grid(half_rows, half_rows)
        own_back = banded(layer, 2, True, k % bz_len - i % bz_len + half, k // bz_len == i // bz_len)
        i, k = grid(half_rows, pairs * edge)
        side, (_, plane, depth, y) = k // (pairs * edge // 2), edge_index(k % edge)
        y = k // edge % (pairs // 2) * half + y
        hop = depth + side * (bz_len + half) - i % bz_len
        for p in range(PLANES):
            mbz[layer, p, :, :half_rows] = own_back
            mbz[layer, p, :, half_rows:] = banded(layer, 2, True, hop, (y == i // bz_len) & (plane == p))
        i, k = grid(PLANES * edge_y, PLANES * edge_y)
        mbzh[layer, :, :PLANES * edge_y] = banded(layer, 2, True, k % bz_len - i % bz_len + half, k // bz_len == i // bz_len)
        i, k = grid(PLANES * edge_y, 2 * edge)
        side, plane, depth, y = edge_index(k)
        hop = depth + side * (bz_len + half) - i % bz_len
        mbzh[layer, :, PLANES * edge_y:] = banded(layer, 2, True, hop, (plane == i // edge_y) & (y == i // bz_len % half))
        wt[layer] = jnp.transpose(w[layer].astype(F32)).astype(BF16)

    lax.fori_loop(0, num_layers, build_forward, 0)
    i, k = grid(2 * edge, PLANES * edge_y)
    side, plane, depth, y = edge_index(i)
    z = depth + side * (bz_len - half)
    sel[...] = jnp.where((k // edge_y == plane) & (k % edge_y == y * bz_len + z), 1.0, 0.0).astype(BF16)

    for layer in range(num_layers):
        vols[layer, planes + half:] = jnp.zeros((half,) + vols.shape[2:], BF16)
        d1[layer, planes + half:] = jnp.zeros((half,) + d1.shape[2:], BF16)

    def zero_halo(where, clear):
        @pl.when(where)
        def _():
            def body(stage, carry):
                clear(stage)
                return carry
            lax.fori_loop(0, 2 * num_layers, body, 0)

    def clear_y(side):
        def clear(stage):
            yh[stage, :, side] = jnp.zeros(yh.shape[1:2] + yh.shape[3:], BF16)
            zh[stage, :, :, side * (pairs + 1)] = jnp.zeros(zh.shape[1:3] + zh.shape[4:], BF16)
        return clear

    def clear_z(side):
        def clear(stage):
            zh[stage, :, side] = jnp.zeros(zh.shape[1:2] + zh.shape[3:], BF16)
        return clear

    zero_halo(my_y == 0, clear_y(0))
    zero_halo(my_y == ny - 1, clear_y(1))
    zero_halo(my_z == 0, clear_z(0))
    zero_halo(my_z == nz - 1, clear_z(1))
    gwx[...] = jnp.zeros(gwx.shape, F32)
    gb_acc[...] = jnp.zeros(gb_acc.shape, F32)

    def wait_in(j, carry):
        in_copy(j).wait()
        return carry

    lax.fori_loop(0, planes, wait_in, 0)

    def x_source(buf, layer, tau, group):
        at = pl.ds(group * edge_y, edge_y)
        return jnp.concatenate([buf[layer, tau * PLANES + p, at, :] for p in range(PLANES + 2 * half)], axis=0)

    def fx(layer, tau):
        if layer == 0 and nt % 2 == 0:
            tau = tau + 1 - 2 * lax.rem(tau, 2)
        wait_x(vols, layer, layer, tau)
        for group in range(pairs):
            total = dot(mfx[layer], x_source(vols, layer, tau, group)).astype(BF16)
            for p in range(PLANES):
                a1[tau * PLANES + p, group * edge_y:(group + 1) * edge_y] = total[p * edge_y:(p + 1) * edge_y]
            for side in range(2):
                first = PLANES * edge_y + side * edge
                zs[layer, tau, side, group] = total[first:first + edge]
        start(exchange(a1, layer, tau))

    def fz(layer, tau):
        wait(exchange(a1, layer, tau))
        bias = b[layer, :][None, :]
        channels = w.shape[1]
        z_halo = [dot(mfyh[layer], zh[layer, tau, side].reshape((pairs + 2) * edge, channels)).astype(BF16) for side in range(2)]
        for p in range(PLANES):
            j = tau * PLANES + p
            for part in range(2):
                if part == 0:
                    source = jnp.concatenate([yh[layer, j, 0], a1[j, :half_rows + edge_y]], axis=0)
                else:
                    source = jnp.concatenate([a1[j, half_rows - edge_y:], yh[layer, j, 1]], axis=0)
                second[p, part] = dot(mfy[layer], source).astype(BF16)
        for p in range(PLANES):
            for part in range(2):
                size = half * half_y
                first = (p * 2 + part) * size
                source = jnp.concatenate([second[p, part]] + [halo[first:first + size] for halo in z_halo], axis=0)
                a3[layer, tau * PLANES + p, part * half_rows:(part + 1) * half_rows] = dot(mfz[layer], source).astype(BF16)
        for p in range(PLANES):
            j = tau * PLANES + p
            for part in range(2):
                pre = dot(a3[layer, j, part * half_rows:(part + 1) * half_rows], w[layer])
                for first in range(0, half_rows, CHUNK):
                    at = slice(part * half_rows + first, part * half_rows + first + CHUNK)
                    z = pre[first:first + CHUNK] + bias
                    cdf = 0.5 * lax.erf(z * SQRT_HALF) + 0.5
                    gp[layer, j, at] = cdf + z * (jnp.exp2((z * z) * -HALF_LOG2_E) * INV_SQRT_2PI)
                    if layer + 1 < num_layers:
                        vols[layer + 1, j + half, at] = (vols[layer, j + half, at].astype(F32) + z * cdf).astype(BF16)
        if layer + 1 < num_layers:
            start_x(vols, layer + 1, layer + 1, tau)

    def bs(layer, tau):
        stage = num_layers + layer
        channels = w.shape[1]
        if layer == num_layers - 1:
            pl.when(tau == 0)(cot_copy.wait)
        total_b = gb_acc[layer]
        for group in range(pairs):
            chunks = []
            for p in range(PLANES):
                j = tau * PLANES + p
                at = slice(group * edge_y, (group + 1) * edge_y)
                scaled = gp[layer, j, at] * grad[x_of(j), at].astype(F32)
                total_b = total_b + jnp.sum(scaled.reshape(edge_y // 8, 8, channels), axis=0)
                chunks.append(scaled.astype(BF16))
                sb[p, at] = chunks[-1]
            mixed = dot(jnp.concatenate(chunks, axis=0), wt[layer]).astype(BF16)
            for p in range(PLANES):
                d3[tau * PLANES + p, group * edge_y:(group + 1) * edge_y] = mixed[p * edge_y:(p + 1) * edge_y]
        for group in range(pairs):
            mixed = jnp.concatenate([d3[tau * PLANES + p, group * edge_y:(group + 1) * edge_y] for p in range(PLANES)], axis=0)
            edges = dot(sel[...], mixed).astype(BF16)
            for side in range(2):
                zs[stage, tau, side, group] = edges[side * edge:(side + 1) * edge]
        gb_acc[layer] = total_b
        start(exchange(d3, stage, tau))
        product = lax.dot_general(
            a3[layer, pl.ds(tau * PLANES, PLANES)].reshape(PLANES * rows, channels), sb[...].reshape(PLANES * rows, channels),
            (((0,), (0,)), ((), ())), preferred_element_type=F32)
        for side in range(nx):
            gwx[layer, side, :part_x] += product[side * part_x:(side + 1) * part_x]

    def by(layer, tau):
        stage = num_layers + layer
        channels = w.shape[1]
        wait(exchange(d3, stage, tau))
        y_halo = []
        for side in range(2):
            corner = side * (pairs + 1)
            source = jnp.concatenate(
                [yh[stage, tau * PLANES + p, side] for p in range(PLANES)] + [zh[stage, tau, z_side, corner] for z_side in range(2)], axis=0)
            y_halo.append(dot(mbzh[layer], source).astype(BF16))
        for p in range(PLANES):
            j = tau * PLANES + p
            for part in range(2):
                halves = [zh[stage, tau, side, pl.ds(1 + part * (pairs // 2), pairs // 2)] for side in range(2)]
                source = jnp.concatenate(
                    [d3[j, part * half_rows:(part + 1) * half_rows]] + [halo.reshape(pairs // 2 * edge, channels) for halo in halves], axis=0)
                second[p, part] = dot(mbz[layer, p], source).astype(BF16)
        for p in range(PLANES):
            j = tau * PLANES + p
            at = slice(p * edge_y, (p + 1) * edge_y)
            for part in range(2):
                if part == 0:
                    source = jnp.concatenate([y_halo[0][at], second[p, 0], second[p, 1, :edge_y]], axis=0)
                else:
                    source = jnp.concatenate([second[p, 0, half_rows - edge_y:], second[p, 1], y_halo[1][at]], axis=0)
                d1[layer, j + half, part * half_rows:(part + 1) * half_rows] = dot(mby[layer], source).astype(BF16)
        start_x(d1, stage, layer, tau)

    def bx(layer, tau):
        wait_x(d1, num_layers + layer, layer, tau)

        for group in range(pairs):
            at = slice(group * edge_y, (group + 1) * edge_y)
            total = dot(mbx[layer], x_source(d1, layer, tau, group))
            for p in range(PLANES):
                x = x_of(tau * PLANES + p)
                grad[x, at] = (grad[x, at].astype(F32) + total[p * edge_y:(p + 1) * edge_y]).astype(BF16)
    def sum_copy(layer, phase, offset, src, dst, device):
        return pltpu.make_async_remote_copy(
            src_ref=src, dst_ref=dst, send_sem=sum_send.at[layer, phase, offset], recv_sem=sum_recv.at[layer, phase, offset],
            device_id=device, device_id_type=MESH)

    def bias_rows(layer):
        return 0 if layer else 8

    def core_copy(layer, phase):
        if phase == 0:
            at = pl.ds(0, part_x + bias_rows(layer))
            return sum_copy(layer, 0, 0, gwx.at[layer, 1 - my_x, at], rx.at[layer, at], x_peer)
        at = pl.ds(pl.multiple_of(my_x * part_x, part_x), part_x)
        return sum_copy(layer, 3, 0, gw_out.at[layer, at], gw_out.at[layer, at], x_peer)

    def own_rows():
        return pl.ds(pl.multiple_of(my_x * part_x + my_q * part_q, part_q), part_q)

    def chip_copy(layer, phase, offset):
        y, z = others[offset]
        device = {'gy': other_y[y], 'gz': other_z[z]}
        if phase == 1:
            at = pl.ds(0, part_q + bias_rows(layer))
            source = rq.at[layer, 1, other_z[z] * ny + other_y[y], at]
            return sum_copy(layer, 1, offset, source, rq.at[layer, 0, my_q, at], device)
        return sum_copy(layer, 2, offset, gw_out.at[layer, own_rows()], gw_out.at[layer, own_rows()], device)

    def each_chip(layer, phase, act):
        for offset in range(group - 1):
            act(chip_copy(layer, phase, offset))

    def r0(layer, tau):
        if bias_rows(layer):
            for side in range(nx):
                for row in range(num_layers):
                    gwx[layer, side, part_x + row, :] = jnp.sum(gb_acc[row], axis=0)
        core_copy(layer, 0).start()

    def r1(layer, tau):
        core_copy(layer, 0).wait()
        extra = bias_rows(layer)
        for q in range(group):
            at = slice(q * part_q, (q + 1) * part_q)
            rq[layer, 1, q, :part_q] = gwx[layer, my_x, at] + rx[layer, at]
            if extra:
                rq[layer, 1, q, part_q:] = gwx[layer, my_x, part_x:] + rx[layer, part_x:]
        rq[layer, 0, my_q, :part_q + extra] = rq[layer, 1, my_q, :part_q + extra]
        each_chip(layer, 1, lambda copy: copy.start())

    def r2(layer, tau):
        each_chip(layer, 1, lambda copy: copy.wait())
        count = part_q + bias_rows(layer)
        total = rq[layer, 0, 0, :count]
        for q in range(1, group):
            total = total + rq[layer, 0, q, :count]
        gw_out[layer, own_rows()] = total[:part_q]
        if bias_rows(layer):
            gb_out[...] = total[part_q:part_q + num_layers]
        each_chip(layer, 2, lambda copy: copy.start())

    def r3(layer, tau):
        each_chip(layer, 2, lambda copy: copy.wait())
        core_copy(layer, 3).start()

    def r4(layer, tau):
        core_copy(layer, 3).wait()

    tasks = {'r0': r0, 'r1': r1, 'r2': r2, 'r3': r3, 'r4': r4, 'm': build_backward, 'fx': fx, 'fz': fz, 'bs': bs, 'by': by, 'bx': bx}
    stages, last = stage_list(num_layers, nt)

    def step(s, carry):
        for kind, layer, first in stages:
            tau = s - first

            @pl.when((tau >= 0) & (tau < (1 if kind[0] in 'rm' else nt)))
            def _():
                tasks[kind](layer, tau)
        return carry

    lax.fori_loop(0, last, step, 0)


def write_kernel(count, grad, gw, gb, grad_out, gw_out, gb_out, sems):
    part = grad.shape[0] // count
    copies = [pltpu.make_async_copy(grad.at[pl.ds(k * part, part)], grad_out.at[pl.ds(k * part, part)], sems.at[k]) for k in range(count)]
    copies += [pltpu.make_async_copy(gw.at[k], gw_out.at[k], sems.at[count + k]) for k in range(gw.shape[0])]
    copies.append(pltpu.make_async_copy(gb, gb_out, sems.at[count + gw.shape[0]]))
    for copy in copies:
        copy.start()
    for copy in copies:
        copy.wait()


def solution(mesh):
    names = ('gx', 'gy', 'gz')
    nx, ny, nz = (mesh.shape[axis_name] for axis_name in names)
    assert nx == 2
    vol_spec = P('dp', 'gx', 'gy', 'gz')

    def local_step(volume, cot_out, filter_taps, w_mix, b_mix):
        channels, planes, by_len, bz_len = volume.shape
        num_layers, _, num_taps = filter_taps.shape
        half = (num_taps - 1) // 2
        rows = by_len * bz_len
        edge_y, pairs, edge = half * bz_len, by_len // half, PLANES * half * half
        half_rows = rows // 2
        nt = planes // PLANES
        stages = 2 * num_layers
        part_x = channels // nx
        part_q = part_x // (ny * nz)

        def to_rows(block):
            return jnp.transpose(block, (1, 2, 3, 0)).reshape(planes, rows, channels)

        any_spec = pl.BlockSpec(memory_space=pl.ANY)
        vmem_spec = pl.BlockSpec(memory_space=pltpu.VMEM)
        smem_spec = pl.BlockSpec(memory_space=pltpu.SMEM)
        block = (planes, rows, channels)
        dma = pltpu.SemaphoreType.DMA
        grad_rows, grad_w, grad_b = pl.pallas_call(
            functools.partial(kernel, (nx, ny, nz, num_layers, num_taps, by_len, bz_len)),
            out_shape=(
                pltpu.VMEM(block, BF16),
                pltpu.VMEM((num_layers, channels, channels), F32),
                pltpu.VMEM((num_layers, channels), F32),
            ),
            in_specs=[any_spec, any_spec, smem_spec, vmem_spec, vmem_spec],
            out_specs=(vmem_spec, vmem_spec, vmem_spec),
            scratch_shapes=[
                pltpu.VMEM((num_layers, planes + 2 * half, rows, channels), BF16),
                pltpu.VMEM(block, BF16),
                pltpu.VMEM((num_layers,) + block, BF16),
                pltpu.VMEM((num_layers,) + block, F32),
                pltpu.VMEM(block, BF16),
                pltpu.VMEM((num_layers, planes + 2 * half, rows, channels), BF16),
                pltpu.VMEM((PLANES, rows, channels), BF16),
                pltpu.VMEM((PLANES, 2, half_rows, channels), BF16),
                pltpu.VMEM((stages, planes, 2, edge_y, channels), BF16),
                pltpu.VMEM((stages, nt, 2, pairs + 2, edge, channels), BF16),
                pltpu.VMEM((stages, nt, 2, pairs, edge, channels), BF16),
                pltpu.VMEM((num_layers, channels, channels), BF16),
                pltpu.VMEM((num_layers, PLANES * edge_y + 2 * edge, (PLANES + 2 * half) * edge_y), BF16),
                pltpu.VMEM((num_layers, half_rows, half_rows + 2 * edge_y), BF16),
                pltpu.VMEM((num_layers, PLANES * half * by_len, (pairs + 2) * edge), BF16),
                pltpu.VMEM((num_layers, half_rows, half_rows + half * by_len), BF16),
                pltpu.VMEM((num_layers, PLANES * edge_y, (PLANES + 2 * half) * edge_y), BF16),
                pltpu.VMEM((num_layers, half_rows, half_rows + 2 * edge_y), BF16),
                pltpu.VMEM((num_layers, PLANES, half_rows, half_rows + pairs * edge), BF16),
                pltpu.VMEM((num_layers, PLANES * edge_y, PLANES * edge_y + 2 * edge), BF16),
                pltpu.VMEM((2 * edge, PLANES * edge_y), BF16),
                pltpu.VMEM((num_layers, nx, part_x + 8, channels), F32),
                pltpu.VMEM((num_layers, 8, channels), F32),
                pltpu.VMEM((num_layers, part_x + 8, channels), F32),
                pltpu.VMEM((num_layers, 2, ny * nz, part_q + 8, channels), F32),
                dma((num_layers, 4, ny * nz)), dma((num_layers, 4, ny * nz)),
                dma((planes,)), dma,
                dma((stages, nt, 8)), dma((stages, nt, 8)),
                dma((stages, half)), dma((stages, half)),
            ],
            compiler_params=pltpu.CompilerParams(
                collective_id=0, has_side_effects=True, vmem_limit_bytes=59000 * 1024),
            name='stack',
        )(to_rows(volume), to_rows(cot_out), filter_taps, w_mix, b_mix)
        count = 4
        grad_rows, grad_w, grad_b = pl.pallas_call(
            functools.partial(write_kernel, count),
            out_shape=(
                jax.ShapeDtypeStruct(block, BF16),
                jax.ShapeDtypeStruct((num_layers, channels, channels), F32),
                jax.ShapeDtypeStruct((num_layers, channels), F32),
            ),
            in_specs=[vmem_spec] * 3,
            out_specs=(any_spec,) * 3,
            scratch_shapes=[dma((count + num_layers + 1,))],
            compiler_params=pltpu.CompilerParams(vmem_limit_bytes=1024 * 1024),
            name='write',
        )(*(pltpu.with_memory_space_constraint(value, pltpu.VMEM) for value in (grad_rows, grad_w, grad_b)))
        grad_volume = jnp.transpose(grad_rows.reshape(planes, by_len, bz_len, channels), (3, 0, 1, 2))
        return grad_volume, grad_w, grad_b

    return jax.shard_map(local_step, mesh=mesh, in_specs=(vol_spec, vol_spec, P(), P(), P()), out_specs=(vol_spec, P('dp'), P('dp')), check_vma=False)
```
